512 devices in a mesh: ctx: 64 (over z, y), tp: 8 (over x, core).
Axes of the slice: x: 4, y: 4, z: 16, core: 2. Of those that a mesh axis runs over, the one named last changes fastest.
Arguments:
- rotated_asking_vectors: bfloat16 [2, 2048, 64, 128], P(None, ('ctx', 'tp')), may hold values from -6 to 6
- rotated_match_vectors: bfloat16 [2, 2048, 8, 128], P(None, ('ctx', 'tp')), may hold values from -6 to 6
- content_vectors: bfloat16 [2, 2048, 8, 128], P(None, ('ctx', 'tp')), may hold values from -6 to 6
- result_cotangent: bfloat16 [2, 2048, 64, 128], P(None, ('ctx', 'tp')), may hold values from -6 to 6
Outputs:
- attended: bfloat16 [2, 2048, 64, 128], P(None, ('ctx', 'tp'))
- grad_query: bfloat16 [2, 2048, 64, 128], P(None, ('ctx', 'tp'))
- grad_key: bfloat16 [2, 2048, 8, 128], P(None, ('ctx', 'tp'))
- grad_value: bfloat16 [2, 2048, 8, 128], P(None, ('ctx', 'tp'))
The draws below stay inside these ranges and needn't reach their ends.
All inputs are finite; a program needn't handle non-finite values.
Results may differ from the reference program's by a relative error of at most 0.002.
Values may be sent and summed in bfloat16 or wider, within the bound.
A program may use at most 64 MiB of HBM per device.

```python
import jax
import jax.numpy as jnp
from jax import lax

ASKING_HEAD_COUNT = 64
SHARED_HEAD_COUNT = 8
HEAD_WIDTH = 128
DEPTH_COUNT = 2
WINDOW_LENGTH = 2048
QUERIES_PER_SHARED = 8


def level_of(key, extent, cuts, least, top_value):
    loudness, own = 1.0, jax.random.fold_in(key, 6)
    for position, parts in cuts:
        steps = jnp.exp(jax.random.uniform(jax.random.fold_in(own, position), (parts,), jnp.float32, least / len(cuts), top_value / len(cuts)))
        loudness = loudness * jnp.repeat(steps, extent[position] // parts).reshape([-1 if axis == position else 1 for axis in range(len(extent))])
    return loudness


def noise(rng, shape, spread, reach, pieces=(), kind=jnp.bfloat16):
    result = spread * jax.random.normal(rng, shape, jnp.float32)
    if pieces:
        result = result * level_of(rng, shape, pieces, -0.22, 0.18)
    return jnp.clip(result, -reach, reach).astype(kind)


def setup_inputs(seed: int = 0) -> dict:
    key_list = jax.random.split(jax.random.key(seed), 5)
    return {
        "rotated_asking_vectors": noise(key_list[0], (DEPTH_COUNT, WINDOW_LENGTH, ASKING_HEAD_COUNT, HEAD_WIDTH), 1.0, 6.0, ((1, 512),)),
        "rotated_match_vectors": noise(key_list[1], (DEPTH_COUNT, WINDOW_LENGTH, SHARED_HEAD_COUNT, HEAD_WIDTH), 1.0, 6.0, ((1, 512),)),
        "content_vectors": noise(key_list[2], (DEPTH_COUNT, WINDOW_LENGTH, SHARED_HEAD_COUNT, HEAD_WIDTH), 1.0, 6.0, ((1, 512),)),
        "result_cotangent": noise(key_list[3], (DEPTH_COUNT, WINDOW_LENGTH, ASKING_HEAD_COUNT, HEAD_WIDTH), 1.0, 6.0, ((1, 512),)),
    }


def head_group(operands):
    query_group, key_group, value_group, grad_group = operands
    softmax_scale = HEAD_WIDTH ** -0.5
    places = jnp.arange(WINDOW_LENGTH, dtype=jnp.int32)
    causal_mask = places[None, :] <= places[:, None]
    scores = jnp.einsum("gid,jd->gij", query_group, key_group, precision=lax.Precision.HIGHEST) * softmax_scale
    scores = jnp.where(causal_mask[None], scores, -jnp.inf)
    highest = jnp.max(scores, axis=-1, keepdims=True)
    log_norm = highest + jnp.log(jnp.sum(jnp.exp(scores - highest), axis=-1, keepdims=True))
    probabilities = jnp.exp(scores - log_norm)
    attended = jnp.einsum("gij,jd->gid", probabilities, value_group, precision=lax.Precision.HIGHEST).astype(jnp.bfloat16)
    saved_out = lax.optimization_barrier(attended).astype(jnp.float32)
    row_delta = jnp.sum(grad_group * saved_out, axis=-1, keepdims=True)
    prob_grad = jnp.einsum("gid,jd->gij", grad_group, value_group, precision=lax.Precision.HIGHEST)
    dscore = probabilities * (prob_grad - row_delta)
    query_grad = softmax_scale * jnp.einsum("gij,jd->gid", dscore, key_group, precision=lax.Precision.HIGHEST)
    key_grad = softmax_scale * jnp.einsum("gij,gid->jd", dscore, query_group, precision=lax.Precision.HIGHEST)
    value_grad = jnp.einsum("gij,gid->jd", probabilities, grad_group, precision=lax.Precision.HIGHEST)
    return attended, query_grad.astype(jnp.bfloat16), key_grad.astype(jnp.bfloat16), value_grad.astype(jnp.bfloat16)


def reference(rotated_asking_vectors, rotated_match_vectors, content_vectors, result_cotangent):
    outputs = ([], [], [], [])
    for depth_position in range(DEPTH_COUNT):
        expanded_asking_vectors = rotated_asking_vectors[depth_position].astype(jnp.float32).reshape(WINDOW_LENGTH, SHARED_HEAD_COUNT, QUERIES_PER_SHARED, HEAD_WIDTH).transpose(1, 2, 0, 3)
        expanded_cotangent = result_cotangent[depth_position].astype(jnp.float32).reshape(WINDOW_LENGTH, SHARED_HEAD_COUNT, QUERIES_PER_SHARED, HEAD_WIDTH).transpose(1, 2, 0, 3)
        key_wide = rotated_match_vectors[depth_position].astype(jnp.float32).transpose(1, 0, 2)
        value_wide = content_vectors[depth_position].astype(jnp.float32).transpose(1, 0, 2)
        attended, query_grad, key_grad, value_grad = lax.map(head_group, (expanded_asking_vectors, key_wide, value_wide, expanded_cotangent))
        outputs[0].append(attended.transpose(2, 0, 1, 3).reshape(WINDOW_LENGTH, ASKING_HEAD_COUNT, HEAD_WIDTH))
        outputs[1].append(query_grad.transpose(2, 0, 1, 3).reshape(WINDOW_LENGTH, ASKING_HEAD_COUNT, HEAD_WIDTH))
        outputs[2].append(key_grad.transpose(1, 0, 2))
        outputs[3].append(value_grad.transpose(1, 0, 2))
    return (jnp.stack(outputs[0]), jnp.stack(outputs[1]), jnp.stack(outputs[2]), jnp.stack(outputs[3]))
```

```python
import functools

import jax
import jax.numpy as jnp
from jax import lax
from jax.experimental import pallas as pl
from jax.experimental.pallas import tpu as pltpu
from jax.sharding import Mesh
from jax.sharding import PartitionSpec as P

MESH = pl.DeviceIdType.MESH
F32 = jnp.float32
BF16 = jnp.bfloat16
NZ, NY, NX = 16, 4, 4
MASKED = -1e30


def nt(a, b):
    return lax.dot_general(a, b, (((1,), (1,)), ((), ())), preferred_element_type=F32)


def nn(a, b):
    return lax.dot_general(a, b, (((1,), (0,)), ((), ())), preferred_element_type=F32)


def split(a):
    high = a.astype(BF16)
    return high, (a - high.astype(F32)).astype(BF16)


def kernel(
    q_hbm, g_hbm, kv_hbm, o_hbm, dq_hbm, dkv_ref,
    q_home, g_home, kv_home, q_rows, g_rows, kv_all,
    keys, values, keys_t, values_t, diagonal, scores, probs, dscores, g_twice, q_twice,
    o_rows, dq_rows, part, other, arrived, final,
    in_sem, zkv_s, zkv_r, zq_s, zq_r, zg_s, zg_r, ag_s, ag_r, fw_s, fw_r,
    o_s, o_r, dq_s, dq_r, sib_s, sib_r, rs_s, rs_r, fin_s, fin_r,
):
    z, y, x, c = (lax.axis_index(a) for a in ("z", "y", "x", "c"))
    chip = y * NX + x
    layer, group = z // 8, lax.rem(z, 8)
    scale = 128 ** -0.5

    stage = [
        pltpu.make_async_copy(kv_hbm, kv_home, in_sem.at[0]),
        pltpu.make_async_copy(kv_hbm.at[layer, group], kv_all.at[chip, c, z], in_sem.at[1]),
        pltpu.make_async_copy(q_hbm, q_home, in_sem.at[2]),
        pltpu.make_async_copy(g_hbm, g_home, in_sem.at[3]),
        pltpu.make_async_copy(q_hbm.at[layer, :, group], q_rows.at[z], in_sem.at[4]),
        pltpu.make_async_copy(g_hbm.at[layer, :, group], g_rows.at[z], in_sem.at[5]),
    ]
    for copy in stage:
        copy.start()

    def z_at(d):
        return lax.rem(z + d, NZ)

    def chip_at(e, sign):
        dy, dx = e // NX, lax.rem(e, NX)
        return lax.rem(y + NY + sign * dy, NY), lax.rem(x + NX + sign * dx, NX)

    barrier = pltpu.get_barrier_semaphore()

    def greet(d, _):
        pl.semaphore_signal(barrier, inc=1, device_id=(z_at(d), y, x, c), device_id_type=MESH)
        pl.semaphore_signal(barrier, inc=1, device_id=(z_at(d), y, x, 1 - c), device_id_type=MESH)
        yy, xx = chip_at(d, 1)
        pl.semaphore_signal(barrier, inc=1, device_id=(z, yy, xx, c), device_id_type=MESH)
        return 0

    lax.fori_loop(1, 16, greet, 0)
    pl.semaphore_signal(barrier, inc=1, device_id=(z, y, x, 1 - c), device_id_type=MESH)

    key_row = lax.broadcasted_iota(jnp.int32, (512, 128), 0)
    lane = lax.broadcasted_iota(jnp.int32, (512, 128), 1)
    key_pos = 128 * ((key_row // 8) % 4) + 8 * (key_row // 32) + key_row % 8
    row_pos = 128 * (lane // 32) + (lane // 8) % 4 + 8 * chip + 4 * c
    diagonal[...] = key_pos - row_pos
    identity = (
        lax.broadcasted_iota(jnp.int32, (128, 128), 0)
        == lax.broadcasted_iota(jnp.int32, (128, 128), 1)
    ).astype(F32).astype(BF16)

    for copy in stage:
        copy.wait()
    pl.semaphore_wait(barrier, 46)

    def to_z(src, dst, send, recv):
        def make(d):
            t = z_at(d)
            return pltpu.make_async_remote_copy(
                src_ref=src(t // 8, lax.rem(t, 8)), dst_ref=dst, send_sem=send.at[d],
                recv_sem=recv.at[d], device_id=(t, y, x, c), device_id_type=MESH,
            )
        return make

    zkv = to_z(lambda l, g: kv_home.at[l, g], kv_all.at[chip, c, z], zkv_s, zkv_r)
    zq = to_z(lambda l, g: q_home.at[l, :, g], q_rows.at[z], zq_s, zq_r)
    zg = to_z(lambda l, g: g_home.at[l, :, g], g_rows.at[z], zg_s, zg_r)

    def loop(low, high, body):
        def step(i, _):
            body(i)
            return 0
        lax.fori_loop(low, high, step, 0)

    loop(1, 16, lambda d: zkv(d).start())
    loop(1, 16, lambda d: zq(d).start())
    loop(1, 16, lambda d: zg(d).start())
    loop(1, 16, lambda d: zkv(d).wait_recv())

    def gather(e):
        yy, xx = chip_at(e, 1)
        return pltpu.make_async_remote_copy(
            src_ref=kv_all.at[chip, c], dst_ref=kv_all.at[chip, c], send_sem=ag_s.at[e],
            recv_sem=ag_r.at[e], device_id=(z, yy, xx, c), device_id_type=MESH,
        )

    def forward(e):
        yy, xx = chip_at(e, -1)
        block = kv_all.at[yy * NX + xx, c]
        return pltpu.make_async_remote_copy(
            src_ref=block, dst_ref=block, send_sem=fw_s.at[e],
            recv_sem=fw_r.at[e], device_id=(z, y, x, 1 - c), device_id_type=MESH,
        )

    loop(1, 16, lambda e: gather(e).start())
    forward(0).start()

    def pass_on(e):
        gather(e).wait_recv()
        forward(e).start()

    loop(1, 16, pass_on)

    low_half = lax.rem(lax.broadcasted_iota(jnp.int32, (128, 128), 0), 8) < 4

    def unpack(e):
        forward(e).wait_recv()
        yy, xx = chip_at(e, -1)
        j = yy * NX + xx
        a = kv_all[j, 0].astype(F32).reshape(128, 128)
        b = kv_all[j, 1].astype(F32).reshape(128, 128)
        k = jnp.where(low_half, a, pltpu.roll(b, 4, 0)).astype(BF16)
        v = jnp.where(low_half, pltpu.roll(a, 124, 0), b).astype(BF16)
        at = pl.ds(pl.multiple_of(j * 32, 32), 32)
        for kg in range(4):
            keys[kg, at, :] = k[32 * kg : 32 * kg + 32]
            values[kg, at, :] = v[32 * kg : 32 * kg + 32]

    loop(0, 16, unpack)

    def transposed(kg):
        keys_t[kg] = nt(identity, keys[kg]).astype(BF16)
        values_t[kg] = nt(identity, values[kg]).astype(BF16)

    loop(0, 4, transposed)
    loop(1, 16, lambda d: zq(d).wait_recv())
    loop(1, 16, lambda d: zg(d).wait_recv())

    def home(rows, out, send, recv):
        def make(t, s):
            return pltpu.make_async_remote_copy(
                src_ref=rows.at[t], dst_ref=out.at[layer, :, group], send_sem=send.at[t],
                recv_sem=recv.at[s], device_id=(t, y, x, c), device_id_type=MESH,
            )
        def own():
            return pltpu.make_async_copy(rows.at[z], out.at[layer, :, group], recv.at[z])
        def start(t):
            @pl.when(t != z)
            def _():
                make(t, z).start()
            @pl.when(t == z)
            def _():
                own().start()
        def finish(t):
            @pl.when(t != z)
            def _():
                make(t, t).wait_recv()
                make(t, z).wait_send()
            @pl.when(t == z)
            def _():
                own().wait()
        return start, finish

    o_start, o_finish = home(o_rows, o_hbm, o_s, o_r)
    dq_start, dq_finish = home(dq_rows, dq_hbm, dq_s, dq_r)

    for rg in range(4):
        q = q_rows[4 * rg : 4 * rg + 4].astype(F32).reshape(128, 128).astype(BF16)
        g = g_rows[4 * rg : 4 * rg + 4].astype(F32).reshape(128, 128).astype(BF16)
        for twice, value in ((q_twice, q), (g_twice, g)):
            twice[256 * rg : 256 * rg + 128] = value
            twice[256 * rg + 128 : 256 * rg + 256] = value
        g_t = nt(identity, g)

        def score(kg, top, last):
            s = nt(keys[kg], q) * scale
            if last:
                s = jnp.where(diagonal[...] <= 0, s, MASKED)
            scores[kg] = s
            return jnp.maximum(top, jnp.max(s.reshape(64, 8, 128), axis=0))

        top = jnp.full((8, 128), MASKED, F32)
        top = lax.fori_loop(0, rg, lambda kg, t: score(kg, t, False), top)
        top = score(rg, top, True)
        top = jnp.max(top, axis=0, keepdims=True)

        def attend(kg, carry):
            total, acc = carry
            p = jnp.exp(scores[kg] - top)
            total = total + jnp.sum(p.reshape(64, 8, 128), axis=0)
            acc = acc + nn(values_t[kg], jnp.concatenate(split(p), axis=1))
            return total, acc

        total, acc = lax.fori_loop(
            0, rg + 1, attend, (jnp.zeros((8, 128), F32), jnp.zeros((128, 256), F32))
        )
        total = jnp.sum(total, axis=0, keepdims=True)
        o_t = (acc[:, :128] + acc[:, 128:]) / total
        log_norm = top + jnp.log(total)
        row_delta = jnp.sum(g_t * o_t.astype(BF16).astype(F32), axis=0, keepdims=True)
        o_rows[4 * rg : 4 * rg + 4] = o_t.T.reshape(4, 4, 8, 128).astype(BF16)
        loop(4 * rg, 4 * rg + 4, o_start)

        def backward(kg, acc):
            p = jnp.exp(scores[kg] - log_norm)
            ds = p * (nt(values[kg], g) - row_delta)
            p2 = jnp.concatenate(split(p), axis=1)
            ds2 = jnp.concatenate(split(ds), axis=1)
            probs[kg, :, 256 * rg : 256 * rg + 256] = p2
            dscores[kg, :, 256 * rg : 256 * rg + 256] = ds2
            return acc + nn(keys_t[kg], ds2)

        acc = lax.fori_loop(0, rg + 1, backward, jnp.zeros((128, 256), F32))
        dq_t = (acc[:, :128] + acc[:, 128:]) * scale
        dq_rows[4 * rg : 4 * rg + 4] = dq_t.T.reshape(4, 4, 8, 128).astype(BF16)
        loop(4 * rg, 4 * rg + 4, dq_start)

    def sibling(kg):
        return pltpu.make_async_remote_copy(
            src_ref=part.at[1 - c, kg], dst_ref=other.at[kg], send_sem=sib_s.at[kg],
            recv_sem=sib_r.at[kg], device_id=(z, y, x, 1 - c), device_id_type=MESH,
        )

    def scatter(kg, e):
        yy, xx = chip_at(e, 1)
        rows = pl.ds(pl.multiple_of((yy * NX + xx) * 32, 32), 32)
        return pltpu.make_async_remote_copy(
            src_ref=part.at[c, kg, rows], dst_ref=arrived.at[e, kg], send_sem=rs_s.at[kg, e],
            recv_sem=rs_r.at[kg, e], device_id=(z, yy, xx, c), device_id_type=MESH,
        )

    for kg in range(4):
        part[0, kg] = nn(dscores[kg, :, 256 * kg :], q_twice[256 * kg :])
        part[1, kg] = nn(probs[kg, :, 256 * kg :], g_twice[256 * kg :])
        sibling(kg).start()

    def combine(kg):
        sibling(kg).wait_recv()
        part[c, kg] = part[c, kg] + other[kg]
        loop(1, 16, lambda e: scatter(kg, e).start())

    loop(0, 4, combine)

    factor = jnp.where(c == 0, scale, 1.0).astype(F32)
    own_rows = pl.ds(pl.multiple_of(chip * 32, 32), 32)

    def finish(kg):
        loop(1, 16, lambda e: scatter(kg, e).wait_recv())
        total = lax.fori_loop(
            1, 16, lambda e, t: t + arrived[e, kg], part[c, kg, own_rows]
        ) * factor
        final[pl.ds(4 * kg, 4)] = total.reshape(4, 8, 128).astype(BF16)

    loop(0, 4, finish)

    def out(d, core):
        t = z_at(d)
        return pltpu.make_async_remote_copy(
            src_ref=final.at[t], dst_ref=dkv_ref.at[c, z], send_sem=fin_s.at[d, core],
            recv_sem=fin_r.at[d, c], device_id=(t, y, x, core), device_id_type=MESH,
        )

    def into(d, core):
        t = z_at(d)
        return pltpu.make_async_remote_copy(
            src_ref=final.at[t], dst_ref=dkv_ref.at[c, z], send_sem=fin_s.at[d, core],
            recv_sem=fin_r.at[d, core], device_id=(t, y, x, c), device_id_type=MESH,
        )

    dkv_ref[c, z] = final[z]
    out(0, 1 - c).start()
    loop(1, 16, lambda d: (out(d, c).start(), out(d, 1 - c).start()))

    loop(1, 16, lambda d: (zkv(d).wait_send(), zq(d).wait_send(), zg(d).wait_send()))
    loop(1, 16, lambda e: gather(e).wait_send())
    loop(0, 16, lambda e: forward(e).wait_send())
    loop(0, 16, lambda t: (o_finish(t), dq_finish(t)))
    loop(0, 4, lambda kg: sibling(kg).wait_send())
    loop(0, 4, lambda kg: loop(1, 16, lambda e: scatter(kg, e).wait_send()))
    out(0, 1 - c).wait_send()
    into(0, 1 - c).wait_recv()
    loop(1, 16, lambda d: (out(d, c).wait_send(), out(d, 1 - c).wait_send()))
    loop(1, 16, lambda d: (into(d, c).wait_recv(), into(d, 1 - c).wait_recv()))


def on_device(q, k, v, g):
    core = lax.axis_index("c")
    kv = jnp.concatenate([k.transpose(0, 2, 1, 3), v.transpose(0, 2, 1, 3)], axis=2)
    wide = (2, 4, 8, 8, 128)
    dma = pltpu.SemaphoreType.DMA
    hbm = pl.BlockSpec(memory_space=pltpu.MemorySpace.HBM)
    vmem = pl.BlockSpec(memory_space=pltpu.VMEM)
    o, dq, dkv = pl.pallas_call(
        kernel,
        out_shape=(
            jax.ShapeDtypeStruct(wide, BF16),
            jax.ShapeDtypeStruct(wide, BF16),
            jax.ShapeDtypeStruct((2, 16, 8, 128), BF16),
        ),
        in_specs=[hbm, hbm, hbm],
        out_specs=(hbm, hbm, vmem),
        scratch_shapes=[
            pltpu.VMEM(wide, BF16),
            pltpu.VMEM(wide, BF16),
            pltpu.VMEM((2, 8, 8, 128), BF16),
            pltpu.VMEM((16, 4, 8, 128), BF16),
            pltpu.VMEM((16, 4, 8, 128), BF16),
            pltpu.VMEM((16, 2, 16, 8, 128), BF16),
            pltpu.VMEM((4, 512, 128), BF16),
            pltpu.VMEM((4, 512, 128), BF16),
            pltpu.VMEM((4, 128, 512), BF16),
            pltpu.VMEM((4, 128, 512), BF16),
            pltpu.VMEM((512, 128), jnp.int32),
            pltpu.VMEM((4, 512, 128), F32),
            pltpu.VMEM((4, 512, 1024), BF16),
            pltpu.VMEM((4, 512, 1024), BF16),
            pltpu.VMEM((1024, 128), BF16),
            pltpu.VMEM((1024, 128), BF16),
            pltpu.VMEM((16, 4, 8, 128), BF16),
            pltpu.VMEM((16, 4, 8, 128), BF16),
            pltpu.VMEM((2, 4, 512, 128), F32),
            pltpu.VMEM((4, 512, 128), F32),
            pltpu.VMEM((16, 4, 32, 128), F32),
            pltpu.VMEM((16, 8, 128), BF16),
            dma((6,)),
            dma((16,)), dma((16,)), dma((16,)), dma((16,)), dma((16,)), dma((16,)),
            dma((16,)), dma((16,)), dma((16,)), dma((16,)),
            dma((16,)), dma((16,)), dma((16,)), dma((16,)),
            dma((4,)), dma((4,)), dma((4, 16)), dma((4, 16)), dma((16, 2)), dma((16, 2)),
        ],
        compiler_params=pltpu.CompilerParams(
            collective_id=1, has_side_effects=True, vmem_limit_bytes=48 * 2**20
        ),
        name="attend",
    )(q.reshape(wide), g.reshape(wide), kv)
    dkv = lax.dynamic_slice_in_dim(dkv.reshape(2, 2, 8, 8, 128), 4 * core, 4, 3)
    dkv = dkv.transpose(0, 1, 3, 2, 4)
    return o.reshape(q.shape), dq.reshape(q.shape), dkv[0], dkv[1]


def solution(mesh):
    grid = Mesh(mesh.devices.reshape(NZ, NY, NX, 2), ("z", "y", "x", "c"))
    spec = P(None, ("z", "y", "x", "c"), None, None)
    return jax.shard_map(
        on_device, mesh=grid, in_specs=(spec,) * 4, out_specs=(spec,) * 4, check_vma=False
    )
```

```python
import functools

import jax
import jax.numpy as jnp
from jax import lax
from jax.experimental import pallas as pl
from jax.experimental.pallas import tpu as pltpu
from jax.sharding import Mesh
from jax.sharding import PartitionSpec as P

MESH = pl.DeviceIdType.MESH
F32 = jnp.float32
BF16 = jnp.bfloat16
NZ, NY, NX = 16, 4, 4
MASKED = -1e30


def nt(a, b):
    return lax.dot_general(a, b, (((1,), (1,)), ((), ())), preferred_element_type=F32)


def nn(a, b):
    return lax.dot_general(a, b, (((1,), (0,)), ((), ())), preferred_element_type=F32)


def split(a):
    high = a.astype(BF16)
    return high, (a - high.astype(F32)).astype(BF16)


def kernel(
    q_hbm, k_hbm, v_hbm, g_hbm, o_hbm, dq_hbm, dkv_ref,
    q_home, k_home, v_home, g_home, kv_wide, kv_home, q_rows, g_rows, kv_all,
    keys, values, keys_t, values_t, diagonal, scores, probs, dscores, g_twice, q_twice,
    o_rows, dq_rows, part, other, arrived, final,
    in_sem, zkv_s, zkv_r, zq_s, zq_r, zg_s, zg_r, ag_s, ag_r, fw_s, fw_r,
    o_s, o_r, dq_s, dq_r, sib_s, sib_r, rs_s, rs_r, fin_s, fin_r,
):
    z, y, x, c = (lax.axis_index(a) for a in ("z", "y", "x", "c"))
    chip = y * NX + x
    layer, group = z // 8, lax.rem(z, 8)
    scale = 128 ** -0.5

    stage = [
        pltpu.make_async_copy(k_hbm, k_home, in_sem.at[0]),
        pltpu.make_async_copy(v_hbm, v_home, in_sem.at[1]),
        pltpu.make_async_copy(q_hbm, q_home, in_sem.at[2]),
        pltpu.make_async_copy(g_hbm, g_home, in_sem.at[3]),
        pltpu.make_async_copy(q_hbm.at[layer, :, group], q_rows.at[z], in_sem.at[4]),
        pltpu.make_async_copy(g_hbm.at[layer, :, group], g_rows.at[z], in_sem.at[5]),
    ]
    for copy in stage:
        copy.start()

    def z_at(d):
        return lax.rem(z + d, NZ)

    def chip_at(e, sign):
        dy, dx = e // NX, lax.rem(e, NX)
        return lax.rem(y + NY + sign * dy, NY), lax.rem(x + NX + sign * dx, NX)

    barrier = pltpu.get_barrier_semaphore()

    def greet(d, _):
        pl.semaphore_signal(barrier, inc=1, device_id=(z_at(d), y, x, c), device_id_type=MESH)
        pl.semaphore_signal(barrier, inc=1, device_id=(z_at(d), y, x, 1 - c), device_id_type=MESH)
        yy, xx = chip_at(d, 1)
        pl.semaphore_signal(barrier, inc=1, device_id=(z, yy, xx, c), device_id_type=MESH)
        return 0

    lax.fori_loop(1, 16, greet, 0)
    pl.semaphore_signal(barrier, inc=1, device_id=(z, y, x, 1 - c), device_id_type=MESH)

    key_row = lax.broadcasted_iota(jnp.int32, (512, 128), 0)
    lane = lax.broadcasted_iota(jnp.int32, (512, 128), 1)
    key_pos = 128 * ((key_row >> 3) & 3) + 8 * (key_row >> 5) + (key_row & 7)
    row_pos = 128 * (lane >> 5) + ((lane >> 3) & 3) + 8 * chip + 4 * c
    diagonal[...] = key_pos - row_pos
    identity = (
        lax.broadcasted_iota(jnp.int32, (128, 128), 0)
        == lax.broadcasted_iota(jnp.int32, (128, 128), 1)
    ).astype(F32).astype(BF16)

    with jax.named_scope("p0_kv"):
        stage[0].wait()
        stage[1].wait()
        for l in range(2):
            for i in range(4):
                kv_wide[l, :, i, :] = k_home[l, i].astype(F32)
                kv_wide[l, :, 4 + i, :] = v_home[l, i].astype(F32)
        kv_home[...] = kv_wide[...].astype(BF16)
        kv_all[chip, c, 8] = kv_wide[layer, group].astype(BF16)
        for copy in stage[2:]:
            copy.wait()
    with jax.named_scope("p1_barrier"):
        pl.semaphore_wait(barrier, 46)

    def to_z(src, dst, send, recv):
        def make(d):
            t = z_at(d)
            return pltpu.make_async_remote_copy(
                src_ref=src(t // 8, lax.rem(t, 8)), dst_ref=dst(d), send_sem=send.at[d],
                recv_sem=recv.at[d], device_id=(t, y, x, c), device_id_type=MESH,
            )
        return make

    zkv = to_z(
        lambda l, g: kv_home.at[l, g], lambda d: kv_all.at[chip, c, (24 - d) & 15], zkv_s, zkv_r
    )
    zq = to_z(lambda l, g: q_home.at[l, :, g], lambda d: q_rows.at[z], zq_s, zq_r)
    zg = to_z(lambda l, g: g_home.at[l, :, g], lambda d: g_rows.at[z], zg_s, zg_r)

    def loop(low, high, body):
        def step(i, _):
            body(i)
            return 0
        lax.fori_loop(low, high, step, 0)

    with jax.named_scope("p2_zstart"):
        loop(1, 16, lambda d: zkv(d).start())
        loop(1, 16, lambda d: zq(d).start())
        loop(1, 16, lambda d: zg(d).start())
    PIECES = ((4, 9), (0, 4), (13, 3))

    def gather(n, e):
        yy, xx = chip_at(e, 1)
        block = kv_all.at[chip, c, pl.ds(*PIECES[n])]
        return pltpu.make_async_remote_copy(
            src_ref=block, dst_ref=block, send_sem=ag_s.at[n, e],
            recv_sem=ag_r.at[n, e], device_id=(z, yy, xx, c), device_id_type=MESH,
        )

    def forward(n, e):
        yy, xx = chip_at(e, -1)
        block = kv_all.at[yy * NX + xx, c, pl.ds(*PIECES[n])]
        return pltpu.make_async_remote_copy(
            src_ref=block, dst_ref=block, send_sem=fw_s.at[n, e],
            recv_sem=fw_r.at[n, e], device_id=(z, y, x, 1 - c), device_id_type=MESH,
        )

    with jax.named_scope("p3_zkv"):
        loop(1, 5, lambda d: zkv(d).wait_recv())
        loop(12, 16, lambda d: zkv(d).wait_recv())
        loop(1, 16, lambda e: gather(0, e).start())
        forward(0, 0).start()
        loop(5, 12, lambda d: zkv(d).wait_recv())
        for n in (1, 2):
            loop(1, 16, lambda e: gather(n, e).start())
            forward(n, 0).start()

    low_half = lax.broadcasted_iota(jnp.int32, (8, 128), 0) < 4

    def pass_on(n, e):
        gather(n, e).wait_recv()
        forward(n, e).start()

    def unpack(e):
        for n in range(3):
            forward(n, e).wait_recv()
        yy, xx = chip_at(e, -1)
        j = yy * NX + xx
        ks, vs = [], []
        for plane in range(16):
            slot = (plane + 24 - z) & 15
            a = kv_all[j, 0, slot].astype(F32)
            b = kv_all[j, 1, slot].astype(F32)
            ks.append(jnp.where(low_half, a, pltpu.roll(b, 4, 0)))
            vs.append(jnp.where(low_half, pltpu.roll(a, 4, 0), b))
        at = pl.ds(pl.multiple_of(j * 32, 32), 32)
        for kg in range(4):
            keys[kg, at, :] = jnp.concatenate(ks[4 * kg : 4 * kg + 4], axis=0).astype(BF16)
            values[kg, at, :] = jnp.concatenate(vs[4 * kg : 4 * kg + 4], axis=0).astype(BF16)

    with jax.named_scope("p5_agwait"):
        loop(1, 16, lambda e: pass_on(0, e))

        def last(e):
            pass_on(1, e)
            pass_on(2, e)

        def step(e):
            last(e)
            unpack(e - 2)

        loop(1, 2, last)
        loop(2, 16, step)
    with jax.named_scope("p6_unpack"):
        loop(14, 16, unpack)

    with jax.named_scope("p8_qwait"):
        loop(1, 16, lambda d: zq(d).wait_recv())
        loop(1, 16, lambda d: zg(d).wait_recv())

    def home(rows, out, send, recv):
        def make(t, s):
            return pltpu.make_async_remote_copy(
                src_ref=rows.at[t], dst_ref=out.at[layer, :, group], send_sem=send.at[t],
                recv_sem=recv.at[s], device_id=(t, y, x, c), device_id_type=MESH,
            )
        def own():
            return pltpu.make_async_copy(rows.at[z], out.at[layer, :, group], recv.at[z])
        def start(t):
            @pl.when(t != z)
            def _():
                make(t, z).start()
            @pl.when(t == z)
            def _():
                own().start()
        def finish(t):
            @pl.when(t != z)
            def _():
                make(t, t).wait_recv()
                make(t, z).wait_send()
            @pl.when(t == z)
            def _():
                own().wait()
        return start, finish

    o_start, o_finish = home(o_rows, o_hbm, o_s, o_r)
    dq_start, dq_finish = home(dq_rows, dq_hbm, dq_s, dq_r)

    factor_2 = scale * 1.4426950408889634

    def block_of(rg):
        q = q_rows[4 * rg : 4 * rg + 4].astype(F32).reshape(128, 128).astype(BF16)
        g = g_rows[4 * rg : 4 * rg + 4].astype(F32).reshape(128, 128).astype(BF16)
        for twice, value in ((q_twice, q), (g_twice, g)):
            twice[256 * rg : 256 * rg + 128] = value
            twice[256 * rg + 128 : 256 * rg + 256] = value
        lanes = slice(256 * rg, 256 * rg + 256)
        top = jnp.full((8, 128), MASKED, F32)
        for kg in range(rg + 1):
            s = nt(keys[kg], q) * factor_2
            if kg == rg:
                s = jnp.where(diagonal[...] <= 0, s, MASKED)
            scores[rg % 2, kg] = s
            top = jnp.maximum(top, jnp.max(s.reshape(64, 8, 128), axis=0))
        top = jnp.max(top, axis=0, keepdims=True)
        total = jnp.zeros((8, 128), F32)
        for kg in range(rg + 1):
            e = jnp.exp2(scores[rg % 2, kg] - top)
            scores[rg % 2, kg] = e
            total = total + jnp.sum(e.reshape(64, 8, 128), axis=0)
        inverse = 1.0 / jnp.sum(total, axis=0, keepdims=True)
        acc = jnp.zeros((128, 256), F32)
        for kg in range(rg + 1):
            p = scores[rg % 2, kg] * inverse
            p2 = jnp.concatenate(split(p), axis=1)
            probs[kg, :, lanes] = p2
            scores[rg % 2, kg] = p
            acc = acc + nn(values_t[kg], p2)
        o_t = acc[:, :128] + acc[:, 128:]
        row_delta = jnp.sum(nt(identity, g) * o_t.astype(BF16).astype(F32), axis=0, keepdims=True)
        o_rows[4 * rg : 4 * rg + 4] = o_t.T.reshape(4, 4, 8, 128).astype(BF16)
        acc = jnp.zeros((128, 256), F32)
        for kg in range(rg + 1):
            ds = scores[rg % 2, kg] * (nt(values[kg], g) - row_delta)
            ds2 = jnp.concatenate(split(ds), axis=1)
            dscores[kg, :, lanes] = ds2
            acc = acc + nn(keys_t[kg], ds2)
        dq_t = (acc[:, :128] + acc[:, 128:]) * scale
        dq_rows[4 * rg : 4 * rg + 4] = dq_t.T.reshape(4, 4, 8, 128).astype(BF16)

    with jax.named_scope("p9_rg01"):
        for kg in range(4):
            keys_t[kg] = nt(identity, keys[kg]).astype(BF16)
            values_t[kg] = nt(identity, values[kg]).astype(BF16)
        block_of(0)
        block_of(1)
    loop(0, 8, lambda t: (o_start(t), dq_start(t)))
    with jax.named_scope("p9_rg23"):
        block_of(2)
        block_of(3)
    loop(8, 16, lambda t: (o_start(t), dq_start(t)))

    def sibling(kg):
        return pltpu.make_async_remote_copy(
            src_ref=part.at[1 - c, kg], dst_ref=other.at[kg], send_sem=sib_s.at[kg],
            recv_sem=sib_r.at[kg], device_id=(z, y, x, 1 - c), device_id_type=MESH,
        )

    def scatter(kg, e):
        yy, xx = chip_at(e, 1)
        rows = pl.ds(pl.multiple_of((yy * NX + xx) * 32, 32), 32)
        return pltpu.make_async_remote_copy(
            src_ref=part.at[c, kg, rows], dst_ref=arrived.at[e, kg], send_sem=rs_s.at[kg, e],
            recv_sem=rs_r.at[kg, e], device_id=(z, yy, xx, c), device_id_type=MESH,
        )

    with jax.named_scope("pa_dkv"):
        for kg in range(4):
            part[0, kg] = nn(dscores[kg, :, 256 * kg :], q_twice[256 * kg :])
            part[1, kg] = nn(probs[kg, :, 256 * kg :], g_twice[256 * kg :])
            sibling(kg).start()

    def combine(kg):
        sibling(kg).wait_recv()
        part[c, kg] = part[c, kg] + other[kg]
        loop(1, 16, lambda e: scatter(kg, e).start())

    with jax.named_scope("pb_combine"):
        loop(0, 4, combine)

    factor = jnp.where(c == 0, scale, 1.0).astype(F32)
    own_rows = pl.ds(pl.multiple_of(chip * 32, 32), 32)

    def finish(kg):
        loop(1, 16, lambda e: scatter(kg, e).wait_recv())
        total = lax.fori_loop(
            1, 16, lambda e, t: t + arrived[e, kg], part[c, kg, own_rows]
        ) * factor
        final[pl.ds(4 * kg, 4)] = total.reshape(4, 8, 128).astype(BF16)

    with jax.named_scope("pc_rs"):
        loop(0, 4, finish)

    def out(d, core):
        t = z_at(d)
        return pltpu.make_async_remote_copy(
            src_ref=final.at[t], dst_ref=dkv_ref.at[c, z], send_sem=fin_s.at[d, core],
            recv_sem=fin_r.at[d, c], device_id=(t, y, x, core), device_id_type=MESH,
        )

    def into(d, core):
        t = z_at(d)
        return pltpu.make_async_remote_copy(
            src_ref=final.at[t], dst_ref=dkv_ref.at[c, z], send_sem=fin_s.at[d, core],
            recv_sem=fin_r.at[d, core], device_id=(t, y, x, c), device_id_type=MESH,
        )

    with jax.named_scope("pd_start"):
        dkv_ref[c, z] = final[z]
        out(0, 1 - c).start()
        loop(1, 16, lambda d: (out(d, c).start(), out(d, 1 - c).start()))

    with jax.named_scope("pe_sends"):
        loop(1, 16, lambda d: (zkv(d).wait_send(), zq(d).wait_send(), zg(d).wait_send()))
        for n in range(3):
            loop(1, 16, lambda e: gather(n, e).wait_send())
            loop(0, 16, lambda e: forward(n, e).wait_send())
        loop(0, 16, lambda t: (o_finish(t), dq_finish(t)))
        loop(0, 4, lambda kg: sibling(kg).wait_send())
        loop(0, 4, lambda kg: loop(1, 16, lambda e: scatter(kg, e).wait_send()))
    with jax.named_scope("pf_dkv"):
        out(0, 1 - c).wait_send()
        into(0, 1 - c).wait_recv()
        loop(1, 16, lambda d: (out(d, c).wait_send(), out(d, 1 - c).wait_send()))
        loop(1, 16, lambda d: (into(d, c).wait_recv(), into(d, 1 - c).wait_recv()))


def on_device(q, k, v, g):
    core = lax.axis_index("c")
    wide = (2, 4, 8, 8, 128)
    dma = pltpu.SemaphoreType.DMA
    hbm = pl.BlockSpec(memory_space=pltpu.MemorySpace.HBM)
    vmem = pl.BlockSpec(memory_space=pltpu.VMEM)
    o, dq, dkv = pl.pallas_call(
        kernel,
        out_shape=(
            jax.ShapeDtypeStruct(wide, BF16),
            jax.ShapeDtypeStruct(wide, BF16),
            jax.ShapeDtypeStruct((2, 16, 8, 128), BF16),
        ),
        in_specs=[hbm, hbm, hbm, hbm],
        out_specs=(hbm, hbm, vmem),
        scratch_shapes=[
            pltpu.VMEM(wide, BF16),
            pltpu.VMEM((2, 4, 8, 128), BF16),
            pltpu.VMEM((2, 4, 8, 128), BF16),
            pltpu.VMEM(wide, BF16),
            pltpu.VMEM((2, 8, 8, 128), F32),
            pltpu.VMEM((2, 8, 8, 128), BF16),
            pltpu.VMEM((16, 4, 8, 128), BF16),
            pltpu.VMEM((16, 4, 8, 128), BF16),
            pltpu.VMEM((16, 2, 16, 8, 128), BF16),
            pltpu.VMEM((4, 512, 128), BF16),
            pltpu.VMEM((4, 512, 128), BF16),
            pltpu.VMEM((4, 128, 512), BF16),
            pltpu.VMEM((4, 128, 512), BF16),
            pltpu.VMEM((512, 128), jnp.int32),
            pltpu.VMEM((2, 4, 512, 128), F32),
            pltpu.VMEM((4, 512, 1024), BF16),
            pltpu.VMEM((4, 512, 1024), BF16),
            pltpu.VMEM((1024, 128), BF16),
            pltpu.VMEM((1024, 128), BF16),
            pltpu.VMEM((16, 4, 8, 128), BF16),
            pltpu.VMEM((16, 4, 8, 128), BF16),
            pltpu.VMEM((2, 4, 512, 128), F32),
            pltpu.VMEM((4, 512, 128), F32),
            pltpu.VMEM((16, 4, 32, 128), F32),
            pltpu.VMEM((16, 8, 128), BF16),
            dma((6,)),
            dma((16,)), dma((16,)), dma((16,)), dma((16,)), dma((16,)), dma((16,)),
            dma((3, 16)), dma((3, 16)), dma((3, 16)), dma((3, 16)),
            dma((16,)), dma((16,)), dma((16,)), dma((16,)),
            dma((4,)), dma((4,)), dma((4, 16)), dma((4, 16)), dma((16, 2)), dma((16, 2)),
        ],
        compiler_params=pltpu.CompilerParams(
            collective_id=1, has_side_effects=True, vmem_limit_bytes=67043328
        ),
        name="attend",
    )(q.reshape(wide), k, v, g.reshape(wide))
    dkv = lax.dynamic_slice_in_dim(dkv.reshape(2, 2, 8, 8, 128), 4 * core, 4, 3)
    dkv = dkv.transpose(0, 1, 3, 2, 4)
    return o.reshape(q.shape), dq.reshape(q.shape), dkv[0], dkv[1]


def solution(mesh):
    grid = Mesh(mesh.devices.reshape(NZ, NY, NX, 2), ("z", "y", "x", "c"))
    spec = P(None, ("z", "y", "x", "c"), None, None)
    return jax.shard_map(
        on_device, mesh=grid, in_specs=(spec,) * 4, out_specs=(spec,) * 4, check_vma=False
    )
```

```python
import functools

import jax
import jax.numpy as jnp
from jax import lax
from jax.experimental import pallas as pl
from jax.experimental.pallas import tpu as pltpu
from jax.sharding import Mesh
from jax.sharding import PartitionSpec as P

MESH = pl.DeviceIdType.MESH
F32 = jnp.float32
BF16 = jnp.bfloat16
NZ, NY, NX = 16, 4, 4
MASKED = -1e30


def nt(a, b):
    return lax.dot_general(a, b, (((1,), (1,)), ((), ())), preferred_element_type=F32)


def nn(a, b):
    return lax.dot_general(a, b, (((1,), (0,)), ((), ())), preferred_element_type=F32)


def split(a):
    high = a.astype(BF16)
    return high, (a - high.astype(F32)).astype(BF16)


def kernel(
    q_hbm, k_hbm, v_hbm, g_hbm, o_hbm, dq_hbm, dkv_ref,
    q_home, k_home, v_home, g_home, kv_wide, kv_home, q_rows, g_rows, kv_all,
    mate, keys_t, values_t, diagonal, scores, probs, dscores, g_twice, q_twice,
    o_rows, dq_rows, part, other, row_in, row_sum, block_in, final,
    in_sem, zkv_s, zkv_r, zq_s, zq_r, zg_s, zg_r, ag_s, ag_r, fw_s, fw_r,
    o_s, o_r, dq_s, dq_r, sib_s, sib_r, row_s, row_r, blk_s, blk_r, fin_s, fin_r,
):
    z, y, x, c = (lax.axis_index(a) for a in ("z", "y", "x", "c"))
    chip = y * NX + x
    layer, group = z // 8, lax.rem(z, 8)
    scale = 128 ** -0.5

    stage = [
        pltpu.make_async_copy(k_hbm, k_home, in_sem.at[0]),
        pltpu.make_async_copy(v_hbm, v_home, in_sem.at[1]),
        pltpu.make_async_copy(q_hbm, q_home, in_sem.at[2]),
        pltpu.make_async_copy(g_hbm, g_home, in_sem.at[3]),
        pltpu.make_async_copy(q_hbm.at[layer, :, group], q_rows.at[z], in_sem.at[4]),
        pltpu.make_async_copy(g_hbm.at[layer, :, group], g_rows.at[z], in_sem.at[5]),
    ]
    for copy in stage:
        copy.start()

    def z_at(d):
        return lax.rem(z + d, NZ)

    def chip_at(e, sign):
        dy, dx = e // NX, lax.rem(e, NX)
        return lax.rem(y + NY + sign * dy, NY), lax.rem(x + NX + sign * dx, NX)

    barrier = pltpu.get_barrier_semaphore()

    def greet(d, _):
        pl.semaphore_signal(barrier, inc=1, device_id=(z_at(d), y, x, c), device_id_type=MESH)
        pl.semaphore_signal(barrier, inc=1, device_id=(z_at(d), y, x, 1 - c), device_id_type=MESH)
        yy, xx = chip_at(d, 1)
        pl.semaphore_signal(barrier, inc=1, device_id=(z, yy, xx, c), device_id_type=MESH)
        return 0

    lax.fori_loop(1, 16, greet, 0)
    pl.semaphore_signal(barrier, inc=1, device_id=(z, y, x, 1 - c), device_id_type=MESH)

    key_pos = lax.broadcasted_iota(jnp.int32, (512, 128), 0)
    lane = lax.broadcasted_iota(jnp.int32, (512, 128), 1)
    row_pos = 128 * (lane >> 5) + ((lane >> 3) & 3) + 8 * chip + 4 * c
    diagonal[...] = key_pos - row_pos
    identity = (
        lax.broadcasted_iota(jnp.int32, (128, 128), 0)
        == lax.broadcasted_iota(jnp.int32, (128, 128), 1)
    ).astype(F32).astype(BF16)

    with jax.named_scope("p0_kv"):
        stage[0].wait()
        stage[1].wait()
        for l in range(2):
            for i in range(4):
                kv_wide[l, :, i, :] = k_home[l, i].astype(F32)
                kv_wide[l, :, 4 + i, :] = v_home[l, i].astype(F32)
        kv_home[...] = kv_wide[...].astype(BF16)
        for copy in stage[2:]:
            copy.wait()
    with jax.named_scope("p1_barrier"):
        pl.semaphore_wait(barrier, 46)

    def to_z(src, dst, send, recv):
        def make(d):
            t = z_at(d)
            return pltpu.make_async_remote_copy(
                src_ref=src.at[t // 8, :, lax.rem(t, 8)], dst_ref=dst.at[z], send_sem=send.at[d],
                recv_sem=recv.at[d], device_id=(t, y, x, c), device_id_type=MESH,
            )
        return make

    half = pl.ds(pl.multiple_of(4 * c, 4), 4)

    def to_core(core, d):
        t = z_at(d)
        return pltpu.make_async_remote_copy(
            src_ref=kv_home.at[t // 8, lax.rem(t, 8), pl.ds(4 * core, 4)],
            dst_ref=kv_all.at[core, (24 - d) & 15, chip, half],
            send_sem=zkv_s.at[core, d], recv_sem=zkv_r.at[c, d],
            device_id=(t, y, x, core), device_id_type=MESH,
        )

    def from_core(core, d):
        return pltpu.make_async_remote_copy(
            src_ref=kv_home.at[0, 0, pl.ds(0, 4)],
            dst_ref=kv_all.at[c, (24 - d) & 15, chip, pl.ds(4 * core, 4)],
            send_sem=zkv_s.at[core, d], recv_sem=zkv_r.at[core, d],
            device_id=(z_at(d), y, x, core), device_id_type=MESH,
        )

    own_kv = pltpu.make_async_remote_copy(
        src_ref=kv_home.at[layer, group], dst_ref=mate, send_sem=zkv_s.at[0, 0],
        recv_sem=zkv_r.at[0, 0], device_id=(z, y, x, 1 - c), device_id_type=MESH,
    )
    zq = to_z(q_home, q_rows, zq_s, zq_r)
    zg = to_z(g_home, g_rows, zg_s, zg_r)

    def loop(low, high, body):
        def step(i, _):
            body(i)
            return 0
        lax.fori_loop(low, high, step, 0)

    with jax.named_scope("p2_zstart"):
        own_kv.start()
        loop(1, 16, lambda d: (to_core(0, d).start(), to_core(1, d).start()))
        loop(1, 16, lambda d: zq(d).start())
        loop(1, 16, lambda d: zg(d).start())

    PIECES = ((4, 9), (0, 4), (13, 3))

    def gather(n, e):
        yy, xx = chip_at(e, 1)
        block = kv_all.at[c, pl.ds(*PIECES[n]), chip]
        return pltpu.make_async_remote_copy(
            src_ref=block, dst_ref=block, send_sem=ag_s.at[n, e],
            recv_sem=ag_r.at[n, e], device_id=(z, yy, xx, c), device_id_type=MESH,
        )

    def forward(n, e):
        yy, xx = chip_at(e, -1)
        block = kv_all.at[c, pl.ds(*PIECES[n]), yy * NX + xx]
        return pltpu.make_async_remote_copy(
            src_ref=block, dst_ref=block, send_sem=fw_s.at[n, e],
            recv_sem=fw_r.at[n, e], device_id=(z, y, x, 1 - c), device_id_type=MESH,
        )

    def backward(n, e):
        yy, xx = chip_at(e, -1)
        block = kv_all.at[1 - c, pl.ds(*PIECES[n]), yy * NX + xx]
        return pltpu.make_async_remote_copy(
            src_ref=block, dst_ref=block, send_sem=fw_s.at[n, e],
            recv_sem=fw_r.at[n, e], device_id=(z, y, x, 1 - c), device_id_type=MESH,
        )

    def received(d):
        from_core(0, d).wait_recv()
        from_core(1, d).wait_recv()

    with jax.named_scope("p3_zkvn"):
        own_kv.wait_recv()
        mine = kv_wide[layer, group]
        theirs = pltpu.roll(mate[...].astype(F32), 4, 0)
        low_half = (lax.broadcasted_iota(jnp.int32, (8, 128), 0) >> 2) == c
        kv_all[c, 8, chip] = jnp.where(low_half, mine, theirs).astype(BF16)
        loop(1, 5, received)
        loop(12, 16, received)
        loop(1, 16, lambda e: gather(0, e).start())
        forward(0, 0).start()
    with jax.named_scope("p3_zkvf"):
        loop(5, 12, received)
        for n in (1, 2):
            loop(1, 16, lambda e: gather(n, e).start())
            forward(n, 0).start()

    def pass_on(n, e):
        gather(n, e).wait_recv()
        forward(n, e).start()

    with jax.named_scope("p4_agnear"):
        loop(1, 16, lambda e: pass_on(0, e))
    with jax.named_scope("p5_agfar"):
        loop(1, 16, lambda e: (pass_on(1, e), pass_on(2, e)))
    with jax.named_scope("p6_fwd"):
        for n in range(3):
            loop(0, 16, lambda e: backward(n, e).wait_recv())

    def plane_group(kind, kg):
        return jnp.concatenate(
            [kv_all[kind, (4 * kg + i + 24 - z) & 15].reshape(128, 128) for i in range(4)], axis=0
        )

    with jax.named_scope("p8_qwait"):
        loop(1, 16, lambda d: zq(d).wait_recv())
        loop(1, 16, lambda d: zg(d).wait_recv())

    def home(rows, out, send, recv):
        def make(t, s):
            return pltpu.make_async_remote_copy(
                src_ref=rows.at[t], dst_ref=out.at[layer, :, group], send_sem=send.at[t],
                recv_sem=recv.at[s], device_id=(t, y, x, c), device_id_type=MESH,
            )
        def own():
            return pltpu.make_async_copy(rows.at[z], out.at[layer, :, group], recv.at[z])
        def start(t):
            @pl.when(t != z)
            def _():
                make(t, z).start()
            @pl.when(t == z)
            def _():
                own().start()
        def finish(t):
            @pl.when(t != z)
            def _():
                make(t, t).wait_recv()
                make(t, z).wait_send()
            @pl.when(t == z)
            def _():
                own().wait()
        return start, finish

    o_start, o_finish = home(o_rows, o_hbm, o_s, o_r)
    dq_start, dq_finish = home(dq_rows, dq_hbm, dq_s, dq_r)

    factor_2 = scale * 1.4426950408889634

    def block_of(rg):
        q = q_rows[4 * rg : 4 * rg + 4].astype(F32).reshape(128, 128).astype(BF16)
        g = g_rows[4 * rg : 4 * rg + 4].astype(F32).reshape(128, 128).astype(BF16)
        for twice, value in ((q_twice, q), (g_twice, g)):
            twice[256 * rg : 256 * rg + 128] = value
            twice[256 * rg + 128 : 256 * rg + 256] = value
        lanes = slice(256 * rg, 256 * rg + 256)
        top = jnp.full((8, 128), MASKED, F32)
        for kg in range(rg + 1):
            s = nt(plane_group(0, kg), q) * factor_2
            if kg == rg:
                s = jnp.where(diagonal[...] <= 0, s, MASKED)
            scores[rg % 2, kg] = s
            top = jnp.maximum(top, jnp.max(s.reshape(64, 8, 128), axis=0))
        top = jnp.max(top, axis=0, keepdims=True)
        total = jnp.zeros((8, 128), F32)
        for kg in range(rg + 1):
            e = jnp.exp2(scores[rg % 2, kg] - top)
            scores[rg % 2, kg] = e
            total = total + jnp.sum(e.reshape(64, 8, 128), axis=0)
        inverse = 1.0 / jnp.sum(total, axis=0, keepdims=True)
        acc = jnp.zeros((128, 256), F32)
        for kg in range(rg + 1):
            p = scores[rg % 2, kg] * inverse
            p2 = jnp.concatenate(split(p), axis=1)
            probs[kg, :, lanes] = p2
            scores[rg % 2, kg] = p
            acc = acc + nn(values_t[kg], p2)
        o_t = acc[:, :128] + acc[:, 128:]
        row_delta = jnp.sum(nt(identity, g) * o_t.astype(BF16).astype(F32), axis=0, keepdims=True)
        o_rows[4 * rg : 4 * rg + 4] = o_t.T.reshape(4, 4, 8, 128).astype(BF16)
        acc = jnp.zeros((128, 256), F32)
        for kg in range(rg + 1):
            ds = scores[rg % 2, kg] * (nt(plane_group(1, kg), g) - row_delta)
            ds2 = jnp.concatenate(split(ds), axis=1)
            dscores[kg, :, lanes] = ds2
            acc = acc + nn(keys_t[kg], ds2)
        dq_t = (acc[:, :128] + acc[:, 128:]) * scale
        dq_rows[4 * rg : 4 * rg + 4] = dq_t.T.reshape(4, 4, 8, 128).astype(BF16)

    with jax.named_scope("p9_rg01"):
        for kg in range(4):
            keys_t[kg] = nt(identity, plane_group(0, kg)).astype(BF16)
            values_t[kg] = nt(identity, plane_group(1, kg)).astype(BF16)
        block_of(0)
        block_of(1)
    loop(0, 8, lambda t: (o_start(t), dq_start(t)))
    with jax.named_scope("p9_rg23"):
        block_of(2)
        block_of(3)
    loop(8, 16, lambda t: (o_start(t), dq_start(t)))

    along = jnp.where(c == 0, x, y)
    across = jnp.where(c == 0, y, x)

    def sibling(kg):
        return pltpu.make_async_remote_copy(
            src_ref=part.at[1 - c, kg], dst_ref=other.at[kg], send_sem=sib_s.at[kg],
            recv_sem=sib_r.at[kg], device_id=(z, y, x, 1 - c), device_id_type=MESH,
        )

    def row_send(kg, a):
        t = (along + a) & 3
        return pltpu.make_async_remote_copy(
            src_ref=part.at[c, kg, :, t], dst_ref=row_in.at[a, kg], send_sem=row_s.at[kg, a],
            recv_sem=row_r.at[kg, a],
            device_id=(z, jnp.where(c == 0, y, t), jnp.where(c == 0, t, x), c), device_id_type=MESH,
        )

    def block_send(kg, a):
        t = (across + a) & 3
        return pltpu.make_async_remote_copy(
            src_ref=row_sum.at[kg, :, t], dst_ref=block_in.at[a, kg], send_sem=blk_s.at[kg, a],
            recv_sem=blk_r.at[kg, a],
            device_id=(z, jnp.where(c == 0, t, y), jnp.where(c == 0, x, t), c), device_id_type=MESH,
        )

    def combine(kg):
        sibling(kg).wait_recv()
        part[c, kg] = part[c, kg] + other[kg]
        loop(1, 4, lambda a: row_send(kg, a).start())

    with jax.named_scope("pa_dkv"):
        for kg in range(4):
            dk = nn(dscores[kg, :, 256 * kg :], q_twice[256 * kg :])
            dv = nn(probs[kg, :, 256 * kg :], g_twice[256 * kg :])
            part[0, kg] = jnp.swapaxes(dk.reshape(4, 4, 4, 8, 128), 1, 2)
            part[1, kg] = dv.reshape(4, 4, 4, 8, 128)
            sibling(kg).start()
            if kg:
                combine(kg - 1)

    with jax.named_scope("pb_combine"):
        combine(3)

    def row_finish(kg):
        total = part[c, kg, :, along]
        for a in range(1, 4):
            row_send(kg, a).wait_recv()
            total = total + row_in[a, kg]
        row_sum[kg] = total
        loop(1, 4, lambda a: block_send(kg, a).start())

    factor = jnp.where(c == 0, scale, 1.0).astype(F32)

    def finish(kg):
        total = row_sum[kg, :, across]
        for a in range(1, 4):
            block_send(kg, a).wait_recv()
            total = total + block_in[a, kg]
        final[pl.ds(4 * kg, 4)] = (total * factor).astype(BF16)

    with jax.named_scope("pc_rows"):
        loop(0, 4, row_finish)
    with jax.named_scope("pc_blocks"):
        loop(0, 4, finish)

    def out(d, core):
        t = z_at(d)
        return pltpu.make_async_remote_copy(
            src_ref=final.at[t], dst_ref=dkv_ref.at[c, z], send_sem=fin_s.at[d, core],
            recv_sem=fin_r.at[d, c], device_id=(t, y, x, core), device_id_type=MESH,
        )

    def into(d, core):
        t = z_at(d)
        return pltpu.make_async_remote_copy(
            src_ref=final.at[t], dst_ref=dkv_ref.at[c, z], send_sem=fin_s.at[d, core],
            recv_sem=fin_r.at[d, core], device_id=(t, y, x, c), device_id_type=MESH,
        )

    with jax.named_scope("pd_start"):
        dkv_ref[c, z] = final[z]
        out(0, 1 - c).start()
        loop(1, 16, lambda d: (out(d, c).start(), out(d, 1 - c).start()))

    with jax.named_scope("pe_sends"):
        own_kv.wait_send()
        loop(1, 16, lambda d: (to_core(0, d).wait_send(), to_core(1, d).wait_send()))
        loop(1, 16, lambda d: (zq(d).wait_send(), zg(d).wait_send()))
        for n in range(3):
            loop(1, 16, lambda e: gather(n, e).wait_send())
            loop(0, 16, lambda e: forward(n, e).wait_send())
        loop(0, 16, lambda t: (o_finish(t), dq_finish(t)))
        loop(0, 4, lambda kg: sibling(kg).wait_send())
        loop(0, 4, lambda kg: loop(1, 4, lambda a: (row_send(kg, a).wait_send(), block_send(kg, a).wait_send())))
    with jax.named_scope("pf_dkv"):
        out(0, 1 - c).wait_send()
        into(0, 1 - c).wait_recv()
        loop(1, 16, lambda d: (out(d, c).wait_send(), out(d, 1 - c).wait_send()))
        loop(1, 16, lambda d: (into(d, c).wait_recv(), into(d, 1 - c).wait_recv()))


def on_device(q, k, v, g):
    core = lax.axis_index("c")
    wide = (2, 4, 8, 8, 128)
    dma = pltpu.SemaphoreType.DMA
    hbm = pl.BlockSpec(memory_space=pltpu.MemorySpace.HBM)
    vmem = pl.BlockSpec(memory_space=pltpu.VMEM)
    o, dq, dkv = pl.pallas_call(
        kernel,
        out_shape=(
            jax.ShapeDtypeStruct(wide, BF16),
            jax.ShapeDtypeStruct(wide, BF16),
            jax.ShapeDtypeStruct((2, 16, 8, 128), BF16),
        ),
        in_specs=[hbm, hbm, hbm, hbm],
        out_specs=(hbm, hbm, vmem),
        scratch_shapes=[
            pltpu.VMEM(wide, BF16),
            pltpu.VMEM((2, 4, 8, 128), BF16),
            pltpu.VMEM((2, 4, 8, 128), BF16),
            pltpu.VMEM(wide, BF16),
            pltpu.VMEM((2, 8, 8, 128), F32),
            pltpu.VMEM((2, 8, 8, 128), BF16),
            pltpu.VMEM((16, 4, 8, 128), BF16),
            pltpu.VMEM((16, 4, 8, 128), BF16),
            pltpu.VMEM((2, 16, 16, 8, 128), BF16),
            pltpu.VMEM((8, 128), BF16),
            pltpu.VMEM((4, 128, 512), BF16),
            pltpu.VMEM((4, 128, 512), BF16),
            pltpu.VMEM((512, 128), jnp.int32),
            pltpu.VMEM((2, 4, 512, 128), F32),
            pltpu.VMEM((4, 512, 1024), BF16),
            pltpu.VMEM((4, 512, 1024), BF16),
            pltpu.VMEM((1024, 128), BF16),
            pltpu.VMEM((1024, 128), BF16),
            pltpu.VMEM((16, 4, 8, 128), BF16),
            pltpu.VMEM((16, 4, 8, 128), BF16),
            pltpu.VMEM((2, 4, 4, 4, 4, 8, 128), F32),
            pltpu.VMEM((4, 4, 4, 4, 8, 128), F32),
            pltpu.VMEM((4, 4, 4, 4, 8, 128), F32),
            pltpu.VMEM((4, 4, 4, 8, 128), F32),
            pltpu.VMEM((4, 4, 4, 8, 128), F32),
            pltpu.VMEM((16, 8, 128), BF16),
            dma((6,)),
            dma((2, 16)), dma((2, 16)), dma((16,)), dma((16,)), dma((16,)), dma((16,)),
            dma((3, 16)), dma((3, 16)), dma((3, 16)), dma((3, 16)),
            dma((16,)), dma((16,)), dma((16,)), dma((16,)),
            dma((4,)), dma((4,)), dma((4, 4)), dma((4, 4)), dma((4, 4)), dma((4, 4)), dma((16, 2)), dma((16, 2)),
        ],
        compiler_params=pltpu.CompilerParams(
            collective_id=1, has_side_effects=True, vmem_limit_bytes=67043328
        ),
        name="attend",
    )(q.reshape(wide), k, v, g.reshape(wide))
    dkv = lax.dynamic_slice_in_dim(dkv.reshape(2, 2, 8, 8, 128), 4 * core, 4, 3)
    dkv = dkv.transpose(0, 1, 3, 2, 4)
    return o.reshape(q.shape), dq.reshape(q.shape), dkv[0], dkv[1]


def solution(mesh):
    grid = Mesh(mesh.devices.reshape(NZ, NY, NX, 2), ("z", "y", "x", "c"))
    spec = P(None, ("z", "y", "x", "c"), None, None)
    return jax.shard_map(
        on_device, mesh=grid, in_specs=(spec,) * 4, out_specs=(spec,) * 4, check_vma=False
    )
```

```python
import functools

import jax
import jax.numpy as jnp
from jax import lax
from jax.experimental import pallas as pl
from jax.experimental.pallas import tpu as pltpu
from jax.sharding import Mesh
from jax.sharding import PartitionSpec as P

MESH = pl.DeviceIdType.MESH
F32 = jnp.float32
BF16 = jnp.bfloat16
NZ, NY, NX = 16, 4, 4
MASKED = -1e30


def nt(a, b):
    return lax.dot_general(a, b, (((1,), (1,)), ((), ())), preferred_element_type=F32)


def nn(a, b):
    return lax.dot_general(a, b, (((1,), (0,)), ((), ())), preferred_element_type=F32)


def split(a):
    high = a.astype(BF16)
    return high, (a - high.astype(F32)).astype(BF16)


def kernel(
    q_hbm, k_hbm, v_hbm, g_hbm, o_hbm, dq_hbm, dkv_ref,
    q_home, k_home, v_home, g_home, kv_wide, kv_home, q_rows, g_rows, kv_all,
    mate, keys_t, values_t, diagonal, scores, probs, dscores, g_twice, q_twice,
    o_rows, dq_rows, part, other, row_in, row_sum, block_in, final,
    in_sem, zkv_s, zkv_r, own_s, own_r, zq_s, zq_r, zg_s, zg_r, ag_s, ag_r, fw_s, fw_r,
    o_s, o_r, own_o, dq_s, dq_r, own_dq, sib_s, sib_r, row_s, row_r, blk_s, blk_r, fin_s, fin_r,
):
    z, y, x, c = (lax.axis_index(a) for a in ("z", "y", "x", "c"))
    chip = y * NX + x
    layer, group = z >> 3, z & 7
    scale = 128 ** -0.5

    def z_at(d):
        return (z + d) & 15

    def chip_at(e, sign):
        dy, dx = e >> 2, e & 3
        return (y + 4 + sign * dy) & 3, (x + 4 + sign * dx) & 3

    barrier = pltpu.get_barrier_semaphore()

    def greet(*device):
        pl.semaphore_signal(barrier, inc=1, device_id=device, device_id_type=MESH)

    for d in (8, 7, 9, 6, 10, 5, 11, 4, 12, 3, 13, 2, 14, 1, 15):
        greet(z_at(d), y, x, c)
        greet(z_at(d), y, x, 1 - c)
    for e in (10, 6, 9, 11, 14, 2, 8, 5, 7, 13, 15, 1, 3, 4, 12):
        greet(z, *chip_at(e, 1), c)
    greet(z, y, x, 1 - c)

    stage = [
        pltpu.make_async_copy(k_hbm, k_home, in_sem.at[0]),
        pltpu.make_async_copy(v_hbm, v_home, in_sem.at[1]),
        pltpu.make_async_copy(q_hbm, q_home, in_sem.at[2]),
        pltpu.make_async_copy(g_hbm, g_home, in_sem.at[3]),
        pltpu.make_async_copy(q_hbm.at[layer, :, group], q_rows.at[z], in_sem.at[4]),
        pltpu.make_async_copy(g_hbm.at[layer, :, group], g_rows.at[z], in_sem.at[5]),
    ]
    for copy in stage:
        copy.start()

    def drain(ref, sem):
        pltpu.make_async_remote_copy(
            src_ref=ref, dst_ref=ref, send_sem=sem, recv_sem=sem,
            device_id=(z, y, x, 1 - c), device_id_type=MESH,
        ).wait_recv()

    key_pos = lax.broadcasted_iota(jnp.int32, (512, 128), 0)
    lane = lax.broadcasted_iota(jnp.int32, (512, 128), 1)
    row_pos = 128 * (lane >> 5) + ((lane >> 3) & 3) + 8 * chip + 4 * c
    diagonal[...] = key_pos - row_pos
    identity = (
        lax.broadcasted_iota(jnp.int32, (128, 128), 0)
        == lax.broadcasted_iota(jnp.int32, (128, 128), 1)
    ).astype(F32).astype(BF16)

    with jax.named_scope("p0_kv"):
        stage[0].wait()
        stage[1].wait()
        for l in range(2):
            for i in range(4):
                kv_wide[l, :, i, :] = k_home[l, i].astype(F32)
                kv_wide[l, :, 4 + i, :] = v_home[l, i].astype(F32)
        kv_home[...] = kv_wide[...].astype(BF16)
        for copy in stage[2:]:
            copy.wait()
    with jax.named_scope("p1_barrier"):
        pl.semaphore_wait(barrier, 46)

    def to_z(src, dst, send, recv):
        def make(d):
            t = z_at(d)
            return pltpu.make_async_remote_copy(
                src_ref=src.at[t >> 3, :, t & 7], dst_ref=dst.at[z], send_sem=send,
                recv_sem=recv, device_id=(t, y, x, c), device_id_type=MESH,
            )
        return make

    half = pl.ds(pl.multiple_of(4 * c, 4), 4)

    def to_core(core, d, far):
        t = z_at(d)
        return pltpu.make_async_remote_copy(
            src_ref=kv_home.at[t >> 3, t & 7, pl.ds(4 * core, 4)],
            dst_ref=kv_all.at[core, (20 - d) & 15, chip, half],
            send_sem=zkv_s, recv_sem=zkv_r.at[far],
            device_id=(t, y, x, core), device_id_type=MESH,
        )

    own_kv = pltpu.make_async_remote_copy(
        src_ref=kv_home.at[layer, group], dst_ref=mate, send_sem=own_s,
        recv_sem=own_r, device_id=(z, y, x, 1 - c), device_id_type=MESH,
    )
    zq = to_z(q_home, q_rows, zq_s, zq_r)
    zg = to_z(g_home, g_rows, zg_s, zg_r)

    def loop(low, high, body):
        def step(i, _):
            body(i)
            return 0
        lax.fori_loop(low, high, step, 0)

    with jax.named_scope("p2_zstart"):
        own_kv.start()
        def send_kv(d, far):
            to_core(0, d, far).start()
            to_core(1, d, far).start()

        loop(5, 12, lambda d: send_kv(d, 1))
        loop(1, 5, lambda d: send_kv(d, 0))
        loop(12, 16, lambda d: send_kv(d, 0))
        loop(1, 16, lambda d: zq(d).start())
        loop(1, 16, lambda d: zg(d).start())

    PIECES = (pl.ds(0, 9), pl.ds(9, 7))

    def gather(n, e):
        block = kv_all.at[c, PIECES[n], chip]
        return pltpu.make_async_remote_copy(
            src_ref=block, dst_ref=block, send_sem=ag_s,
            recv_sem=ag_r.at[n, e], device_id=(z, *chip_at(e, 1), c), device_id_type=MESH,
        )

    def forward(n, e):
        yy, xx = chip_at(e, -1)
        block = kv_all.at[c, PIECES[n], yy * NX + xx]
        return pltpu.make_async_remote_copy(
            src_ref=block, dst_ref=block, send_sem=fw_s,
            recv_sem=fw_r.at[n], device_id=(z, y, x, 1 - c), device_id_type=MESH,
        )

    with jax.named_scope("p3_zkvn"):
        own_kv.wait_recv()
        mine = kv_wide[layer, group]
        theirs = pltpu.roll(mate[...].astype(F32), 4, 0)
        low_half = (lax.broadcasted_iota(jnp.int32, (8, 128), 0) >> 2) == c
        kv_all[c, 4, chip] = jnp.where(low_half, mine, theirs).astype(BF16)
        drain(kv_home.at[0], zkv_r.at[0])
        loop(1, 16, lambda e: gather(0, e).start())
        forward(0, 0).start()
    with jax.named_scope("p3_zkvf"):
        drain(kv_home.at[0, pl.ds(0, 7)], zkv_r.at[1])
        loop(1, 16, lambda e: gather(1, e).start())
        forward(1, 0).start()

    def pass_on(n, e):
        gather(n, e).wait_recv()
        forward(n, e).start()

    with jax.named_scope("p4_agnear"):
        loop(1, 16, lambda e: pass_on(0, e))
    with jax.named_scope("p5_agfar"):
        loop(1, 16, lambda e: pass_on(1, e))
    with jax.named_scope("p6_fwd"):
        drain(kv_all.at[1 - c, PIECES[0]], fw_r.at[0])
        drain(kv_all.at[1 - c, PIECES[1]], fw_r.at[1])

    def plane_group(kind, kg):
        return jnp.concatenate(
            [kv_all[kind, (4 * kg + i + 20 - z) & 15].reshape(128, 128) for i in range(4)], axis=0
        )

    with jax.named_scope("p8_qwait"):
        drain(q_rows.at[pl.ds(0, 15)], zq_r)
        drain(g_rows.at[pl.ds(0, 15)], zg_r)

    def home(rows, out, send, recv, own_sem):
        def make(t):
            return pltpu.make_async_remote_copy(
                src_ref=rows.at[t], dst_ref=out.at[layer, :, group], send_sem=send,
                recv_sem=recv, device_id=(t, y, x, c), device_id_type=MESH,
            )
        own = pltpu.make_async_copy(rows.at[z], out.at[layer, :, group], own_sem)
        def start(t):
            @pl.when(t != z)
            def _():
                make(t).start()
            @pl.when(t == z)
            def _():
                own.start()
        def finish():
            drain(rows.at[pl.ds(0, 15)], send)
            drain(rows.at[pl.ds(0, 15)], recv)
            own.wait()
        return start, finish

    o_start, o_finish = home(o_rows, o_hbm, o_s, o_r, own_o)
    dq_start, dq_finish = home(dq_rows, dq_hbm, dq_s, dq_r, own_dq)

    factor_2 = scale * 1.4426950408889634

    def block_of(rg):
        q = q_rows[4 * rg : 4 * rg + 4].astype(F32).reshape(128, 128).astype(BF16)
        g = g_rows[4 * rg : 4 * rg + 4].astype(F32).reshape(128, 128).astype(BF16)
        for twice, value in ((q_twice, q), (g_twice, g)):
            twice[256 * rg : 256 * rg + 128] = value
            twice[256 * rg + 128 : 256 * rg + 256] = value
        lanes = slice(256 * rg, 256 * rg + 256)
        top = jnp.full((8, 128), MASKED, F32)
        for kg in range(rg + 1):
            s = nt(plane_group(0, kg), q) * factor_2
            if kg == rg:
                s = jnp.where(diagonal[...] <= 0, s, MASKED)
            scores[rg % 2, kg] = s
            top = jnp.maximum(top, jnp.max(s.reshape(64, 8, 128), axis=0))
        top = jnp.max(top, axis=0, keepdims=True)
        total = jnp.zeros((8, 128), F32)
        for kg in range(rg + 1):
            e = jnp.exp2(scores[rg % 2, kg] - top)
            scores[rg % 2, kg] = e
            total = total + jnp.sum(e.reshape(64, 8, 128), axis=0)
        inverse = 1.0 / jnp.sum(total, axis=0, keepdims=True)
        acc = jnp.zeros((128, 256), F32)
        for kg in range(rg + 1):
            p = scores[rg % 2, kg] * inverse
            p2 = jnp.concatenate(split(p), axis=1)
            probs[kg, :, lanes] = p2
            scores[rg % 2, kg] = p
            acc = acc + nn(values_t[kg], p2)
        o_t = acc[:, :128] + acc[:, 128:]
        row_delta = jnp.sum(nt(identity, g) * o_t.astype(BF16).astype(F32), axis=0, keepdims=True)
        o_rows[4 * rg : 4 * rg + 4] = o_t.T.reshape(4, 4, 8, 128).astype(BF16)
        acc = jnp.zeros((128, 256), F32)
        for kg in range(rg + 1):
            ds = scores[rg % 2, kg] * (nt(plane_group(1, kg), g) - row_delta)
            ds2 = jnp.concatenate(split(ds), axis=1)
            dscores[kg, :, lanes] = ds2
            acc = acc + nn(keys_t[kg], ds2)
        dq_t = (acc[:, :128] + acc[:, 128:]) * scale
        dq_rows[4 * rg : 4 * rg + 4] = dq_t.T.reshape(4, 4, 8, 128).astype(BF16)

    along = jnp.where(c == 0, x, y)
    across = jnp.where(c == 0, y, x)

    def sibling(kg):
        return pltpu.make_async_remote_copy(
            src_ref=part.at[1 - c, kg], dst_ref=other.at[kg], send_sem=sib_s,
            recv_sem=sib_r.at[kg], device_id=(z, y, x, 1 - c), device_id_type=MESH,
        )

    def row_send(kg, a):
        t = (along + a) & 3
        return pltpu.make_async_remote_copy(
            src_ref=part.at[c, kg, :, t], dst_ref=row_in.at[kg, a - 1], send_sem=row_s,
            recv_sem=row_r.at[kg],
            device_id=(z, jnp.where(c == 0, y, t), jnp.where(c == 0, t, x), c), device_id_type=MESH,
        )

    def block_send(kg, a):
        t = (across + a) & 3
        return pltpu.make_async_remote_copy(
            src_ref=row_sum.at[kg, :, t], dst_ref=block_in.at[kg, a - 1], send_sem=blk_s,
            recv_sem=blk_r.at[kg],
            device_id=(z, jnp.where(c == 0, t, y), jnp.where(c == 0, x, t), c), device_id_type=MESH,
        )

    def combine(kg):
        sibling(kg).wait_recv()
        part[c, kg] = part[c, kg] + other[kg]
        loop(1, 4, lambda a: row_send(kg, a).start())

    with jax.named_scope("p9_trans"):
        for kg in range(4):
            keys_t[kg] = nt(identity, plane_group(0, kg)).astype(BF16)
            values_t[kg] = nt(identity, plane_group(1, kg)).astype(BF16)
    for rg in (3, 2, 1, 0):
        with jax.named_scope(f"p9_rg{rg}"):
            block_of(rg)
            dk = nn(dscores[rg, :, 256 * rg :], q_twice[256 * rg :])
            dv = nn(probs[rg, :, 256 * rg :], g_twice[256 * rg :])
            part[0, rg] = jnp.swapaxes(dk.reshape(4, 4, 4, 8, 128), 1, 2)
            part[1, rg] = dv.reshape(4, 4, 4, 8, 128)
            sibling(rg).start()
        with jax.named_scope(f"pa_comb{rg}"):
            if rg < 3:
                combine(rg + 1)
            loop(4 * rg, 4 * rg + 4, lambda t: (o_start(t), dq_start(t)))

    with jax.named_scope("pb_combine"):
        combine(0)

    def row_finish(i):
        kg = 3 - i
        drain(row_in.at[kg], row_r.at[kg])
        total = part[c, kg, :, along]
        for a in range(3):
            total = total + row_in[kg, a]
        row_sum[kg] = total
        loop(1, 4, lambda a: block_send(kg, a).start())

    factor = jnp.where(c == 0, scale, 1.0).astype(F32)

    def finish(i):
        kg = 3 - i
        drain(block_in.at[kg], blk_r.at[kg])
        total = row_sum[kg, :, across]
        for a in range(3):
            total = total + block_in[kg, a]
        final[pl.ds(4 * kg, 4)] = (total * factor).astype(BF16)

    with jax.named_scope("pc_rows"):
        loop(0, 4, row_finish)
    with jax.named_scope("pc_blocks"):
        loop(0, 4, finish)

    def out(d, other_core):
        t = z_at(d)
        core = 1 - c if other_core else c
        return pltpu.make_async_remote_copy(
            src_ref=final.at[t], dst_ref=dkv_ref.at[c, z], send_sem=fin_s.at[other_core],
            recv_sem=fin_r.at[other_core], device_id=(t, y, x, core), device_id_type=MESH,
        )

    with jax.named_scope("pd_start"):
        loop(1, 16, lambda d: (out(d, 0).start(), out(d, 1).start()))
        out(0, 1).start()
        dkv_ref[c, z] = final[z]

    with jax.named_scope("pe_sends"):
        own_kv.wait_send()
        drain(kv_all.at[0, 0, pl.ds(0, 15)], zkv_s)
        drain(q_rows.at[pl.ds(0, 15)], zq_s)
        drain(g_rows.at[pl.ds(0, 15)], zg_s)
        drain(kv_all.at[0, :, pl.ds(0, 15)], ag_s)
        drain(kv_all.at[0], fw_s)
        o_finish()
        dq_finish()
        drain(other, sib_s)
        drain(row_in, row_s)
        drain(block_in, blk_s)
    with jax.named_scope("pf_dkv"):
        drain(dkv_ref.at[0, pl.ds(0, 15)], fin_s.at[0])
        drain(dkv_ref.at[0], fin_s.at[1])
        drain(dkv_ref.at[0, pl.ds(0, 15)], fin_r.at[0])
        drain(dkv_ref.at[1], fin_r.at[1])


def on_device(q, k, v, g):
    core = lax.axis_index("c")
    wide = (2, 4, 8, 8, 128)
    dma = pltpu.SemaphoreType.DMA
    hbm = pl.BlockSpec(memory_space=pltpu.MemorySpace.HBM)
    vmem = pl.BlockSpec(memory_space=pltpu.VMEM)
    o, dq, dkv = pl.pallas_call(
        kernel,
        out_shape=(
            jax.ShapeDtypeStruct(wide, BF16),
            jax.ShapeDtypeStruct(wide, BF16),
            jax.ShapeDtypeStruct((2, 16, 8, 128), BF16),
        ),
        in_specs=[hbm, hbm, hbm, hbm],
        out_specs=(hbm, hbm, vmem),
        scratch_shapes=[
            pltpu.VMEM(wide, BF16),
            pltpu.VMEM((2, 4, 8, 128), BF16),
            pltpu.VMEM((2, 4, 8, 128), BF16),
            pltpu.VMEM(wide, BF16),
            pltpu.VMEM((2, 8, 8, 128), F32),
            pltpu.VMEM((2, 8, 8, 128), BF16),
            pltpu.VMEM((16, 4, 8, 128), BF16),
            pltpu.VMEM((16, 4, 8, 128), BF16),
            pltpu.VMEM((2, 16, 16, 8, 128), BF16),
            pltpu.VMEM((8, 128), BF16),
            pltpu.VMEM((4, 128, 512), BF16),
            pltpu.VMEM((4, 128, 512), BF16),
            pltpu.VMEM((512, 128), jnp.int32),
            pltpu.VMEM((2, 4, 512, 128), F32),
            pltpu.VMEM((4, 512, 1024), BF16),
            pltpu.VMEM((4, 512, 1024), BF16),
            pltpu.VMEM((1024, 128), BF16),
            pltpu.VMEM((1024, 128), BF16),
            pltpu.VMEM((16, 4, 8, 128), BF16),
            pltpu.VMEM((16, 4, 8, 128), BF16),
            pltpu.VMEM((2, 4, 4, 4, 4, 8, 128), F32),
            pltpu.VMEM((4, 4, 4, 4, 8, 128), F32),
            pltpu.VMEM((4, 3, 4, 4, 8, 128), F32),
            pltpu.VMEM((4, 4, 4, 8, 128), F32),
            pltpu.VMEM((4, 3, 4, 8, 128), F32),
            pltpu.VMEM((16, 8, 128), BF16),
            dma((6,)),
            dma, dma((2,)), dma, dma, dma, dma, dma, dma,
            dma, dma((2, 16)), dma, dma((2,)),
            dma, dma, dma, dma, dma, dma,
            dma, dma((4,)), dma, dma((4,)), dma, dma((4,)), dma((2,)), dma((2,)),
        ],
        compiler_params=pltpu.CompilerParams(
            collective_id=1, has_side_effects=True, vmem_limit_bytes=67043328
        ),
        name="attend",
    )(q.reshape(wide), k, v, g.reshape(wide))
    dkv = lax.dynamic_slice_in_dim(dkv.reshape(2, 2, 8, 8, 128), 4 * core, 4, 3)
    dkv = dkv.transpose(0, 1, 3, 2, 4)
    return o.reshape(q.shape), dq.reshape(q.shape), dkv[0], dkv[1]


def solution(mesh):
    grid = Mesh(mesh.devices.reshape(NZ, NY, NX, 2), ("z", "y", "x", "c"))
    spec = P(None, ("z", "y", "x", "c"), None, None)
    return jax.shard_map(
        on_device, mesh=grid, in_specs=(spec,) * 4, out_specs=(spec,) * 4, check_vma=False
    )
```

```python
import functools

import jax
import jax.numpy as jnp
from jax import lax
from jax.experimental import pallas as pl
from jax.experimental.pallas import tpu as pltpu
from jax.sharding import Mesh
from jax.sharding import PartitionSpec as P

MESH = pl.DeviceIdType.MESH
F32 = jnp.float32
BF16 = jnp.bfloat16
NZ, NY, NX = 16, 4, 4
MASKED = -1e30


def nt(a, b):
    return lax.dot_general(a, b, (((1,), (1,)), ((), ())), preferred_element_type=F32)


def nn(a, b):
    return lax.dot_general(a, b, (((1,), (0,)), ((), ())), preferred_element_type=F32)


def split(a):
    high = a.astype(BF16)
    return high, (a - high.astype(F32)).astype(BF16)


def kernel(
    q_hbm, k_hbm, v_hbm, g_hbm, o_hbm, dq_hbm, dkv_ref,
    q_home, k_home, v_home, g_home, kv_wide, kv_home, q_rows, g_rows, kv_all,
    mate, keys_t, values_t, diagonal, row_delta, scores, probs, dscores, g_twice, q_twice,
    o_rows, dq_rows, part, other, row_in, row_sum, block_in, final,
    in_sem, zkv_s, zkv_r, own_s, own_r, zq_s, zq_r, zg_s, zg_r, ag_s, ag_r, fw_s, fw_r,
    o_s, o_r, own_o, dq_s, dq_r, own_dq, sib_s, sib_r, row_s, row_r, blk_s, blk_r, fin_s, fin_r,
):
    z, y, x, c = (lax.axis_index(a) for a in ("z", "y", "x", "c"))
    chip = y * NX + x
    layer, group = z >> 3, z & 7
    scale = 128 ** -0.5

    def z_at(d):
        return (z + d) & 15

    def chip_at(e, sign):
        dy, dx = e >> 2, e & 3
        return (y + 4 + sign * dy) & 3, (x + 4 + sign * dx) & 3

    barrier = pltpu.get_barrier_semaphore()

    def greet(*device):
        pl.semaphore_signal(barrier, inc=1, device_id=device, device_id_type=MESH)

    for d in (8, 7, 9, 6, 10, 5, 11, 4, 12, 3, 13, 2, 14, 1, 15):
        greet(z_at(d), y, x, c)
        greet(z_at(d), y, x, 1 - c)
    for e in (10, 6, 9, 11, 14, 2, 8, 5, 7, 13, 15, 1, 3, 4, 12):
        greet(z, *chip_at(e, 1), c)
    greet(z, y, x, 1 - c)

    stage = [
        pltpu.make_async_copy(k_hbm, k_home, in_sem.at[0]),
        pltpu.make_async_copy(v_hbm, v_home, in_sem.at[1]),
        pltpu.make_async_copy(q_hbm, q_home, in_sem.at[2]),
        pltpu.make_async_copy(g_hbm, g_home, in_sem.at[3]),
        pltpu.make_async_copy(q_hbm.at[layer, :, group], q_rows.at[z], in_sem.at[4]),
        pltpu.make_async_copy(g_hbm.at[layer, :, group], g_rows.at[z], in_sem.at[5]),
    ]
    for copy in stage:
        copy.start()

    def drain(ref, sem):
        pltpu.make_async_remote_copy(
            src_ref=ref, dst_ref=ref, send_sem=sem, recv_sem=sem,
            device_id=(z, y, x, 1 - c), device_id_type=MESH,
        ).wait_recv()

    key_pos = lax.broadcasted_iota(jnp.int32, (512, 128), 0)
    lane = lax.broadcasted_iota(jnp.int32, (512, 128), 1)
    row_pos = 128 * (lane >> 5) + ((lane >> 3) & 3) + 8 * chip + 4 * c
    diagonal[...] = key_pos - row_pos
    identity = (
        lax.broadcasted_iota(jnp.int32, (128, 128), 0)
        == lax.broadcasted_iota(jnp.int32, (128, 128), 1)
    ).astype(F32).astype(BF16)

    with jax.named_scope("p0_kv"):
        stage[0].wait()
        stage[1].wait()
        for l in range(2):
            for i in range(4):
                kv_wide[l, :, i, :] = k_home[l, i].astype(F32)
                kv_wide[l, :, 4 + i, :] = v_home[l, i].astype(F32)
        kv_home[...] = kv_wide[...].astype(BF16)
        for copy in stage[2:]:
            copy.wait()
    with jax.named_scope("p1_barrier"):
        pl.semaphore_wait(barrier, 46)

    def to_z(src, dst, send, recv):
        def make(d):
            t = z_at(d)
            return pltpu.make_async_remote_copy(
                src_ref=src.at[t >> 3, :, t & 7], dst_ref=dst.at[z], send_sem=send,
                recv_sem=recv, device_id=(t, y, x, c), device_id_type=MESH,
            )
        return make

    half = pl.ds(pl.multiple_of(4 * c, 4), 4)

    def to_core(core, d, far):
        t = z_at(d)
        return pltpu.make_async_remote_copy(
            src_ref=kv_home.at[t >> 3, t & 7, pl.ds(4 * core, 4)],
            dst_ref=kv_all.at[core, (20 - d) & 15, chip, half],
            send_sem=zkv_s, recv_sem=zkv_r.at[far],
            device_id=(t, y, x, core), device_id_type=MESH,
        )

    own_kv = pltpu.make_async_remote_copy(
        src_ref=kv_home.at[layer, group], dst_ref=mate, send_sem=own_s,
        recv_sem=own_r, device_id=(z, y, x, 1 - c), device_id_type=MESH,
    )
    zq = to_z(q_home, q_rows, zq_s, zq_r)
    zg = to_z(g_home, g_rows, zg_s, zg_r)

    def loop(low, high, body):
        def step(i, _):
            body(i)
            return 0
        lax.fori_loop(low, high, step, 0)

    with jax.named_scope("p2_zstart"):
        own_kv.start()
        def send_kv(d, far):
            to_core(0, d, far).start()
            to_core(1, d, far).start()

        loop(1, 5, lambda d: (send_kv(d, 0), send_kv(16 - d, 0)))
        loop(5, 12, lambda d: send_kv(d, 1))
        loop(1, 16, lambda d: zq(d).start())
        loop(1, 16, lambda d: zg(d).start())

    PIECES = (pl.ds(0, 9), pl.ds(9, 7))

    def gather(n, e):
        block = kv_all.at[c, PIECES[n], chip]
        return pltpu.make_async_remote_copy(
            src_ref=block, dst_ref=block, send_sem=ag_s,
            recv_sem=ag_r.at[n, e], device_id=(z, *chip_at(e, 1), c), device_id_type=MESH,
        )

    def forward(n, e):
        yy, xx = chip_at(e, -1)
        block = kv_all.at[c, PIECES[n], yy * NX + xx]
        return pltpu.make_async_remote_copy(
            src_ref=block, dst_ref=block, send_sem=fw_s,
            recv_sem=fw_r.at[n], device_id=(z, y, x, 1 - c), device_id_type=MESH,
        )

    with jax.named_scope("p3_zkvn"):
        own_kv.wait_recv()
        mine = kv_wide[layer, group]
        theirs = pltpu.roll(mate[...].astype(F32), 4, 0)
        low_half = (lax.broadcasted_iota(jnp.int32, (8, 128), 0) >> 2) == c
        kv_all[c, 4, chip] = jnp.where(low_half, mine, theirs).astype(BF16)
        drain(kv_home.at[0], zkv_r.at[0])
        loop(1, 16, lambda e: gather(0, e).start())
        forward(0, 0).start()
    with jax.named_scope("p3_zkvf"):
        drain(kv_home.at[0, pl.ds(0, 7)], zkv_r.at[1])
        loop(1, 16, lambda e: gather(1, e).start())
        forward(1, 0).start()

    def pass_on(n, e):
        gather(n, e).wait_recv()
        forward(n, e).start()

    with jax.named_scope("p4_agnear"):
        loop(1, 16, lambda e: pass_on(0, e))
    with jax.named_scope("p5_agfar"):
        loop(1, 16, lambda e: pass_on(1, e))
    with jax.named_scope("p6_fwd"):
        drain(kv_all.at[1 - c, PIECES[0]], fw_r.at[0])
        drain(kv_all.at[1 - c, PIECES[1]], fw_r.at[1])

    def plane_group(kind, kg):
        return jnp.concatenate(
            [kv_all[kind, (4 * kg + i + 20 - z) & 15].reshape(128, 128) for i in range(4)], axis=0
        )

    with jax.named_scope("p8_qwait"):
        drain(q_rows.at[pl.ds(0, 15)], zq_r)
        drain(g_rows.at[pl.ds(0, 15)], zg_r)

    def home(rows, out, send, recv, own_sem):
        def make(t):
            return pltpu.make_async_remote_copy(
                src_ref=rows.at[t], dst_ref=out.at[layer, :, group], send_sem=send,
                recv_sem=recv, device_id=(t, y, x, c), device_id_type=MESH,
            )
        own = pltpu.make_async_copy(rows.at[z], out.at[layer, :, group], own_sem)
        def start():
            loop(1, 16, lambda d: make(z_at(d)).start())
            own.start()
        def finish():
            drain(rows.at[pl.ds(0, 15)], send)
            drain(rows.at[pl.ds(0, 15)], recv)
            own.wait()
        return start, finish

    o_start, o_finish = home(o_rows, o_hbm, o_s, o_r, own_o)
    dq_start, dq_finish = home(dq_rows, dq_hbm, dq_s, dq_r, own_dq)

    factor_2 = scale * 1.4426950408889634

    def pair(rg):
        return slice(256 * rg, 256 * rg + 128), slice(256 * rg, 256 * rg + 256)

    def forward_of(rg):
        first, lanes = pair(rg)
        q = q_rows[4 * rg : 4 * rg + 4].astype(F32).reshape(128, 128).astype(BF16)
        g = g_rows[4 * rg : 4 * rg + 4].astype(F32).reshape(128, 128).astype(BF16)
        q_twice[lanes] = jnp.concatenate([q, q], axis=0)
        g_twice[lanes] = jnp.concatenate([g, g], axis=0)
        top = jnp.full((8, 128), MASKED, F32)
        for kg in range(rg + 1):
            s = nt(plane_group(0, kg), q) * factor_2
            if kg == rg:
                s = jnp.where(diagonal[...] <= 0, s, MASKED)
            scores[rg, kg] = s
            top = jnp.maximum(top, jnp.max(s.reshape(64, 8, 128), axis=0))
        top = jnp.max(top, axis=0, keepdims=True)
        total = jnp.zeros((8, 128), F32)
        for kg in range(rg + 1):
            e = jnp.exp2(scores[rg, kg] - top)
            scores[rg, kg] = e
            total = total + jnp.sum(e.reshape(64, 8, 128), axis=0)
        inverse = 1.0 / jnp.sum(total, axis=0, keepdims=True)
        acc = jnp.zeros((128, 256), F32)
        for kg in range(rg + 1):
            p = scores[rg, kg] * inverse
            p2 = jnp.concatenate(split(p), axis=1)
            probs[kg, :, lanes] = p2
            scores[rg, kg] = p
            acc = acc + nn(values_t[kg], p2)
        o_t = acc[:, :128] + acc[:, 128:]
        delta = nt(identity, g) * o_t.astype(BF16).astype(F32)
        row_delta[rg : rg + 1] = jnp.sum(delta, axis=0, keepdims=True)
        o_rows[4 * rg : 4 * rg + 4] = o_t.T.reshape(4, 4, 8, 128).astype(BF16)

    def backward_of(rg):
        first, lanes = pair(rg)
        g = g_twice[first]
        delta = row_delta[rg : rg + 1]
        acc = jnp.zeros((128, 256), F32)
        for kg in range(rg + 1):
            ds = scores[rg, kg] * (nt(plane_group(1, kg), g) - delta)
            ds2 = jnp.concatenate(split(ds), axis=1)
            dscores[kg, :, lanes] = ds2
            acc = acc + nn(keys_t[kg], ds2)
        dq_t = (acc[:, :128] + acc[:, 128:]) * scale
        dq_rows[4 * rg : 4 * rg + 4] = dq_t.T.reshape(4, 4, 8, 128).astype(BF16)

    def value_sum(kg, low, high):
        lanes = slice(256 * low, 256 * high)
        return nn(probs[kg, :, lanes], g_twice[lanes]).reshape(4, 4, 4, 8, 128)

    def key_sum(kg, low, high):
        lanes = slice(256 * low, 256 * high)
        dk = nn(dscores[kg, :, lanes], q_twice[lanes])
        return jnp.swapaxes(dk.reshape(4, 4, 4, 8, 128), 1, 2)

    kind = 1 - c
    along = jnp.where(c == 0, y, x)
    across = jnp.where(c == 0, x, y)

    def sibling(kg):
        return pltpu.make_async_remote_copy(
            src_ref=part.at[c, kg], dst_ref=other.at[kg], send_sem=sib_s,
            recv_sem=sib_r.at[kg], device_id=(z, y, x, 1 - c), device_id_type=MESH,
        )

    def row_send(kg, a):
        t = (along + a) & 3
        return pltpu.make_async_remote_copy(
            src_ref=part.at[kind, kg, :, t], dst_ref=row_in.at[kg, a - 1], send_sem=row_s,
            recv_sem=row_r.at[kg],
            device_id=(z, jnp.where(c == 0, t, y), jnp.where(c == 0, x, t), c), device_id_type=MESH,
        )

    def block_send(kg, a):
        t = (across + a) & 3
        return pltpu.make_async_remote_copy(
            src_ref=row_sum.at[kg, :, t], dst_ref=block_in.at[kg, a - 1], send_sem=blk_s,
            recv_sem=blk_r.at[kg],
            device_id=(z, jnp.where(c == 0, y, t), jnp.where(c == 0, t, x), c), device_id_type=MESH,
        )

    def combine(kg):
        sibling(kg).wait_recv()
        part[kind, kg] = part[kind, kg] + other[kg]
        loop(1, 4, lambda a: row_send(kg, a).start())

    with jax.named_scope("p9_fwd"):
        for kg in range(4):
            keys_t[kg] = nt(identity, plane_group(0, kg)).astype(BF16)
            values_t[kg] = nt(identity, plane_group(1, kg)).astype(BF16)
        for rg in (3, 2, 1, 0):
            forward_of(rg)
            if rg < 3:
                part[1, rg + 1] = value_sum(rg + 1, rg + 1, 4)
        part[1, 0] = value_sum(0, 0, 4)

    def of_core(core, body):
        @pl.when(c == core)
        def _():
            body()

    with jax.named_scope("pa_osend"):
        of_core(1, lambda: loop(0, 4, lambda i: sibling(3 - i).start()))
        o_start()
    with jax.named_scope("p9_bwd3"):
        backward_of(3)
        part[0, 3] = key_sum(3, 3, 4)
    with jax.named_scope("pa_comb3"):
        of_core(0, lambda: (sibling(3).start(), loop(0, 4, lambda i: combine(3 - i))))
    with jax.named_scope("p9_bwd2"):
        backward_of(2)
        part[0, 2] = key_sum(2, 2, 4)
    with jax.named_scope("pa_comb2"):
        of_core(0, lambda: sibling(2).start())
        of_core(1, lambda: combine(3))
    with jax.named_scope("p9_bwd1"):
        backward_of(1)
        part[0, 1] = key_sum(1, 1, 4)
    with jax.named_scope("pa_comb1"):
        of_core(0, lambda: sibling(1).start())
        of_core(1, lambda: combine(2))
    with jax.named_scope("p9_bwd0"):
        backward_of(0)
        part[0, 0] = key_sum(0, 0, 4)
    with jax.named_scope("pa_comb0"):
        of_core(0, lambda: sibling(0).start())
        dq_start()
        of_core(1, lambda: (combine(1), combine(0)))

    def row_finish(i):
        kg = 3 - i
        drain(row_in.at[kg], row_r.at[kg])
        total = part[kind, kg, :, along]
        for a in range(3):
            total = total + row_in[kg, a]
        row_sum[kg] = total
        loop(1, 4, lambda a: block_send(kg, a).start())

    factor = jnp.where(c == 0, 1.0, scale).astype(F32)

    def finish(i):
        kg = 3 - i
        drain(block_in.at[kg], blk_r.at[kg])
        total = row_sum[kg, :, across]
        for a in range(3):
            total = total + block_in[kg, a]
        final[pl.ds(4 * kg, 4)] = (total * factor).astype(BF16)

    with jax.named_scope("pc_rows"):
        loop(0, 4, row_finish)
    with jax.named_scope("pc_blocks"):
        loop(0, 4, finish)

    def out(d, other_core):
        t = z_at(d)
        core = 1 - c if other_core else c
        return pltpu.make_async_remote_copy(
            src_ref=final.at[t], dst_ref=dkv_ref.at[kind, z], send_sem=fin_s.at[other_core],
            recv_sem=fin_r.at[other_core], device_id=(t, y, x, core), device_id_type=MESH,
        )

    with jax.named_scope("pd_start"):
        loop(1, 16, lambda d: (out(d, 0).start(), out(d, 1).start()))
        out(0, 1).start()
        dkv_ref[kind, z] = final[z]

    with jax.named_scope("pe_sends"):
        own_kv.wait_send()
        drain(kv_all.at[0, 0, pl.ds(0, 15)], zkv_s)
        drain(q_rows.at[pl.ds(0, 15)], zq_s)
        drain(g_rows.at[pl.ds(0, 15)], zg_s)
        drain(kv_all.at[0, :, pl.ds(0, 15)], ag_s)
        drain(kv_all.at[0], fw_s)
        o_finish()
        dq_finish()
        drain(other, sib_s)
        drain(row_in, row_s)
        drain(block_in, blk_s)
    with jax.named_scope("pf_dkv"):
        drain(dkv_ref.at[0, pl.ds(0, 15)], fin_s.at[0])
        drain(dkv_ref.at[0], fin_s.at[1])
        drain(dkv_ref.at[0, pl.ds(0, 15)], fin_r.at[0])
        drain(dkv_ref.at[1], fin_r.at[1])


def on_device(q, k, v, g):
    core = lax.axis_index("c")
    wide = (2, 4, 8, 8, 128)
    dma = pltpu.SemaphoreType.DMA
    hbm = pl.BlockSpec(memory_space=pltpu.MemorySpace.HBM)
    vmem = pl.BlockSpec(memory_space=pltpu.VMEM)
    o, dq, dkv = pl.pallas_call(
        kernel,
        out_shape=(
            jax.ShapeDtypeStruct(wide, BF16),
            jax.ShapeDtypeStruct(wide, BF16),
            jax.ShapeDtypeStruct((2, 16, 8, 128), BF16),
        ),
        in_specs=[hbm, hbm, hbm, hbm],
        out_specs=(hbm, hbm, vmem),
        scratch_shapes=[
            pltpu.VMEM(wide, BF16),
            pltpu.VMEM((2, 4, 8, 128), BF16),
            pltpu.VMEM((2, 4, 8, 128), BF16),
            pltpu.VMEM(wide, BF16),
            pltpu.VMEM((2, 8, 8, 128), F32),
            pltpu.VMEM((2, 8, 8, 128), BF16),
            pltpu.VMEM((16, 4, 8, 128), BF16),
            pltpu.VMEM((16, 4, 8, 128), BF16),
            pltpu.VMEM((2, 16, 16, 8, 128), BF16),
            pltpu.VMEM((8, 128), BF16),
            pltpu.VMEM((4, 128, 512), BF16),
            pltpu.VMEM((4, 128, 512), BF16),
            pltpu.VMEM((512, 128), jnp.int32),
            pltpu.VMEM((8, 128), F32),
            pltpu.VMEM((4, 4, 512, 128), F32),
            pltpu.VMEM((4, 512, 1024), BF16),
            pltpu.VMEM((4, 512, 1024), BF16),
            pltpu.VMEM((1024, 128), BF16),
            pltpu.VMEM((1024, 128), BF16),
            pltpu.VMEM((16, 4, 8, 128), BF16),
            pltpu.VMEM((16, 4, 8, 128), BF16),
            pltpu.VMEM((2, 4, 4, 4, 4, 8, 128), F32),
            pltpu.VMEM((4, 4, 4, 4, 8, 128), F32),
            pltpu.VMEM((4, 3, 4, 4, 8, 128), F32),
            pltpu.VMEM((4, 4, 4, 8, 128), F32),
            pltpu.VMEM((4, 3, 4, 8, 128), F32),
            pltpu.VMEM((16, 8, 128), BF16),
            dma((6,)),
            dma, dma((2,)), dma, dma, dma, dma, dma, dma,
            dma, dma((2, 16)), dma, dma((2,)),
            dma, dma, dma, dma, dma, dma,
            dma, dma((4,)), dma, dma((4,)), dma, dma((4,)), dma((2,)), dma((2,)),
        ],
        compiler_params=pltpu.CompilerParams(
            collective_id=1, has_side_effects=True, vmem_limit_bytes=67043328
        ),
        name="attend",
    )(q.reshape(wide), k, v, g.reshape(wide))
    dkv = lax.dynamic_slice_in_dim(dkv.reshape(2, 2, 8, 8, 128), 4 * core, 4, 3)
    dkv = dkv.transpose(0, 1, 3, 2, 4)
    return o.reshape(q.shape), dq.reshape(q.shape), dkv[0], dkv[1]


def solution(mesh):
    grid = Mesh(mesh.devices.reshape(NZ, NY, NX, 2), ("z", "y", "x", "c"))
    spec = P(None, ("z", "y", "x", "c"), None, None)
    return jax.shard_map(
        on_device, mesh=grid, in_specs=(spec,) * 4, out_specs=(spec,) * 4, check_vma=False
    )
```

```python
import functools

import jax
import jax.numpy as jnp
from jax import lax
from jax.experimental import pallas as pl
from jax.experimental.pallas import tpu as pltpu
from jax.sharding import Mesh
from jax.sharding import PartitionSpec as P

MESH = pl.DeviceIdType.MESH
F32 = jnp.float32
BF16 = jnp.bfloat16
NZ, NY, NX = 16, 4, 4
MASKED = -1e30


def nt(a, b):
    return lax.dot_general(a, b, (((1,), (1,)), ((), ())), preferred_element_type=F32)


def nn(a, b):
    return lax.dot_general(a, b, (((1,), (0,)), ((), ())), preferred_element_type=F32)


def split(a):
    high = a.astype(BF16)
    return high, (a - high.astype(F32)).astype(BF16)


def kernel(
    q_hbm, k_hbm, v_hbm, g_hbm, o_hbm, dq_hbm, dkv_ref,
    q_home, k_home, v_home, g_home, kv_wide, kv_home, q_rows, g_rows, kv_all,
    mate, keys_t, values_t, diagonal, row_delta, attended_t, dq_t, scores, probs, dscores, g_twice, q_twice,
    o_rows, dq_rows, part, other, row_in, row_sum, block_in, final,
    in_sem, zkv_s, zkv_r, own_s, own_r, zq_s, zq_r, zg_s, zg_r, ag_s, ag_r, fw_s, fw_r,
    o_s, o_r, own_o, dq_s, dq_r, own_dq, sib_s, sib_r, row_s, row_r, blk_s, blk_r, fin_s, fin_r,
):
    z, y, x, c = (lax.axis_index(a) for a in ("z", "y", "x", "c"))
    chip = y * NX + x
    layer, group = z >> 3, z & 7
    scale = 128 ** -0.5

    def z_at(d):
        return (z + d) & 15

    def chip_at(e, sign):
        dy, dx = e >> 2, e & 3
        return (y + 4 + sign * dy) & 3, (x + 4 + sign * dx) & 3

    barrier = pltpu.get_barrier_semaphore()

    def greet(*device):
        pl.semaphore_signal(barrier, inc=1, device_id=device, device_id_type=MESH)

    for d in (8, 7, 9, 6, 10, 5, 11, 4, 12, 3, 13, 2, 14, 1, 15):
        greet(z_at(d), y, x, c)
        greet(z_at(d), y, x, 1 - c)
    for e in (10, 6, 9, 11, 14, 2, 8, 5, 7, 13, 15, 1, 3, 4, 12):
        greet(z, *chip_at(e, 1), c)
    greet(z, y, x, 1 - c)

    stage = [
        pltpu.make_async_copy(k_hbm, k_home, in_sem.at[0]),
        pltpu.make_async_copy(v_hbm, v_home, in_sem.at[1]),
        pltpu.make_async_copy(q_hbm, q_home, in_sem.at[2]),
        pltpu.make_async_copy(g_hbm, g_home, in_sem.at[3]),
        pltpu.make_async_copy(q_hbm.at[layer, :, group], q_rows.at[z], in_sem.at[4]),
        pltpu.make_async_copy(g_hbm.at[layer, :, group], g_rows.at[z], in_sem.at[5]),
    ]
    for copy in stage:
        copy.start()

    def drain(ref, sem):
        pltpu.make_async_remote_copy(
            src_ref=ref, dst_ref=ref, send_sem=sem, recv_sem=sem,
            device_id=(z, y, x, 1 - c), device_id_type=MESH,
        ).wait_recv()

    key_pos = lax.broadcasted_iota(jnp.int32, (512, 128), 0)
    lane = lax.broadcasted_iota(jnp.int32, (512, 128), 1)
    row_pos = 128 * (lane >> 5) + ((lane >> 3) & 3) + 8 * chip + 4 * c
    diagonal[...] = key_pos - row_pos
    identity = (
        lax.broadcasted_iota(jnp.int32, (128, 128), 0)
        == lax.broadcasted_iota(jnp.int32, (128, 128), 1)
    ).astype(F32).astype(BF16)

    with jax.named_scope("p0_kv"):
        stage[0].wait()
        stage[1].wait()
        for l in range(2):
            for i in range(4):
                kv_wide[l, :, i, :] = k_home[l, i].astype(F32)
                kv_wide[l, :, 4 + i, :] = v_home[l, i].astype(F32)
        kv_home[...] = kv_wide[...].astype(BF16)
        for copy in stage[2:]:
            copy.wait()
    with jax.named_scope("p1_barrier"):
        pl.semaphore_wait(barrier, 46)

    def to_z(src, dst, send, recv):
        def make(d):
            t = z_at(d)
            return pltpu.make_async_remote_copy(
                src_ref=src.at[t >> 3, :, t & 7], dst_ref=dst.at[z], send_sem=send,
                recv_sem=recv, device_id=(t, y, x, c), device_id_type=MESH,
            )
        return make

    half = pl.ds(pl.multiple_of(4 * c, 4), 4)

    def to_core(core, d, far):
        t = z_at(d)
        return pltpu.make_async_remote_copy(
            src_ref=kv_home.at[t >> 3, t & 7, pl.ds(4 * core, 4)],
            dst_ref=kv_all.at[core, (20 - d) & 15, chip, half],
            send_sem=zkv_s, recv_sem=zkv_r.at[far],
            device_id=(t, y, x, core), device_id_type=MESH,
        )

    own_kv = pltpu.make_async_remote_copy(
        src_ref=kv_home.at[layer, group], dst_ref=mate, send_sem=own_s,
        recv_sem=own_r, device_id=(z, y, x, 1 - c), device_id_type=MESH,
    )
    zq = to_z(q_home, q_rows, zq_s, zq_r)
    zg = to_z(g_home, g_rows, zg_s, zg_r)

    def loop(low, high, body):
        def step(i, _):
            body(i)
            return 0
        lax.fori_loop(low, high, step, 0)

    with jax.named_scope("p2_zstart"):
        own_kv.start()
        def send_kv(d, far):
            to_core(0, d, far).start()
            to_core(1, d, far).start()

        loop(1, 5, lambda d: (send_kv(d, 0), send_kv(16 - d, 0)))
        loop(5, 12, lambda d: send_kv(d, 1))
        loop(1, 16, lambda d: zq(d).start())
        loop(1, 16, lambda d: zg(d).start())

    PIECES = (pl.ds(0, 9), pl.ds(9, 7))

    def gather(n, e):
        block = kv_all.at[c, PIECES[n], chip]
        return pltpu.make_async_remote_copy(
            src_ref=block, dst_ref=block, send_sem=ag_s,
            recv_sem=ag_r.at[n, e], device_id=(z, *chip_at(e, 1), c), device_id_type=MESH,
        )

    def forward(n, e):
        yy, xx = chip_at(e, -1)
        block = kv_all.at[c, PIECES[n], yy * NX + xx]
        return pltpu.make_async_remote_copy(
            src_ref=block, dst_ref=block, send_sem=fw_s,
            recv_sem=fw_r.at[n], device_id=(z, y, x, 1 - c), device_id_type=MESH,
        )

    with jax.named_scope("p3_zkvn"):
        own_kv.wait_recv()
        mine = kv_wide[layer, group]
        theirs = pltpu.roll(mate[...].astype(F32), 4, 0)
        low_half = (lax.broadcasted_iota(jnp.int32, (8, 128), 0) >> 2) == c
        kv_all[c, 4, chip] = jnp.where(low_half, mine, theirs).astype(BF16)
        drain(kv_home.at[0], zkv_r.at[0])
        loop(1, 16, lambda e: gather(0, e).start())
        forward(0, 0).start()
    with jax.named_scope("p3_zkvf"):
        drain(kv_home.at[0, pl.ds(0, 7)], zkv_r.at[1])
        loop(1, 16, lambda e: gather(1, e).start())
        forward(1, 0).start()

    def pass_on(n, e):
        gather(n, e).wait_recv()
        forward(n, e).start()

    with jax.named_scope("p4_agnear"):
        loop(1, 16, lambda e: pass_on(0, e))
    with jax.named_scope("p5_agfar"):
        loop(1, 16, lambda e: pass_on(1, e))
    with jax.named_scope("p6_fwd"):
        drain(kv_all.at[1 - c, PIECES[0]], fw_r.at[0])
        drain(kv_all.at[1 - c, PIECES[1]], fw_r.at[1])

    def plane_group(kind, kg):
        return jnp.concatenate(
            [kv_all[kind, (4 * kg + i + 20 - z) & 15].reshape(128, 128) for i in range(4)], axis=0
        )

    with jax.named_scope("p8_qwait"):
        drain(q_rows.at[pl.ds(0, 15)], zq_r)

    def home(rows, out, send, recv, own_sem):
        def make(t):
            return pltpu.make_async_remote_copy(
                src_ref=rows.at[t], dst_ref=out.at[layer, :, group], send_sem=send,
                recv_sem=recv, device_id=(t, y, x, c), device_id_type=MESH,
            )
        own = pltpu.make_async_copy(rows.at[z], out.at[layer, :, group], own_sem)
        def start():
            loop(1, 16, lambda d: make(z_at(d)).start())
            own.start()
        def start_at(t):
            @pl.when(t != z)
            def _():
                make(t).start()
            @pl.when(t == z)
            def _():
                own.start()
        def finish():
            drain(rows.at[pl.ds(0, 15)], send)
            drain(rows.at[pl.ds(0, 15)], recv)
            own.wait()
        return start, start_at, finish

    o_start, _, o_finish = home(o_rows, o_hbm, o_s, o_r, own_o)
    _, dq_start, dq_finish = home(dq_rows, dq_hbm, dq_s, dq_r, own_dq)

    factor_2 = scale * 1.4426950408889634

    def pair(rg):
        return slice(256 * rg, 256 * rg + 256)

    def forward_of(rg):
        lanes = pair(rg)
        q = q_rows[4 * rg : 4 * rg + 4].astype(F32).reshape(128, 128).astype(BF16)
        q_twice[lanes] = jnp.concatenate([q, q], axis=0)
        top = jnp.full((8, 128), MASKED, F32)
        for kg in range(rg + 1):
            s = nt(plane_group(0, kg), q) * factor_2
            if kg == rg:
                s = jnp.where(diagonal[...] <= 0, s, MASKED)
            scores[rg, kg] = s
            top = jnp.maximum(top, jnp.max(s.reshape(64, 8, 128), axis=0))
        top = jnp.max(top, axis=0, keepdims=True)
        total = jnp.zeros((8, 128), F32)
        for kg in range(rg + 1):
            e = jnp.exp2(scores[rg, kg] - top)
            scores[rg, kg] = e
            total = total + jnp.sum(e.reshape(64, 8, 128), axis=0)
        inverse = 1.0 / jnp.sum(total, axis=0, keepdims=True)
        acc = jnp.zeros((128, 256), F32)
        for kg in range(rg + 1):
            p = scores[rg, kg] * inverse
            p2 = jnp.concatenate(split(p), axis=1)
            probs[kg, :, lanes] = p2
            scores[rg, kg] = p
            acc = acc + nn(values_t[kg], p2)
        o_t = acc[:, :128] + acc[:, 128:]
        attended_t[rg] = o_t.astype(BF16).astype(F32)
        o_rows[4 * rg : 4 * rg + 4] = o_t.T.reshape(4, 4, 8, 128).astype(BF16)

    def deltas(rg):
        g = g_rows[4 * rg : 4 * rg + 4].astype(F32).reshape(128, 128).astype(BF16)
        g_twice[pair(rg)] = jnp.concatenate([g, g], axis=0)
        delta = nt(identity, g) * attended_t[rg]
        row_delta[rg : rg + 1] = jnp.sum(delta, axis=0, keepdims=True)

    def backward_of(kg):
        for rg in range(kg, 4):
            g = g_twice[256 * rg : 256 * rg + 128]
            ds = scores[rg, kg] * (nt(plane_group(1, kg), g) - row_delta[rg : rg + 1])
            ds2 = jnp.concatenate(split(ds), axis=1)
            dscores[kg, :, pair(rg)] = ds2
            term = nn(keys_t[kg], ds2)
            term = term[:, :128] + term[:, 128:]
            dq_t[rg] = dq_t[rg] + term if kg else term
        dq_rows[4 * kg : 4 * kg + 4] = (dq_t[kg] * scale).T.reshape(4, 4, 8, 128).astype(BF16)
        part[0, kg] = key_sum(kg, kg, 4)
        part[1, kg] = value_sum(kg, kg, 4)

    def value_sum(kg, low, high):
        lanes = slice(256 * low, 256 * high)
        return nn(probs[kg, :, lanes], g_twice[lanes]).reshape(4, 4, 4, 8, 128)

    def key_sum(kg, low, high):
        lanes = slice(256 * low, 256 * high)
        dk = nn(dscores[kg, :, lanes], q_twice[lanes])
        return jnp.swapaxes(dk.reshape(4, 4, 4, 8, 128), 1, 2)

    kind = 1 - c
    along = jnp.where(c == 0, y, x)
    across = jnp.where(c == 0, x, y)

    def sibling(kg):
        return pltpu.make_async_remote_copy(
            src_ref=part.at[c, kg], dst_ref=other.at[kg], send_sem=sib_s,
            recv_sem=sib_r.at[kg], device_id=(z, y, x, 1 - c), device_id_type=MESH,
        )

    def row_send(kg, a):
        t = (along + a) & 3
        return pltpu.make_async_remote_copy(
            src_ref=part.at[kind, kg, :, t], dst_ref=row_in.at[kg, a - 1], send_sem=row_s,
            recv_sem=row_r.at[kg],
            device_id=(z, jnp.where(c == 0, t, y), jnp.where(c == 0, x, t), c), device_id_type=MESH,
        )

    def block_send(kg, a):
        t = (across + a) & 3
        return pltpu.make_async_remote_copy(
            src_ref=row_sum.at[kg, :, t], dst_ref=block_in.at[kg, a - 1], send_sem=blk_s,
            recv_sem=blk_r.at[kg],
            device_id=(z, jnp.where(c == 0, y, t), jnp.where(c == 0, t, x), c), device_id_type=MESH,
        )

    def combine(kg):
        sibling(kg).wait_recv()
        part[kind, kg] = part[kind, kg] + other[kg]
        loop(1, 4, lambda a: row_send(kg, a).start())

    with jax.named_scope("p9_fwd"):
        for kg in range(4):
            keys_t[kg] = nt(identity, plane_group(0, kg)).astype(BF16)
            values_t[kg] = nt(identity, plane_group(1, kg)).astype(BF16)
        for rg in range(4):
            forward_of(rg)

    with jax.named_scope("pa_osend"):
        o_start()
        drain(g_rows.at[pl.ds(0, 15)], zg_r)
    for kg in range(4):
        with jax.named_scope(f"p9_bwd{kg}"):
            if kg == 0:
                for rg in range(4):
                    deltas(rg)
            backward_of(kg)
        with jax.named_scope(f"pa_comb{kg}"):
            sibling(kg).start()
            loop(4 * kg, 4 * kg + 4, dq_start)
            if kg:
                combine(kg - 1)
    with jax.named_scope("pb_combine"):
        combine(3)

    def row_finish(kg):
        drain(row_in.at[kg], row_r.at[kg])
        total = part[kind, kg, :, along]
        for a in range(3):
            total = total + row_in[kg, a]
        row_sum[kg] = total
        loop(1, 4, lambda a: block_send(kg, a).start())

    factor = jnp.where(c == 0, 1.0, scale).astype(F32)

    def finish(kg):
        drain(block_in.at[kg], blk_r.at[kg])
        total = row_sum[kg, :, across]
        for a in range(3):
            total = total + block_in[kg, a]
        final[pl.ds(4 * kg, 4)] = (total * factor).astype(BF16)

    def out(t, other_core):
        core = 1 - c if other_core else c
        return pltpu.make_async_remote_copy(
            src_ref=final.at[t], dst_ref=dkv_ref.at[kind, z], send_sem=fin_s.at[other_core],
            recv_sem=fin_r.at[other_core], device_id=(t, y, x, core), device_id_type=MESH,
        )

    def send_out(t):
        out(t, 1).start()
        @pl.when(t != z)
        def _():
            out(t, 0).start()

    for kg in range(5):
        if kg < 4:
            with jax.named_scope(f"pc_row{kg}"):
                row_finish(kg)
        if kg > 0:
            with jax.named_scope(f"pc_blk{kg - 1}"):
                finish(kg - 1)
                loop(4 * kg - 4, 4 * kg, send_out)
    dkv_ref[kind, z] = final[z]

    with jax.named_scope("pe_sends"):
        own_kv.wait_send()
        drain(kv_all.at[0, 0, pl.ds(0, 15)], zkv_s)
        drain(q_rows.at[pl.ds(0, 15)], zq_s)
        drain(g_rows.at[pl.ds(0, 15)], zg_s)
        drain(kv_all.at[0, :, pl.ds(0, 15)], ag_s)
        drain(kv_all.at[0], fw_s)
        o_finish()
        dq_finish()
        drain(other, sib_s)
        drain(row_in, row_s)
        drain(block_in, blk_s)
    with jax.named_scope("pf_dkv"):
        drain(dkv_ref.at[0, pl.ds(0, 15)], fin_s.at[0])
        drain(dkv_ref.at[0], fin_s.at[1])
        drain(dkv_ref.at[0, pl.ds(0, 15)], fin_r.at[0])
        drain(dkv_ref.at[1], fin_r.at[1])


def on_device(q, k, v, g):
    core = lax.axis_index("c")
    wide = (2, 4, 8, 8, 128)
    dma = pltpu.SemaphoreType.DMA
    hbm = pl.BlockSpec(memory_space=pltpu.MemorySpace.HBM)
    vmem = pl.BlockSpec(memory_space=pltpu.VMEM)
    o, dq, dkv = pl.pallas_call(
        kernel,
        out_shape=(
            jax.ShapeDtypeStruct(wide, BF16),
            jax.ShapeDtypeStruct(wide, BF16),
            jax.ShapeDtypeStruct((2, 16, 8, 128), BF16),
        ),
        in_specs=[hbm, hbm, hbm, hbm],
        out_specs=(hbm, hbm, vmem),
        scratch_shapes=[
            pltpu.VMEM(wide, BF16),
            pltpu.VMEM((2, 4, 8, 128), BF16),
            pltpu.VMEM((2, 4, 8, 128), BF16),
            pltpu.VMEM(wide, BF16),
            pltpu.VMEM((2, 8, 8, 128), F32),
            pltpu.VMEM((2, 8, 8, 128), BF16),
            pltpu.VMEM((16, 4, 8, 128), BF16),
            pltpu.VMEM((16, 4, 8, 128), BF16),
            pltpu.VMEM((2, 16, 16, 8, 128), BF16),
            pltpu.VMEM((8, 128), BF16),
            pltpu.VMEM((4, 128, 512), BF16),
            pltpu.VMEM((4, 128, 512), BF16),
            pltpu.VMEM((512, 128), jnp.int32),
            pltpu.VMEM((8, 128), F32),
            pltpu.VMEM((4, 128, 128), F32),
            pltpu.VMEM((4, 128, 128), F32),
            pltpu.VMEM((4, 4, 512, 128), F32),
            pltpu.VMEM((4, 512, 1024), BF16),
            pltpu.VMEM((4, 512, 1024), BF16),
            pltpu.VMEM((1024, 128), BF16),
            pltpu.VMEM((1024, 128), BF16),
            pltpu.VMEM((16, 4, 8, 128), BF16),
            pltpu.VMEM((16, 4, 8, 128), BF16),
            pltpu.VMEM((2, 4, 4, 4, 4, 8, 128), F32),
            pltpu.VMEM((4, 4, 4, 4, 8, 128), F32),
            pltpu.VMEM((4, 3, 4, 4, 8, 128), F32),
            pltpu.VMEM((4, 4, 4, 8, 128), F32),
            pltpu.VMEM((4, 3, 4, 8, 128), F32),
            pltpu.VMEM((16, 8, 128), BF16),
            dma((6,)),
            dma, dma((2,)), dma, dma, dma, dma, dma, dma,
            dma, dma((2, 16)), dma, dma((2,)),
            dma, dma, dma, dma, dma, dma,
            dma, dma((4,)), dma, dma((4,)), dma, dma((4,)), dma((2,)), dma((2,)),
        ],
        compiler_params=pltpu.CompilerParams(
            collective_id=1, has_side_effects=True, vmem_limit_bytes=67043328
        ),
        name="attend",
    )(q.reshape(wide), k, v, g.reshape(wide))
    dkv = lax.dynamic_slice_in_dim(dkv.reshape(2, 2, 8, 8, 128), 4 * core, 4, 3)
    dkv = dkv.transpose(0, 1, 3, 2, 4)
    return o.reshape(q.shape), dq.reshape(q.shape), dkv[0], dkv[1]


def solution(mesh):
    grid = Mesh(mesh.devices.reshape(NZ, NY, NX, 2), ("z", "y", "x", "c"))
    spec = P(None, ("z", "y", "x", "c"), None, None)
    return jax.shard_map(
        on_device, mesh=grid, in_specs=(spec,) * 4, out_specs=(spec,) * 4, check_vma=False
    )
```

```python
import functools

import jax
import jax.numpy as jnp
from jax import lax
from jax.experimental import pallas as pl
from jax.experimental.pallas import tpu as pltpu
from jax.sharding import Mesh
from jax.sharding import PartitionSpec as P

MESH = pl.DeviceIdType.MESH
F32 = jnp.float32
BF16 = jnp.bfloat16
NZ, NY, NX = 16, 4, 4
MASKED = -1e30
PIECES = ((0, 7), (7, 6), (13, 3))


def nt(a, b):
    return lax.dot_general(a, b, (((1,), (1,)), ((), ())), preferred_element_type=F32)


def nn(a, b):
    return lax.dot_general(a, b, (((1,), (0,)), ((), ())), preferred_element_type=F32)


def split(a):
    high = a.astype(BF16)
    return high, (a - high.astype(F32)).astype(BF16)


def kernel(
    q_hbm, k_hbm, v_hbm, g_hbm, o_hbm, dq_hbm, dkv_ref,
    q_home, k_home, v_home, g_home, kv_wide, kv_home, q_rows, g_rows, kv_all,
    mate, keys_t, values_t, diagonal, row_delta, attended_t, dq_t, scores, probs, dscores, g_twice, q_twice,
    o_rows, dq_rows, part, other, row_in, row_sum, block_in, final,
    in_sem, zkv_s, zkv_r, own_s, own_r, zq_s, zq_r, zg_s, zg_r, ag_s, ag_r, fw_s, fw_r,
    o_s, o_r, own_o, dq_s, dq_r, own_dq, sib_s, sib_r, row_s, row_r, blk_s, blk_r, fin_s, fin_r,
):
    z, y, x, c = (lax.axis_index(a) for a in ("z", "y", "x", "c"))
    chip = y * NX + x
    layer, group = z >> 3, z & 7
    scale = 128 ** -0.5

    def z_at(d):
        return (z + d) & 15

    def chip_at(e, sign):
        dy, dx = e >> 2, e & 3
        return (y + 4 + sign * dy) & 3, (x + 4 + sign * dx) & 3

    barrier = pltpu.get_barrier_semaphore()

    def greet(*device):
        pl.semaphore_signal(barrier, inc=1, device_id=device, device_id_type=MESH)

    for d in (8, 7, 9, 6, 10, 5, 11, 4, 12, 3, 13, 2, 14, 1, 15):
        greet(z_at(d), y, x, c)
        greet(z_at(d), y, x, 1 - c)
    for e in (10, 6, 9, 11, 14, 2, 8, 5, 7, 13, 15, 1, 3, 4, 12):
        greet(z, *chip_at(e, 1), c)
    greet(z, y, x, 1 - c)

    stage = [
        pltpu.make_async_copy(k_hbm, k_home, in_sem.at[0]),
        pltpu.make_async_copy(v_hbm, v_home, in_sem.at[1]),
        pltpu.make_async_copy(q_hbm, q_home, in_sem.at[2]),
        pltpu.make_async_copy(g_hbm, g_home, in_sem.at[3]),
        pltpu.make_async_copy(q_hbm.at[layer, :, group], q_rows.at[z], in_sem.at[4]),
        pltpu.make_async_copy(g_hbm.at[layer, :, group], g_rows.at[z], in_sem.at[5]),
    ]
    for copy in stage:
        copy.start()

    def drain(ref, sem):
        pltpu.make_async_remote_copy(
            src_ref=ref, dst_ref=ref, send_sem=sem, recv_sem=sem,
            device_id=(z, y, x, 1 - c), device_id_type=MESH,
        ).wait_recv()

    key_pos = lax.broadcasted_iota(jnp.int32, (512, 128), 0)
    lane = lax.broadcasted_iota(jnp.int32, (512, 128), 1)
    row_pos = 128 * (lane >> 5) + ((lane >> 3) & 3) + 8 * chip + 4 * c
    diagonal[...] = key_pos - row_pos
    identity = (
        lax.broadcasted_iota(jnp.int32, (128, 128), 0)
        == lax.broadcasted_iota(jnp.int32, (128, 128), 1)
    ).astype(F32).astype(BF16)

    with jax.named_scope("p0_kv"):
        stage[0].wait()
        stage[1].wait()
        for l in range(2):
            for i in range(4):
                kv_wide[l, :, i, :] = k_home[l, i].astype(F32)
                kv_wide[l, :, 4 + i, :] = v_home[l, i].astype(F32)
        kv_home[...] = kv_wide[...].astype(BF16)
        for copy in stage[2:]:
            copy.wait()
    with jax.named_scope("p1_barrier"):
        pl.semaphore_wait(barrier, 46)

    def to_z(src, dst, send, recv):
        def make(d):
            t = z_at(d)
            return pltpu.make_async_remote_copy(
                src_ref=src.at[t >> 3, :, t & 7], dst_ref=dst.at[z], send_sem=send,
                recv_sem=recv, device_id=(t, y, x, c), device_id_type=MESH,
            )
        return make

    half = pl.ds(pl.multiple_of(4 * c, 4), 4)

    def slot_of(u):
        return u + jnp.where(u < 10, 0, jnp.where(u < 13, 3, -3))

    def to_core(core, d, far):
        t = z_at(d)
        return pltpu.make_async_remote_copy(
            src_ref=kv_home.at[t >> 3, t & 7, pl.ds(4 * core, 4)],
            dst_ref=kv_all.at[core, slot_of((19 - d) & 15), chip, half],
            send_sem=zkv_s, recv_sem=zkv_r.at[far],
            device_id=(t, y, x, core), device_id_type=MESH,
        )

    own_kv = pltpu.make_async_remote_copy(
        src_ref=kv_home.at[layer, group], dst_ref=mate, send_sem=own_s,
        recv_sem=own_r, device_id=(z, y, x, 1 - c), device_id_type=MESH,
    )
    zq = to_z(q_home, q_rows, zq_s, zq_r)
    zg = to_z(g_home, g_rows, zg_s, zg_r)

    def loop(low, high, body):
        def step(i, _):
            body(i)
            return 0
        lax.fori_loop(low, high, step, 0)

    with jax.named_scope("p2_zstart"):
        own_kv.start()
        def send_kv(d, far):
            to_core(0, d, far).start()
            to_core(1, d, far).start()

        loop(1, 4, lambda d: (send_kv(d, 0), send_kv(16 - d, 0)))
        loop(4, 7, lambda d: (send_kv(d, 1), send_kv(16 - d, 1)))
        loop(7, 10, lambda d: send_kv(d, 2))
        loop(1, 16, lambda d: zq(d).start())
        loop(1, 16, lambda d: zg(d).start())


    def gather(n, e):
        block = kv_all.at[c, pl.ds(*PIECES[n]), chip]
        return pltpu.make_async_remote_copy(
            src_ref=block, dst_ref=block, send_sem=ag_s,
            recv_sem=ag_r.at[n, e], device_id=(z, *chip_at(e, 1), c), device_id_type=MESH,
        )

    def forward(n, e):
        yy, xx = chip_at(e, -1)
        block = kv_all.at[c, pl.ds(*PIECES[n]), yy * NX + xx]
        return pltpu.make_async_remote_copy(
            src_ref=block, dst_ref=block, send_sem=fw_s,
            recv_sem=fw_r.at[n], device_id=(z, y, x, 1 - c), device_id_type=MESH,
        )

    with jax.named_scope("p3_zkvn"):
        own_kv.wait_recv()
        mine = kv_wide[layer, group]
        theirs = pltpu.roll(mate[...].astype(F32), 4, 0)
        low_half = (lax.broadcasted_iota(jnp.int32, (8, 128), 0) >> 2) == c
        kv_all[c, 3, chip] = jnp.where(low_half, mine, theirs).astype(BF16)
        drain(kv_all.at[0, 0, pl.ds(0, 6)], zkv_r.at[0])
        loop(1, 16, lambda e: gather(0, e).start())
        forward(0, 0).start()
    with jax.named_scope("p3_zkvm"):
        drain(kv_all.at[0, 0, pl.ds(0, 6)], zkv_r.at[1])
        loop(1, 16, lambda e: gather(1, e).start())
        forward(1, 0).start()
    with jax.named_scope("p3_zkvf"):
        drain(kv_all.at[0, 0, pl.ds(0, 3)], zkv_r.at[2])
        loop(1, 16, lambda e: gather(2, e).start())
        forward(2, 0).start()

    def pass_on(n, e):
        gather(n, e).wait_recv()
        forward(n, e).start()

    with jax.named_scope("p4_agnear"):
        loop(1, 16, lambda e: pass_on(0, e))
    with jax.named_scope("p4_agmid"):
        loop(1, 16, lambda e: pass_on(1, e))
    with jax.named_scope("p5_agfar"):
        loop(1, 16, lambda e: pass_on(2, e))
    with jax.named_scope("p6_fwd"):
        for n in range(3):
            drain(kv_all.at[1 - c, pl.ds(*PIECES[n])], fw_r.at[n])

    def plane_group(kind, kg):
        return jnp.concatenate(
            [kv_all[kind, slot_of((4 * kg + i + 19 - z) & 15)].reshape(128, 128) for i in range(4)], axis=0
        )

    with jax.named_scope("p8_qwait"):
        drain(q_rows.at[pl.ds(0, 15)], zq_r)

    def home(rows, out, send, recv, own_sem):
        def make(t):
            return pltpu.make_async_remote_copy(
                src_ref=rows.at[t], dst_ref=out.at[layer, :, group], send_sem=send,
                recv_sem=recv, device_id=(t, y, x, c), device_id_type=MESH,
            )
        own = pltpu.make_async_copy(rows.at[z], out.at[layer, :, group], own_sem)
        def start():
            loop(1, 16, lambda d: make(z_at(d)).start())
            own.start()
        def start_at(t):
            @pl.when(t != z)
            def _():
                make(t).start()
            @pl.when(t == z)
            def _():
                own.start()
        def finish():
            drain(rows.at[pl.ds(0, 15)], send)
            drain(rows.at[pl.ds(0, 15)], recv)
            own.wait()
        return start, start_at, finish

    o_start, _, o_finish = home(o_rows, o_hbm, o_s, o_r, own_o)
    _, dq_start, dq_finish = home(dq_rows, dq_hbm, dq_s, dq_r, own_dq)

    factor_2 = scale * 1.4426950408889634

    def pair(rg):
        return slice(256 * rg, 256 * rg + 256)

    def forward_of(rg):
        lanes = pair(rg)
        q = q_rows[4 * rg : 4 * rg + 4].astype(F32).reshape(128, 128).astype(BF16)
        q_twice[lanes] = jnp.concatenate([q, q], axis=0)
        top = jnp.full((8, 128), MASKED, F32)
        for kg in range(rg + 1):
            s = nt(plane_group(0, kg), q) * factor_2
            if kg == rg:
                s = jnp.where(diagonal[...] <= 0, s, MASKED)
            scores[rg, kg] = s
            top = jnp.maximum(top, jnp.max(s.reshape(64, 8, 128), axis=0))
        top = jnp.max(top, axis=0, keepdims=True)
        total = jnp.zeros((8, 128), F32)
        for kg in range(rg + 1):
            e = jnp.exp2(scores[rg, kg] - top)
            scores[rg, kg] = e
            total = total + jnp.sum(e.reshape(64, 8, 128), axis=0)
        inverse = 1.0 / jnp.sum(total, axis=0, keepdims=True)
        acc = jnp.zeros((128, 256), F32)
        for kg in range(rg + 1):
            p = scores[rg, kg] * inverse
            p2 = jnp.concatenate(split(p), axis=1)
            probs[kg, :, lanes] = p2
            scores[rg, kg] = p
            acc = acc + nn(values_t[kg], p2)
        o_t = acc[:, :128] + acc[:, 128:]
        attended_t[rg] = o_t.astype(BF16).astype(F32)
        o_rows[4 * rg : 4 * rg + 4] = o_t.T.reshape(4, 4, 8, 128).astype(BF16)

    def deltas(rg):
        g = g_rows[4 * rg : 4 * rg + 4].astype(F32).reshape(128, 128).astype(BF16)
        g_twice[pair(rg)] = jnp.concatenate([g, g], axis=0)
        delta = nt(identity, g) * attended_t[rg]
        row_delta[rg : rg + 1] = jnp.sum(delta, axis=0, keepdims=True)

    def backward_of(kg):
        for rg in range(kg, 4):
            g = g_twice[256 * rg : 256 * rg + 128]
            ds = scores[rg, kg] * (nt(plane_group(1, kg), g) - row_delta[rg : rg + 1])
            ds2 = jnp.concatenate(split(ds), axis=1)
            dscores[kg, :, pair(rg)] = ds2
            term = nn(keys_t[kg], ds2)
            term = term[:, :128] + term[:, 128:]
            dq_t[rg] = dq_t[rg] + term if kg else term
        dq_rows[4 * kg : 4 * kg + 4] = (dq_t[kg] * scale).T.reshape(4, 4, 8, 128).astype(BF16)
        part[0, kg] = key_sum(kg, kg, 4)
        part[1, kg] = value_sum(kg, kg, 4)

    def value_sum(kg, low, high):
        lanes = slice(256 * low, 256 * high)
        return nn(probs[kg, :, lanes], g_twice[lanes]).reshape(4, 4, 4, 8, 128)

    def key_sum(kg, low, high):
        lanes = slice(256 * low, 256 * high)
        dk = nn(dscores[kg, :, lanes], q_twice[lanes])
        return jnp.swapaxes(dk.reshape(4, 4, 4, 8, 128), 1, 2)

    kind = 1 - c
    along = jnp.where(c == 0, y, x)
    across = jnp.where(c == 0, x, y)

    def sibling(kg):
        return pltpu.make_async_remote_copy(
            src_ref=part.at[c, kg], dst_ref=other.at[kg], send_sem=sib_s,
            recv_sem=sib_r.at[kg], device_id=(z, y, x, 1 - c), device_id_type=MESH,
        )

    def row_send(kg, a):
        t = (along + a) & 3
        return pltpu.make_async_remote_copy(
            src_ref=part.at[kind, kg, :, t], dst_ref=row_in.at[kg, a - 1], send_sem=row_s,
            recv_sem=row_r.at[kg],
            device_id=(z, jnp.where(c == 0, t, y), jnp.where(c == 0, x, t), c), device_id_type=MESH,
        )

    def block_send(kg, a):
        t = (across + a) & 3
        return pltpu.make_async_remote_copy(
            src_ref=row_sum.at[kg, :, t], dst_ref=block_in.at[kg, a - 1], send_sem=blk_s,
            recv_sem=blk_r.at[kg],
            device_id=(z, jnp.where(c == 0, y, t), jnp.where(c == 0, t, x), c), device_id_type=MESH,
        )

    def combine(kg):
        sibling(kg).wait_recv()
        part[kind, kg] = part[kind, kg] + other[kg]
        loop(1, 4, lambda a: row_send(kg, a).start())

    with jax.named_scope("p9_fwd"):
        for kg in range(4):
            keys_t[kg] = nt(identity, plane_group(0, kg)).astype(BF16)
            values_t[kg] = nt(identity, plane_group(1, kg)).astype(BF16)
        for rg in range(4):
            forward_of(rg)

    with jax.named_scope("pa_osend"):
        o_start()
        drain(g_rows.at[pl.ds(0, 15)], zg_r)
    for kg in range(4):
        with jax.named_scope(f"p9_bwd{kg}"):
            if kg == 0:
                for rg in range(4):
                    deltas(rg)
            backward_of(kg)
        with jax.named_scope(f"pa_comb{kg}"):
            sibling(kg).start()
            loop(4 * kg, 4 * kg + 4, dq_start)
            if kg:
                combine(kg - 1)
    with jax.named_scope("pb_combine"):
        combine(3)

    def row_finish(kg):
        drain(row_in.at[kg], row_r.at[kg])
        total = part[kind, kg, :, along]
        for a in range(3):
            total = total + row_in[kg, a]
        row_sum[kg] = total
        loop(1, 4, lambda a: block_send(kg, a).start())

    factor = jnp.where(c == 0, 1.0, scale).astype(F32)

    def finish(kg):
        drain(block_in.at[kg], blk_r.at[kg])
        total = row_sum[kg, :, across]
        for a in range(3):
            total = total + block_in[kg, a]
        final[pl.ds(4 * kg, 4)] = (total * factor).astype(BF16)

    def out(t, other_core):
        core = 1 - c if other_core else c
        return pltpu.make_async_remote_copy(
            src_ref=final.at[t], dst_ref=dkv_ref.at[kind, z], send_sem=fin_s.at[other_core],
            recv_sem=fin_r.at[other_core], device_id=(t, y, x, core), device_id_type=MESH,
        )

    def send_out(t):
        out(t, 1).start()
        @pl.when(t != z)
        def _():
            out(t, 0).start()

    for kg in range(5):
        if kg < 4:
            with jax.named_scope(f"pc_row{kg}"):
                row_finish(kg)
        if kg > 0:
            with jax.named_scope(f"pc_blk{kg - 1}"):
                finish(kg - 1)
                loop(4 * kg - 4, 4 * kg, send_out)
    dkv_ref[kind, z] = final[z]

    with jax.named_scope("pe_sends"):
        own_kv.wait_send()
        drain(kv_all.at[0, 0, pl.ds(0, 15)], zkv_s)
        drain(q_rows.at[pl.ds(0, 15)], zq_s)
        drain(g_rows.at[pl.ds(0, 15)], zg_s)
        drain(kv_all.at[0, :, pl.ds(0, 15)], ag_s)
        drain(kv_all.at[0], fw_s)
        o_finish()
        dq_finish()
        drain(other, sib_s)
        drain(row_in, row_s)
        drain(block_in, blk_s)
    with jax.named_scope("pf_dkv"):
        drain(dkv_ref.at[0, pl.ds(0, 15)], fin_s.at[0])
        drain(dkv_ref.at[0], fin_s.at[1])
        drain(dkv_ref.at[0, pl.ds(0, 15)], fin_r.at[0])
        drain(dkv_ref.at[1], fin_r.at[1])


def deliver(o_ref, dq_ref, dkv_ref, o_hbm, dq_hbm, dk_hbm, dv_hbm, wide, narrow, sem):
    c = lax.axis_index("c")
    copies = [
        pltpu.make_async_copy(o_ref, o_hbm, sem.at[0]),
        pltpu.make_async_copy(dq_ref, dq_hbm, sem.at[1]),
        pltpu.make_async_copy(narrow.at[0], dk_hbm, sem.at[2]),
        pltpu.make_async_copy(narrow.at[1], dv_hbm, sem.at[3]),
    ]
    copies[0].start()
    copies[1].start()
    wide[...] = dkv_ref[...].astype(F32)
    for core in range(2):
        @pl.when(c == core)
        def _():
            for kind in range(2):
                for l in range(2):
                    for i in range(4):
                        rows = wide[kind, 8 * l : 8 * l + 8, 4 * core + i, :]
                        narrow[kind, l, i] = rows.astype(BF16)
    copies[2].start()
    copies[3].start()
    for copy in copies:
        copy.wait()


def on_device(q, k, v, g):
    wide = (2, 4, 8, 8, 128)
    dma = pltpu.SemaphoreType.DMA
    hbm = pl.BlockSpec(memory_space=pltpu.MemorySpace.HBM)
    vmem = pl.BlockSpec(memory_space=pltpu.VMEM)
    inputs = (q.reshape(wide), k, v, g.reshape(wide))
    o, dq, dkv = pl.pallas_call(
        kernel,
        out_shape=(
            jax.ShapeDtypeStruct(wide, BF16),
            jax.ShapeDtypeStruct(wide, BF16),
            jax.ShapeDtypeStruct((2, 16, 8, 128), BF16),
        ),
        in_specs=[hbm, hbm, hbm, hbm],
        out_specs=(hbm, hbm, vmem),
        scratch_shapes=[
            pltpu.VMEM(wide, BF16),
            pltpu.VMEM((2, 4, 8, 128), BF16),
            pltpu.VMEM((2, 4, 8, 128), BF16),
            pltpu.VMEM(wide, BF16),
            pltpu.VMEM((2, 8, 8, 128), F32),
            pltpu.VMEM((2, 8, 8, 128), BF16),
            pltpu.VMEM((16, 4, 8, 128), BF16),
            pltpu.VMEM((16, 4, 8, 128), BF16),
            pltpu.VMEM((2, 16, 16, 8, 128), BF16),
            pltpu.VMEM((8, 128), BF16),
            pltpu.VMEM((4, 128, 512), BF16),
            pltpu.VMEM((4, 128, 512), BF16),
            pltpu.VMEM((512, 128), jnp.int32),
            pltpu.VMEM((8, 128), F32),
            pltpu.VMEM((4, 128, 128), F32),
            pltpu.VMEM((4, 128, 128), F32),
            pltpu.VMEM((4, 4, 512, 128), F32),
            pltpu.VMEM((4, 512, 1024), BF16),
            pltpu.VMEM((4, 512, 1024), BF16),
            pltpu.VMEM((1024, 128), BF16),
            pltpu.VMEM((1024, 128), BF16),
            pltpu.VMEM((16, 4, 8, 128), BF16),
            pltpu.VMEM((16, 4, 8, 128), BF16),
            pltpu.VMEM((2, 4, 4, 4, 4, 8, 128), F32),
            pltpu.VMEM((4, 4, 4, 4, 8, 128), F32),
            pltpu.VMEM((4, 3, 4, 4, 8, 128), F32),
            pltpu.VMEM((4, 4, 4, 8, 128), F32),
            pltpu.VMEM((4, 3, 4, 8, 128), F32),
            pltpu.VMEM((16, 8, 128), BF16),
            dma((6,)),
            dma, dma((3,)), dma, dma, dma, dma, dma, dma,
            dma, dma((3, 16)), dma, dma((3,)),
            dma, dma, dma, dma, dma, dma,
            dma, dma((4,)), dma, dma((4,)), dma, dma((4,)), dma((2,)), dma((2,)),
        ],
        compiler_params=pltpu.CompilerParams(
            collective_id=1, has_side_effects=True, vmem_limit_bytes=48 * 2**20
        ),
        name="attend",
    )(*(pltpu.with_memory_space_constraint(a, pltpu.MemorySpace.HBM) for a in inputs))
    o, dq, dk, dv = pl.pallas_call(
        deliver,
        out_shape=tuple(jax.ShapeDtypeStruct(a.shape, BF16) for a in (o, dq, k, v)),
        in_specs=[hbm, hbm, vmem],
        out_specs=(hbm,) * 4,
        scratch_shapes=[
            pltpu.VMEM((2, 16, 8, 128), F32), pltpu.VMEM((2, 2, 4, 8, 128), BF16), dma((4,))
        ],
        compiler_params=pltpu.CompilerParams(vmem_limit_bytes=8 * 2**20),
        name="deliver",
    )(o, dq, dkv)
    return o.reshape(q.shape), dq.reshape(q.shape), dk, dv


def solution(mesh):
    grid = Mesh(mesh.devices.reshape(NZ, NY, NX, 2), ("z", "y", "x", "c"))
    spec = P(None, ("z", "y", "x", "c"), None, None)
    return jax.shard_map(
        on_device, mesh=grid, in_specs=(spec,) * 4, out_specs=(spec,) * 4, check_vma=False
    )
```

```python
import functools

import jax
import jax.numpy as jnp
from jax import lax
from jax.experimental import pallas as pl
from jax.experimental.pallas import tpu as pltpu
from jax.sharding import Mesh
from jax.sharding import PartitionSpec as P

MESH = pl.DeviceIdType.MESH
F32 = jnp.float32
BF16 = jnp.bfloat16
NZ, NY, NX = 16, 4, 4
MASKED = -1e30
PIECES = ((0, 7), (7, 6), (13, 3))


def nt(a, b):
    return lax.dot_general(a, b, (((1,), (1,)), ((), ())), preferred_element_type=F32)


def nn(a, b):
    return lax.dot_general(a, b, (((1,), (0,)), ((), ())), preferred_element_type=F32)


def split(a):
    high = a.astype(BF16)
    return high, (a - high.astype(F32)).astype(BF16)


def kernel(
    q_hbm, k_hbm, v_hbm, g_hbm, o_hbm, dq_hbm, dkv_ref,
    q_home, k_home, v_home, g_home, kv_wide, kv_home, q_rows, g_rows, kv_all,
    mate, keys_t, values_t, diagonal, row_delta, attended_t, dq_t, scores, probs, dscores, g_twice, q_twice,
    o_rows, dq_rows, part, other, row_in, row_sum, block_in, first_in, final,
    in_sem, zkv_s, zkv_r, own_s, own_r, zq_s, zq_r, zg_s, zg_r, ag_s, ag_r, fw_s, fw_r,
    o_s, o_r, own_o, dq_s, dq_r, own_dq, sib_s, sib_r, row_s, row_r, blk_s, blk_r, dir_s, dir_r, fin_s, fin_r,
):
    z, y, x, c = (lax.axis_index(a) for a in ("z", "y", "x", "c"))
    chip = y * NX + x
    layer, group = z >> 3, z & 7
    scale = 128 ** -0.5

    def z_at(d):
        return (z + d) & 15

    def chip_at(e, sign):
        dy, dx = e >> 2, e & 3
        return (y + 4 + sign * dy) & 3, (x + 4 + sign * dx) & 3

    barrier = pltpu.get_barrier_semaphore()

    def greet(*device):
        pl.semaphore_signal(barrier, inc=1, device_id=device, device_id_type=MESH)

    for d in (8, 7, 9, 6, 10, 5, 11, 4, 12, 3, 13, 2, 14, 1, 15):
        greet(z_at(d), y, x, c)
        greet(z_at(d), y, x, 1 - c)
    for e in (10, 6, 9, 11, 14, 2, 8, 5, 7, 13, 15, 1, 3, 4, 12):
        greet(z, *chip_at(e, 1), c)
    greet(z, y, x, 1 - c)

    stage = [
        pltpu.make_async_copy(k_hbm, k_home, in_sem.at[0]),
        pltpu.make_async_copy(v_hbm, v_home, in_sem.at[1]),
        pltpu.make_async_copy(q_hbm, q_home, in_sem.at[2]),
        pltpu.make_async_copy(g_hbm, g_home, in_sem.at[3]),
        pltpu.make_async_copy(q_hbm.at[layer, :, group], q_rows.at[z], in_sem.at[4]),
        pltpu.make_async_copy(g_hbm.at[layer, :, group], g_rows.at[z], in_sem.at[5]),
    ]
    for copy in stage:
        copy.start()

    def drain(ref, sem):
        pltpu.make_async_remote_copy(
            src_ref=ref, dst_ref=ref, send_sem=sem, recv_sem=sem,
            device_id=(z, y, x, 1 - c), device_id_type=MESH,
        ).wait_recv()

    key_pos = lax.broadcasted_iota(jnp.int32, (512, 128), 0)
    lane = lax.broadcasted_iota(jnp.int32, (512, 128), 1)
    row_pos = 128 * (lane >> 5) + ((lane >> 3) & 3) + 8 * chip + 4 * c
    diagonal[...] = key_pos - row_pos
    identity = (
        lax.broadcasted_iota(jnp.int32, (128, 128), 0)
        == lax.broadcasted_iota(jnp.int32, (128, 128), 1)
    ).astype(F32).astype(BF16)

    with jax.named_scope("p0_kv"):
        stage[0].wait()
        stage[1].wait()
        for l in range(2):
            for i in range(4):
                kv_wide[l, :, i, :] = k_home[l, i].astype(F32)
                kv_wide[l, :, 4 + i, :] = v_home[l, i].astype(F32)
        kv_home[...] = kv_wide[...].astype(BF16)
        for copy in stage[2:]:
            copy.wait()
    with jax.named_scope("p1_barrier"):
        pl.semaphore_wait(barrier, 46)

    def to_z(src, dst, send, recv):
        def make(d):
            t = z_at(d)
            return pltpu.make_async_remote_copy(
                src_ref=src.at[t >> 3, :, t & 7], dst_ref=dst.at[z], send_sem=send,
                recv_sem=recv, device_id=(t, y, x, c), device_id_type=MESH,
            )
        return make

    half = pl.ds(pl.multiple_of(4 * c, 4), 4)

    def slot_of(u):
        return u + jnp.where(u < 10, 0, jnp.where(u < 13, 3, -3))

    def to_core(core, d, far):
        t = z_at(d)
        return pltpu.make_async_remote_copy(
            src_ref=kv_home.at[t >> 3, t & 7, pl.ds(4 * core, 4)],
            dst_ref=kv_all.at[core, slot_of((19 - d) & 15), chip, half],
            send_sem=zkv_s, recv_sem=zkv_r.at[far],
            device_id=(t, y, x, core), device_id_type=MESH,
        )

    own_kv = pltpu.make_async_remote_copy(
        src_ref=kv_home.at[layer, group], dst_ref=mate, send_sem=own_s,
        recv_sem=own_r, device_id=(z, y, x, 1 - c), device_id_type=MESH,
    )
    zq = to_z(q_home, q_rows, zq_s, zq_r)
    zg = to_z(g_home, g_rows, zg_s, zg_r)

    def loop(low, high, body):
        def step(i, _):
            body(i)
            return 0
        lax.fori_loop(low, high, step, 0)

    def far_first(body):
        loop(1, 9, lambda i: body(9 - i))
        loop(9, 16, body)

    with jax.named_scope("p2_zstart"):
        own_kv.start()
        def send_kv(d, far):
            to_core(0, d, far).start()
            to_core(1, d, far).start()

        loop(1, 4, lambda d: (send_kv(d, 0), send_kv(16 - d, 0)))
        loop(4, 7, lambda d: (send_kv(d, 1), send_kv(16 - d, 1)))
        loop(7, 10, lambda d: send_kv(d, 2))
        loop(1, 16, lambda d: zq(d).start())
        far_first(lambda d: zg(d).start())


    def gather(n, e):
        block = kv_all.at[c, pl.ds(*PIECES[n]), chip]
        return pltpu.make_async_remote_copy(
            src_ref=block, dst_ref=block, send_sem=ag_s,
            recv_sem=ag_r.at[n, e], device_id=(z, *chip_at(e, 1), c), device_id_type=MESH,
        )

    def forward(n, e):
        yy, xx = chip_at(e, -1)
        block = kv_all.at[c, pl.ds(*PIECES[n]), yy * NX + xx]
        return pltpu.make_async_remote_copy(
            src_ref=block, dst_ref=block, send_sem=fw_s,
            recv_sem=fw_r.at[n], device_id=(z, y, x, 1 - c), device_id_type=MESH,
        )

    with jax.named_scope("p3_zkvn"):
        own_kv.wait_recv()
        mine = kv_wide[layer, group]
        theirs = pltpu.roll(mate[...].astype(F32), 4, 0)
        low_half = (lax.broadcasted_iota(jnp.int32, (8, 128), 0) >> 2) == c
        kv_all[c, 3, chip] = jnp.where(low_half, mine, theirs).astype(BF16)
        drain(kv_all.at[0, 0, pl.ds(0, 6)], zkv_r.at[0])
        loop(1, 16, lambda e: gather(0, e).start())
        forward(0, 0).start()
    with jax.named_scope("p3_zkvm"):
        drain(kv_all.at[0, 0, pl.ds(0, 6)], zkv_r.at[1])
        loop(1, 16, lambda e: gather(1, e).start())
        forward(1, 0).start()
    with jax.named_scope("p3_zkvf"):
        drain(kv_all.at[0, 0, pl.ds(0, 3)], zkv_r.at[2])
        loop(1, 16, lambda e: gather(2, e).start())
        forward(2, 0).start()

    def pass_on(n, e):
        gather(n, e).wait_recv()
        forward(n, e).start()

    with jax.named_scope("p4_agnear"):
        loop(1, 16, lambda e: pass_on(0, e))
    with jax.named_scope("p4_agmid"):
        loop(1, 16, lambda e: pass_on(1, e))
    with jax.named_scope("p5_agfar"):
        loop(1, 16, lambda e: pass_on(2, e))
    with jax.named_scope("p6_fwd"):
        for n in range(3):
            drain(kv_all.at[1 - c, pl.ds(*PIECES[n])], fw_r.at[n])

    def plane_group(kind, kg):
        return jnp.concatenate(
            [kv_all[kind, slot_of((4 * kg + i + 19 - z) & 15)].reshape(128, 128) for i in range(4)], axis=0
        )

    with jax.named_scope("p8_qwait"):
        drain(q_rows.at[pl.ds(0, 15)], zq_r)

    def home(rows, out, send, recv, own_sem):
        def make(t):
            return pltpu.make_async_remote_copy(
                src_ref=rows.at[t], dst_ref=out.at[layer, :, group], send_sem=send,
                recv_sem=recv, device_id=(t, y, x, c), device_id_type=MESH,
            )
        own = pltpu.make_async_copy(rows.at[z], out.at[layer, :, group], own_sem)
        def start():
            far_first(lambda d: make(z_at(d)).start())
            own.start()
        def start_at(t):
            @pl.when(t != z)
            def _():
                make(t).start()
            @pl.when(t == z)
            def _():
                own.start()
        def finish():
            drain(rows.at[pl.ds(0, 15)], send)
            drain(rows.at[pl.ds(0, 15)], recv)
            own.wait()
        return start, start_at, finish

    o_start, _, o_finish = home(o_rows, o_hbm, o_s, o_r, own_o)
    _, dq_start, dq_finish = home(dq_rows, dq_hbm, dq_s, dq_r, own_dq)

    factor_2 = scale * 1.4426950408889634

    def pair(rg):
        return slice(256 * rg, 256 * rg + 256)

    def forward_of(rg):
        lanes = pair(rg)
        q = q_rows[4 * rg : 4 * rg + 4].astype(F32).reshape(128, 128).astype(BF16)
        q_twice[lanes] = jnp.concatenate([q, q], axis=0)
        top = jnp.full((8, 128), MASKED, F32)
        for kg in range(rg + 1):
            s = nt(plane_group(0, kg), q) * factor_2
            if kg == rg:
                s = jnp.where(diagonal[...] <= 0, s, MASKED)
            scores[rg, kg] = s
            top = jnp.maximum(top, jnp.max(s.reshape(64, 8, 128), axis=0))
        top = jnp.max(top, axis=0, keepdims=True)
        total = jnp.zeros((8, 128), F32)
        for kg in range(rg + 1):
            e = jnp.exp2(scores[rg, kg] - top)
            scores[rg, kg] = e
            total = total + jnp.sum(e.reshape(64, 8, 128), axis=0)
        inverse = 1.0 / jnp.sum(total, axis=0, keepdims=True)
        acc = jnp.zeros((128, 256), F32)
        for kg in range(rg + 1):
            p = scores[rg, kg] * inverse
            p2 = jnp.concatenate(split(p), axis=1)
            probs[kg, :, lanes] = p2
            scores[rg, kg] = p
            acc = acc + nn(values_t[kg], p2)
        o_t = acc[:, :128] + acc[:, 128:]
        attended_t[rg] = o_t.astype(BF16).astype(F32)
        o_rows[4 * rg : 4 * rg + 4] = o_t.T.reshape(4, 4, 8, 128).astype(BF16)

    def deltas(rg):
        g = g_rows[4 * rg : 4 * rg + 4].astype(F32).reshape(128, 128).astype(BF16)
        g_twice[pair(rg)] = jnp.concatenate([g, g], axis=0)
        delta = nt(identity, g) * attended_t[rg]
        row_delta[rg : rg + 1] = jnp.sum(delta, axis=0, keepdims=True)

    def backward_of(kg):
        for rg in range(kg, 4):
            g = g_twice[256 * rg : 256 * rg + 128]
            ds = scores[rg, kg] * (nt(plane_group(1, kg), g) - row_delta[rg : rg + 1])
            ds2 = jnp.concatenate(split(ds), axis=1)
            dscores[kg, :, pair(rg)] = ds2
            term = nn(keys_t[kg], ds2)
            term = term[:, :128] + term[:, 128:]
            dq_t[rg] = dq_t[rg] + term if kg else term
        dq_rows[4 * kg : 4 * kg + 4] = (dq_t[kg] * scale).T.reshape(4, 4, 8, 128).astype(BF16)
        part[0, kg] = key_sum(kg, kg, 4)
        part[1, kg] = value_sum(kg, kg, 4)

    def value_sum(kg, low, high):
        lanes = slice(256 * low, 256 * high)
        return nn(probs[kg, :, lanes], g_twice[lanes]).reshape(4, 4, 4, 8, 128)

    def key_sum(kg, low, high):
        lanes = slice(256 * low, 256 * high)
        dk = nn(dscores[kg, :, lanes], q_twice[lanes])
        return jnp.swapaxes(dk.reshape(4, 4, 4, 8, 128), 1, 2)

    kind = 1 - c
    along = jnp.where(c == 0, y, x)
    across = jnp.where(c == 0, x, y)

    def sibling(kg):
        return pltpu.make_async_remote_copy(
            src_ref=part.at[c, kg], dst_ref=other.at[kg], send_sem=sib_s,
            recv_sem=sib_r.at[kg], device_id=(z, y, x, 1 - c), device_id_type=MESH,
        )

    def row_send(kg, a):
        t = (along + a) & 3
        return pltpu.make_async_remote_copy(
            src_ref=part.at[kind, kg, :, t], dst_ref=row_in.at[kg, a - 1], send_sem=row_s,
            recv_sem=row_r.at[kg],
            device_id=(z, jnp.where(c == 0, t, y), jnp.where(c == 0, x, t), c), device_id_type=MESH,
        )

    def block_send(kg, a):
        t = (across + a) & 3
        return pltpu.make_async_remote_copy(
            src_ref=row_sum.at[kg, :, t], dst_ref=block_in.at[kg, a - 1], send_sem=blk_s,
            recv_sem=blk_r.at[kg],
            device_id=(z, jnp.where(c == 0, y, t), jnp.where(c == 0, t, x), c), device_id_type=MESH,
        )

    def direct_send(j):
        yy, xx = j >> 2, j & 3
        a, b = jnp.where(c == 0, yy, xx), jnp.where(c == 0, xx, yy)
        return pltpu.make_async_remote_copy(
            src_ref=part.at[kind, 0, :, a, b], dst_ref=first_in.at[(j - chip + 15) & 15],
            send_sem=dir_s, recv_sem=dir_r, device_id=(z, yy, xx, c), device_id_type=MESH,
        )

    def combine(kg):
        sibling(kg).wait_recv()
        part[kind, kg] = part[kind, kg] + other[kg]
        if kg:
            loop(1, 4, lambda a: row_send(kg, a).start())
        else:
            loop(1, 16, lambda e: direct_send(jnp.where(e - 1 < chip, e - 1, e)).start())

    with jax.named_scope("p9_fwd"):
        for kg in range(4):
            keys_t[kg] = nt(identity, plane_group(0, kg)).astype(BF16)
            values_t[kg] = nt(identity, plane_group(1, kg)).astype(BF16)
        for rg in range(4):
            forward_of(rg)

    with jax.named_scope("pa_osend"):
        o_start()
        drain(g_rows.at[pl.ds(0, 15)], zg_r)
    for kg in range(4):
        with jax.named_scope(f"p9_bwd{kg}"):
            if kg == 0:
                for rg in range(4):
                    deltas(rg)
            backward_of(kg)
        with jax.named_scope(f"pa_comb{kg}"):
            sibling(kg).start()
            loop(4 * kg, 4 * kg + 4, dq_start)
            if kg:
                combine(kg - 1)
    with jax.named_scope("pb_combine"):
        combine(3)

    def row_finish(kg):
        drain(row_in.at[kg], row_r.at[kg])
        total = part[kind, kg, :, along]
        for a in range(3):
            total = total + row_in[kg, a]
        row_sum[kg] = total
        loop(1, 4, lambda a: block_send(kg, a).start())

    factor = jnp.where(c == 0, 1.0, scale).astype(F32)

    def finish_first():
        drain(first_in, dir_r)
        total = part[kind, 0, :, along, across]
        for e in range(15):
            total = total + first_in[e]
        final[pl.ds(0, 4)] = (total * factor).astype(BF16)

    def finish(kg):
        drain(block_in.at[kg], blk_r.at[kg])
        total = row_sum[kg, :, across]
        for a in range(3):
            total = total + block_in[kg, a]
        final[pl.ds(4 * kg, 4)] = (total * factor).astype(BF16)

    def out(t, other_core):
        core = 1 - c if other_core else c
        return pltpu.make_async_remote_copy(
            src_ref=final.at[t], dst_ref=dkv_ref.at[kind, z], send_sem=fin_s.at[other_core],
            recv_sem=fin_r.at[other_core], device_id=(t, y, x, core), device_id_type=MESH,
        )

    def send_out(t):
        out(t, 1).start()
        @pl.when(t != z)
        def _():
            out(t, 0).start()

    with jax.named_scope("pc_first"):
        finish_first()
        loop(0, 4, send_out)
    for kg in range(1, 5):
        if kg < 4:
            with jax.named_scope(f"pc_row{kg}"):
                row_finish(kg)
        if kg > 1:
            with jax.named_scope(f"pc_blk{kg - 1}"):
                finish(kg - 1)
                loop(4 * kg - 4, 4 * kg, send_out)
    dkv_ref[kind, z] = final[z]

    with jax.named_scope("pe_sends"):
        own_kv.wait_send()
        drain(kv_all.at[0, 0, pl.ds(0, 15)], zkv_s)
        drain(q_rows.at[pl.ds(0, 15)], zq_s)
        drain(g_rows.at[pl.ds(0, 15)], zg_s)
        drain(kv_all.at[0, :, pl.ds(0, 15)], ag_s)
        drain(kv_all.at[0], fw_s)
        o_finish()
        dq_finish()
        drain(other, sib_s)
        drain(first_in, dir_s)
        drain(row_in.at[pl.ds(0, 3)], row_s)
        drain(block_in.at[pl.ds(0, 3)], blk_s)
    with jax.named_scope("pf_dkv"):
        drain(dkv_ref.at[0, pl.ds(0, 15)], fin_s.at[0])
        drain(dkv_ref.at[0], fin_s.at[1])
        drain(dkv_ref.at[0, pl.ds(0, 15)], fin_r.at[0])
        drain(dkv_ref.at[1], fin_r.at[1])


def deliver(o_ref, dq_ref, dkv_ref, o_hbm, dq_hbm, dk_hbm, dv_hbm, wide, narrow, sem):
    c = lax.axis_index("c")
    copies = [
        pltpu.make_async_copy(o_ref, o_hbm, sem.at[0]),
        pltpu.make_async_copy(dq_ref, dq_hbm, sem.at[1]),
        pltpu.make_async_copy(narrow.at[0], dk_hbm, sem.at[2]),
        pltpu.make_async_copy(narrow.at[1], dv_hbm, sem.at[3]),
    ]
    copies[0].start()
    copies[1].start()
    wide[...] = dkv_ref[...].astype(F32)
    for core in range(2):
        @pl.when(c == core)
        def _():
            for kind in range(2):
                for l in range(2):
                    for i in range(4):
                        rows = wide[kind, 8 * l : 8 * l + 8, 4 * core + i, :]
                        narrow[kind, l, i] = rows.astype(BF16)
    copies[2].start()
    copies[3].start()
    for copy in copies:
        copy.wait()


def on_device(q, k, v, g):
    wide = (2, 4, 8, 8, 128)
    dma = pltpu.SemaphoreType.DMA
    hbm = pl.BlockSpec(memory_space=pltpu.MemorySpace.HBM)
    vmem = pl.BlockSpec(memory_space=pltpu.VMEM)
    inputs = (q.reshape(wide), k, v, g.reshape(wide))
    o, dq, dkv = pl.pallas_call(
        kernel,
        out_shape=(
            jax.ShapeDtypeStruct(wide, BF16),
            jax.ShapeDtypeStruct(wide, BF16),
            jax.ShapeDtypeStruct((2, 16, 8, 128), BF16),
        ),
        in_specs=[hbm, hbm, hbm, hbm],
        out_specs=(hbm, hbm, vmem),
        scratch_shapes=[
            pltpu.VMEM(wide, BF16),
            pltpu.VMEM((2, 4, 8, 128), BF16),
            pltpu.VMEM((2, 4, 8, 128), BF16),
            pltpu.VMEM(wide, BF16),
            pltpu.VMEM((2, 8, 8, 128), F32),
            pltpu.VMEM((2, 8, 8, 128), BF16),
            pltpu.VMEM((16, 4, 8, 128), BF16),
            pltpu.VMEM((16, 4, 8, 128), BF16),
            pltpu.VMEM((2, 16, 16, 8, 128), BF16),
            pltpu.VMEM((8, 128), BF16),
            pltpu.VMEM((4, 128, 512), BF16),
            pltpu.VMEM((4, 128, 512), BF16),
            pltpu.VMEM((512, 128), jnp.int32),
            pltpu.VMEM((8, 128), F32),
            pltpu.VMEM((4, 128, 128), F32),
            pltpu.VMEM((4, 128, 128), F32),
            pltpu.VMEM((4, 4, 512, 128), F32),
            pltpu.VMEM((4, 512, 1024), BF16),
            pltpu.VMEM((4, 512, 1024), BF16),
            pltpu.VMEM((1024, 128), BF16),
            pltpu.VMEM((1024, 128), BF16),
            pltpu.VMEM((16, 4, 8, 128), BF16),
            pltpu.VMEM((16, 4, 8, 128), BF16),
            pltpu.VMEM((2, 4, 4, 4, 4, 8, 128), F32),
            pltpu.VMEM((4, 4, 4, 4, 8, 128), F32),
            pltpu.VMEM((4, 3, 4, 4, 8, 128), F32),
            pltpu.VMEM((4, 4, 4, 8, 128), F32),
            pltpu.VMEM((4, 3, 4, 8, 128), F32),
            pltpu.VMEM((15, 4, 8, 128), F32),
            pltpu.VMEM((16, 8, 128), BF16),
            dma((6,)),
            dma, dma((3,)), dma, dma, dma, dma, dma, dma,
            dma, dma((3, 16)), dma, dma((3,)),
            dma, dma, dma, dma, dma, dma,
            dma, dma((4,)), dma, dma((4,)), dma, dma((4,)), dma, dma, dma((2,)), dma((2,)),
        ],
        compiler_params=pltpu.CompilerParams(
            collective_id=1, has_side_effects=True, vmem_limit_bytes=48 * 2**20
        ),
        name="attend",
    )(*(pltpu.with_memory_space_constraint(a, pltpu.MemorySpace.HBM) for a in inputs))
    o, dq, dk, dv = pl.pallas_call(
        deliver,
        out_shape=tuple(jax.ShapeDtypeStruct(a.shape, BF16) for a in (o, dq, k, v)),
        in_specs=[hbm, hbm, vmem],
        out_specs=(hbm,) * 4,
        scratch_shapes=[
            pltpu.VMEM((2, 16, 8, 128), F32), pltpu.VMEM((2, 2, 4, 8, 128), BF16), dma((4,))
        ],
        compiler_params=pltpu.CompilerParams(vmem_limit_bytes=8 * 2**20),
        name="deliver",
    )(o, dq, dkv)
    return o.reshape(q.shape), dq.reshape(q.shape), dk, dv


def solution(mesh):
    grid = Mesh(mesh.devices.reshape(NZ, NY, NX, 2), ("z", "y", "x", "c"))
    spec = P(None, ("z", "y", "x", "c"), None, None)
    return jax.shard_map(
        on_device, mesh=grid, in_specs=(spec,) * 4, out_specs=(spec,) * 4, check_vma=False
    )
```

```python
import functools

import jax
import jax.numpy as jnp
from jax import lax
from jax.experimental import pallas as pl
from jax.experimental.pallas import tpu as pltpu
from jax.sharding import Mesh
from jax.sharding import PartitionSpec as P

MESH = pl.DeviceIdType.MESH
F32 = jnp.float32
BF16 = jnp.bfloat16
NZ, NY, NX = 16, 4, 4
MASKED = -1e30
PIECES = ((0, 7), (7, 6), (13, 3))


def nt(a, b):
    return lax.dot_general(a, b, (((1,), (1,)), ((), ())), preferred_element_type=F32)


def nn(a, b):
    return lax.dot_general(a, b, (((1,), (0,)), ((), ())), preferred_element_type=F32)


def split(a):
    high = a.astype(BF16)
    return high, (a - high.astype(F32)).astype(BF16)


def kernel(
    q_hbm, k_hbm, v_hbm, g_hbm, o_hbm, dq_hbm, dkv_ref,
    q_home, k_home, v_home, g_home, kv_wide, kv_home, q_rows, g_rows, kv_all,
    mate, keys_t, values_t, diagonal, row_delta, tops, attended_t, dq_t, scores, probs, dscores, g_twice, q_twice,
    o_rows, dq_rows, part, other, row_in, row_sum, block_in, first_in, final,
    in_sem, zkv_s, zkv_r, own_s, own_r, zq_s, zq_r, zg_s, zg_r, ag_s, ag_r, fw_s, fw_r,
    o_s, o_r, own_o, dq_s, dq_r, own_dq, sib_s, sib_r, row_s, row_r, blk_s, blk_r, dir_s, dir_r, fin_s, fin_r,
):
    z, y, x, c = (lax.axis_index(a) for a in ("z", "y", "x", "c"))
    chip = y * NX + x
    layer, group = z >> 3, z & 7
    scale = 128 ** -0.5

    def z_at(d):
        return (z + d) & 15

    def chip_at(e, sign):
        dy, dx = e >> 2, e & 3
        return (y + 4 + sign * dy) & 3, (x + 4 + sign * dx) & 3

    barrier = pltpu.get_barrier_semaphore()

    def greet(*device):
        pl.semaphore_signal(barrier, inc=1, device_id=device, device_id_type=MESH)

    for d in (8, 7, 9, 6, 10, 5, 11, 4, 12, 3, 13, 2, 14, 1, 15):
        greet(z_at(d), y, x, c)
        greet(z_at(d), y, x, 1 - c)
    for e in (10, 6, 9, 11, 14, 2, 8, 5, 7, 13, 15, 1, 3, 4, 12):
        greet(z, *chip_at(e, 1), c)
    greet(z, y, x, 1 - c)

    stage = [
        pltpu.make_async_copy(k_hbm, k_home, in_sem.at[0]),
        pltpu.make_async_copy(v_hbm, v_home, in_sem.at[1]),
        pltpu.make_async_copy(q_hbm, q_home, in_sem.at[2]),
        pltpu.make_async_copy(g_hbm, g_home, in_sem.at[3]),
        pltpu.make_async_copy(q_hbm.at[layer, :, group], q_rows.at[z], in_sem.at[4]),
        pltpu.make_async_copy(g_hbm.at[layer, :, group], g_rows.at[z], in_sem.at[5]),
    ]
    for copy in stage:
        copy.start()

    def drain(ref, sem):
        pltpu.make_async_remote_copy(
            src_ref=ref, dst_ref=ref, send_sem=sem, recv_sem=sem,
            device_id=(z, y, x, 1 - c), device_id_type=MESH,
        ).wait_recv()

    key_pos = lax.broadcasted_iota(jnp.int32, (512, 128), 0)
    lane = lax.broadcasted_iota(jnp.int32, (512, 128), 1)
    row_pos = 128 * (lane >> 5) + ((lane >> 3) & 3) + 8 * chip + 4 * c
    diagonal[...] = key_pos - row_pos
    identity = (
        lax.broadcasted_iota(jnp.int32, (128, 128), 0)
        == lax.broadcasted_iota(jnp.int32, (128, 128), 1)
    ).astype(F32).astype(BF16)

    with jax.named_scope("p0_kv"):
        stage[0].wait()
        stage[1].wait()
        for l in range(2):
            for i in range(4):
                kv_wide[l, :, i, :] = k_home[l, i].astype(F32)
                kv_wide[l, :, 4 + i, :] = v_home[l, i].astype(F32)
        kv_home[...] = kv_wide[...].astype(BF16)
        for copy in stage[2:]:
            copy.wait()
    with jax.named_scope("p1_barrier"):
        pl.semaphore_wait(barrier, 46)

    def to_z(src, dst, send, recv):
        def make(d):
            t = z_at(d)
            return pltpu.make_async_remote_copy(
                src_ref=src.at[t >> 3, :, t & 7], dst_ref=dst.at[z], send_sem=send,
                recv_sem=recv, device_id=(t, y, x, c), device_id_type=MESH,
            )
        return make

    half = pl.ds(pl.multiple_of(4 * c, 4), 4)

    def slot_of(u):
        return u + jnp.where(u < 10, 0, jnp.where(u < 13, 3, -3))

    def to_core(core, d, far):
        t = z_at(d)
        return pltpu.make_async_remote_copy(
            src_ref=kv_home.at[t >> 3, t & 7, pl.ds(4 - 4 * core, 4)],
            dst_ref=kv_all.at[1 - core, slot_of((19 - d) & 15), chip, half],
            send_sem=zkv_s, recv_sem=zkv_r.at[far],
            device_id=(t, y, x, core), device_id_type=MESH,
        )

    own_kv = pltpu.make_async_remote_copy(
        src_ref=kv_home.at[layer, group], dst_ref=mate, send_sem=own_s,
        recv_sem=own_r, device_id=(z, y, x, 1 - c), device_id_type=MESH,
    )
    zq = to_z(q_home, q_rows, zq_s, zq_r)
    zg = to_z(g_home, g_rows, zg_s, zg_r)

    def loop(low, high, body):
        def step(i, _):
            body(i)
            return 0
        lax.fori_loop(low, high, step, 0)

    def far_first(body):
        loop(1, 9, lambda i: body(9 - i))
        loop(9, 16, body)

    with jax.named_scope("p2_zstart"):
        own_kv.start()
        def send_kv(d, far):
            to_core(0, d, far).start()
            to_core(1, d, far).start()

        loop(1, 4, lambda d: (send_kv(d, 0), send_kv(16 - d, 0)))
        loop(4, 7, lambda d: (send_kv(d, 1), send_kv(16 - d, 1)))
        loop(7, 10, lambda d: send_kv(d, 2))
        loop(1, 16, lambda d: zq(d).start())
        far_first(lambda d: zg(d).start())


    def gather(n, e):
        block = kv_all.at[1 - c, pl.ds(*PIECES[n]), chip]
        return pltpu.make_async_remote_copy(
            src_ref=block, dst_ref=block, send_sem=ag_s,
            recv_sem=ag_r.at[n], device_id=(z, *chip_at(e, 1), c), device_id_type=MESH,
        )

    def forward(n):
        block = kv_all.at[1 - c, pl.ds(*PIECES[n])]
        return pltpu.make_async_remote_copy(
            src_ref=block, dst_ref=block, send_sem=fw_s,
            recv_sem=fw_r.at[n], device_id=(z, y, x, 1 - c), device_id_type=MESH,
        )

    with jax.named_scope("p3_zkvn"):
        own_kv.wait_recv()
        mine = pltpu.roll(kv_wide[layer, group], 4, 0)
        own_half = (lax.broadcasted_iota(jnp.int32, (8, 128), 0) >> 2) == c
        kv_all[1 - c, 3, chip] = jnp.where(own_half, mine, mate[...].astype(F32)).astype(BF16)
        drain(kv_all.at[0, 0, pl.ds(0, 6)], zkv_r.at[0])
        loop(1, 16, lambda e: gather(0, e).start())
    with jax.named_scope("p3_zkvm"):
        drain(kv_all.at[0, 0, pl.ds(0, 6)], zkv_r.at[1])
        loop(1, 16, lambda e: gather(1, e).start())
    with jax.named_scope("p3_zkvf"):
        drain(kv_all.at[0, 0, pl.ds(0, 3)], zkv_r.at[2])
        loop(1, 16, lambda e: gather(2, e).start())

    for n in range(3):
        with jax.named_scope(f"p4_ag{n}"):
            drain(kv_all.at[1 - c, pl.ds(*PIECES[n]), pl.ds(0, 15)], ag_r.at[n])
            forward(n).start()
    def of_core(core, body):
        @pl.when(c == core)
        def _():
            body()

    def from_sibling():
        for n in range(3):
            drain(kv_all.at[c, pl.ds(*PIECES[n])], fw_r.at[n])

    with jax.named_scope("p6_keys"):
        of_core(0, from_sibling)

    def plane_group(kind, kg):
        return jnp.concatenate(
            [kv_all[kind, slot_of((4 * kg + i + 19 - z) & 15)].reshape(128, 128) for i in range(4)], axis=0
        )

    with jax.named_scope("p8_qwait"):
        drain(q_rows.at[pl.ds(0, 15)], zq_r)

    def home(rows, out, send, recv, own_sem):
        def make(t):
            return pltpu.make_async_remote_copy(
                src_ref=rows.at[t], dst_ref=out.at[layer, :, group], send_sem=send,
                recv_sem=recv, device_id=(t, y, x, c), device_id_type=MESH,
            )
        own = pltpu.make_async_copy(rows.at[z], out.at[layer, :, group], own_sem)
        def start():
            far_first(lambda d: make(z_at(d)).start())
            own.start()
        def start_at(t):
            @pl.when(t != z)
            def _():
                make(t).start()
            @pl.when(t == z)
            def _():
                own.start()
        def finish():
            drain(rows.at[pl.ds(0, 15)], send)
            drain(rows.at[pl.ds(0, 15)], recv)
            own.wait()
        return start, start_at, finish

    o_start, _, o_finish = home(o_rows, o_hbm, o_s, o_r, own_o)
    _, dq_start, dq_finish = home(dq_rows, dq_hbm, dq_s, dq_r, own_dq)

    factor_2 = scale * 1.4426950408889634

    def pair(rg):
        return slice(256 * rg, 256 * rg + 256)

    def scores_of(rg):
        lanes = pair(rg)
        q = q_rows[4 * rg : 4 * rg + 4].astype(F32).reshape(128, 128).astype(BF16)
        q_twice[lanes] = jnp.concatenate([q, q], axis=0)
        top = jnp.full((8, 128), MASKED, F32)
        for kg in range(rg + 1):
            s = nt(plane_group(0, kg), q) * factor_2
            if kg == rg:
                s = jnp.where(diagonal[...] <= 0, s, MASKED)
            scores[rg, kg] = s
            top = jnp.maximum(top, jnp.max(s.reshape(64, 8, 128), axis=0))
        return jnp.max(top, axis=0, keepdims=True)

    def forward_of(rg, top):
        lanes = pair(rg)
        total = jnp.zeros((8, 128), F32)
        for kg in range(rg + 1):
            e = jnp.exp2(scores[rg, kg] - top)
            scores[rg, kg] = e
            total = total + jnp.sum(e.reshape(64, 8, 128), axis=0)
        inverse = 1.0 / jnp.sum(total, axis=0, keepdims=True)
        acc = jnp.zeros((128, 256), F32)
        for kg in range(rg + 1):
            p = scores[rg, kg] * inverse
            p2 = jnp.concatenate(split(p), axis=1)
            probs[kg, :, lanes] = p2
            scores[rg, kg] = p
            acc = acc + nn(values_t[kg], p2)
        o_t = acc[:, :128] + acc[:, 128:]
        attended_t[rg] = o_t.astype(BF16).astype(F32)
        o_rows[4 * rg : 4 * rg + 4] = o_t.T.reshape(4, 4, 8, 128).astype(BF16)

    def deltas(rg):
        g = g_rows[4 * rg : 4 * rg + 4].astype(F32).reshape(128, 128).astype(BF16)
        g_twice[pair(rg)] = jnp.concatenate([g, g], axis=0)
        delta = nt(identity, g) * attended_t[rg]
        row_delta[rg : rg + 1] = jnp.sum(delta, axis=0, keepdims=True)

    def backward_of(kg):
        for rg in range(kg, 4):
            g = g_twice[256 * rg : 256 * rg + 128]
            ds = scores[rg, kg] * (nt(plane_group(1, kg), g) - row_delta[rg : rg + 1])
            ds2 = jnp.concatenate(split(ds), axis=1)
            dscores[kg, :, pair(rg)] = ds2
            term = nn(keys_t[kg], ds2)
            term = term[:, :128] + term[:, 128:]
            dq_t[rg] = dq_t[rg] + term if kg else term
        dq_rows[4 * kg : 4 * kg + 4] = (dq_t[kg] * scale).T.reshape(4, 4, 8, 128).astype(BF16)
        part[0, kg] = key_sum(kg, kg, 4)
        part[1, kg] = value_sum(kg, kg, 4)

    def value_sum(kg, low, high):
        lanes = slice(256 * low, 256 * high)
        return nn(probs[kg, :, lanes], g_twice[lanes]).reshape(4, 4, 4, 8, 128)

    def key_sum(kg, low, high):
        lanes = slice(256 * low, 256 * high)
        dk = nn(dscores[kg, :, lanes], q_twice[lanes])
        return jnp.swapaxes(dk.reshape(4, 4, 4, 8, 128), 1, 2)

    kind = 1 - c
    along = jnp.where(c == 0, y, x)
    across = jnp.where(c == 0, x, y)

    def sibling(kg):
        return pltpu.make_async_remote_copy(
            src_ref=part.at[c, kg], dst_ref=other.at[kg], send_sem=sib_s,
            recv_sem=sib_r.at[kg], device_id=(z, y, x, 1 - c), device_id_type=MESH,
        )

    def row_send(kg, a):
        t = (along + a) & 3
        return pltpu.make_async_remote_copy(
            src_ref=part.at[kind, kg, :, t], dst_ref=row_in.at[kg, a - 1], send_sem=row_s,
            recv_sem=row_r.at[kg],
            device_id=(z, jnp.where(c == 0, t, y), jnp.where(c == 0, x, t), c), device_id_type=MESH,
        )

    def block_send(kg, a):
        t = (across + a) & 3
        return pltpu.make_async_remote_copy(
            src_ref=row_sum.at[kg, :, t], dst_ref=block_in.at[kg, a - 1], send_sem=blk_s,
            recv_sem=blk_r.at[kg],
            device_id=(z, jnp.where(c == 0, y, t), jnp.where(c == 0, t, x), c), device_id_type=MESH,
        )

    def direct_send(j):
        yy, xx = j >> 2, j & 3
        a, b = jnp.where(c == 0, yy, xx), jnp.where(c == 0, xx, yy)
        return pltpu.make_async_remote_copy(
            src_ref=part.at[kind, 0, :, a, b], dst_ref=first_in.at[(j - chip + 15) & 15],
            send_sem=dir_s, recv_sem=dir_r, device_id=(z, yy, xx, c), device_id_type=MESH,
        )

    def combine(kg):
        sibling(kg).wait_recv()
        part[kind, kg] = part[kind, kg] + other[kg]
        if kg:
            loop(1, 4, lambda a: row_send(kg, a).start())
        else:
            loop(1, 16, lambda e: direct_send(jnp.where(e - 1 < chip, e - 1, e)).start())

    with jax.named_scope("p9_scores"):
        for rg in range(4):
            tops[rg : rg + 1] = scores_of(rg)
        for kg in range(4):
            keys_t[kg] = nt(identity, plane_group(0, kg)).astype(BF16)
    with jax.named_scope("p9_values"):
        of_core(1, from_sibling)
    with jax.named_scope("p9_fwd"):
        for kg in range(4):
            values_t[kg] = nt(identity, plane_group(1, kg)).astype(BF16)
        for rg in range(4):
            forward_of(rg, tops[rg : rg + 1])

    with jax.named_scope("pa_osend"):
        o_start()
        drain(g_rows.at[pl.ds(0, 15)], zg_r)
    for kg in range(4):
        with jax.named_scope(f"p9_bwd{kg}"):
            if kg == 0:
                for rg in range(4):
                    deltas(rg)
            backward_of(kg)
        with jax.named_scope(f"pa_comb{kg}"):
            sibling(kg).start()
            loop(4 * kg, 4 * kg + 4, dq_start)
            if kg:
                combine(kg - 1)
    with jax.named_scope("pb_combine"):
        combine(3)

    def row_finish(kg):
        drain(row_in.at[kg], row_r.at[kg])
        total = part[kind, kg, :, along]
        for a in range(3):
            total = total + row_in[kg, a]
        row_sum[kg] = total
        loop(1, 4, lambda a: block_send(kg, a).start())

    factor = jnp.where(c == 0, 1.0, scale).astype(F32)

    def finish_first():
        drain(first_in, dir_r)
        total = part[kind, 0, :, along, across]
        for e in range(15):
            total = total + first_in[e]
        final[pl.ds(0, 4)] = (total * factor).astype(BF16)

    def finish(kg):
        drain(block_in.at[kg], blk_r.at[kg])
        total = row_sum[kg, :, across]
        for a in range(3):
            total = total + block_in[kg, a]
        final[pl.ds(4 * kg, 4)] = (total * factor).astype(BF16)

    def out(t, other_core):
        core = 1 - c if other_core else c
        return pltpu.make_async_remote_copy(
            src_ref=final.at[t], dst_ref=dkv_ref.at[kind, z], send_sem=fin_s.at[other_core],
            recv_sem=fin_r.at[other_core], device_id=(t, y, x, core), device_id_type=MESH,
        )

    def send_out(t):
        out(t, 1).start()
        @pl.when(t != z)
        def _():
            out(t, 0).start()

    with jax.named_scope("pc_first"):
        finish_first()
        loop(0, 4, send_out)
    for kg in range(1, 4):
        with jax.named_scope(f"pc_row{kg}"):
            row_finish(kg)
    for kg in range(1, 4):
        with jax.named_scope(f"pc_blk{kg}"):
            finish(kg)
            loop(4 * kg, 4 * kg + 4, send_out)
    dkv_ref[kind, z] = final[z]

    with jax.named_scope("pe_sends"):
        own_kv.wait_send()
        drain(kv_all.at[0, 0, pl.ds(0, 15)], zkv_s)
        drain(q_rows.at[pl.ds(0, 15)], zq_s)
        drain(g_rows.at[pl.ds(0, 15)], zg_s)
        drain(kv_all.at[0, :, pl.ds(0, 15)], ag_s)
        drain(kv_all.at[0], fw_s)
        o_finish()
        dq_finish()
        drain(other, sib_s)
        drain(first_in, dir_s)
        drain(row_in.at[pl.ds(0, 3)], row_s)
        drain(block_in.at[pl.ds(0, 3)], blk_s)
    with jax.named_scope("pf_dkv"):
        drain(dkv_ref.at[0, pl.ds(0, 15)], fin_s.at[0])
        drain(dkv_ref.at[0], fin_s.at[1])
        drain(dkv_ref.at[0, pl.ds(0, 15)], fin_r.at[0])
        drain(dkv_ref.at[1], fin_r.at[1])


def deliver(o_ref, dq_ref, dkv_ref, o_hbm, dq_hbm, dk_hbm, dv_hbm, wide, narrow, sem):
    c = lax.axis_index("c")
    copies = [
        pltpu.make_async_copy(o_ref, o_hbm, sem.at[0]),
        pltpu.make_async_copy(dq_ref, dq_hbm, sem.at[1]),
        pltpu.make_async_copy(narrow.at[0], dk_hbm, sem.at[2]),
        pltpu.make_async_copy(narrow.at[1], dv_hbm, sem.at[3]),
    ]
    copies[0].start()
    copies[1].start()
    wide[...] = dkv_ref[...].astype(F32)
    for core in range(2):
        @pl.when(c == core)
        def _():
            for kind in range(2):
                for l in range(2):
                    for i in range(4):
                        rows = wide[kind, 8 * l : 8 * l + 8, 4 * core + i, :]
                        narrow[kind, l, i] = rows.astype(BF16)
    copies[2].start()
    copies[3].start()
    for copy in copies:
        copy.wait()


def on_device(q, k, v, g):
    wide = (2, 4, 8, 8, 128)
    dma = pltpu.SemaphoreType.DMA
    hbm = pl.BlockSpec(memory_space=pltpu.MemorySpace.HBM)
    vmem = pl.BlockSpec(memory_space=pltpu.VMEM)
    inputs = (q.reshape(wide), k, v, g.reshape(wide))
    o, dq, dkv = pl.pallas_call(
        kernel,
        out_shape=(
            jax.ShapeDtypeStruct(wide, BF16),
            jax.ShapeDtypeStruct(wide, BF16),
            jax.ShapeDtypeStruct((2, 16, 8, 128), BF16),
        ),
        in_specs=[hbm, hbm, hbm, hbm],
        out_specs=(hbm, hbm, vmem),
        scratch_shapes=[
            pltpu.VMEM(wide, BF16),
            pltpu.VMEM((2, 4, 8, 128), BF16),
            pltpu.VMEM((2, 4, 8, 128), BF16),
            pltpu.VMEM(wide, BF16),
            pltpu.VMEM((2, 8, 8, 128), F32),
            pltpu.VMEM((2, 8, 8, 128), BF16),
            pltpu.VMEM((16, 4, 8, 128), BF16),
            pltpu.VMEM((16, 4, 8, 128), BF16),
            pltpu.VMEM((2, 16, 16, 8, 128), BF16),
            pltpu.VMEM((8, 128), BF16),
            pltpu.VMEM((4, 128, 512), BF16),
            pltpu.VMEM((4, 128, 512), BF16),
            pltpu.VMEM((512, 128), jnp.int32),
            pltpu.VMEM((8, 128), F32),
            pltpu.VMEM((8, 128), F32),
            pltpu.VMEM((4, 128, 128), F32),
            pltpu.VMEM((4, 128, 128), F32),
            pltpu.VMEM((4, 4, 512, 128), F32),
            pltpu.VMEM((4, 512, 1024), BF16),
            pltpu.VMEM((4, 512, 1024), BF16),
            pltpu.VMEM((1024, 128), BF16),
            pltpu.VMEM((1024, 128), BF16),
            pltpu.VMEM((16, 4, 8, 128), BF16),
            pltpu.VMEM((16, 4, 8, 128), BF16),
            pltpu.VMEM((2, 4, 4, 4, 4, 8, 128), F32),
            pltpu.VMEM((4, 4, 4, 4, 8, 128), F32),
            pltpu.VMEM((4, 3, 4, 4, 8, 128), F32),
            pltpu.VMEM((4, 4, 4, 8, 128), F32),
            pltpu.VMEM((4, 3, 4, 8, 128), F32),
            pltpu.VMEM((15, 4, 8, 128), F32),
            pltpu.VMEM((16, 8, 128), BF16),
            dma((6,)),
            dma, dma((3,)), dma, dma, dma, dma, dma, dma,
            dma, dma((3,)), dma, dma((3,)),
            dma, dma, dma, dma, dma, dma,
            dma, dma((4,)), dma, dma((4,)), dma, dma((4,)), dma, dma, dma((2,)), dma((2,)),
        ],
        compiler_params=pltpu.CompilerParams(
            collective_id=1, has_side_effects=True, vmem_limit_bytes=48 * 2**20
        ),
        name="attend",
    )(*(pltpu.with_memory_space_constraint(a, pltpu.MemorySpace.HBM) for a in inputs))
    o, dq, dk, dv = pl.pallas_call(
        deliver,
        out_shape=tuple(jax.ShapeDtypeStruct(a.shape, BF16) for a in (o, dq, k, v)),
        in_specs=[hbm, hbm, vmem],
        out_specs=(hbm,) * 4,
        scratch_shapes=[
            pltpu.VMEM((2, 16, 8, 128), F32), pltpu.VMEM((2, 2, 4, 8, 128), BF16), dma((4,))
        ],
        compiler_params=pltpu.CompilerParams(vmem_limit_bytes=8 * 2**20),
        name="deliver",
    )(o, dq, dkv)
    return o.reshape(q.shape), dq.reshape(q.shape), dk, dv


def solution(mesh):
    grid = Mesh(mesh.devices.reshape(NZ, NY, NX, 2), ("z", "y", "x", "c"))
    spec = P(None, ("z", "y", "x", "c"), None, None)
    return jax.shard_map(
        on_device, mesh=grid, in_specs=(spec,) * 4, out_specs=(spec,) * 4, check_vma=False
    )
```

```python
import functools

import jax
import jax.numpy as jnp
from jax import lax
from jax.experimental import pallas as pl
from jax.experimental.pallas import tpu as pltpu
from jax.sharding import Mesh
from jax.sharding import PartitionSpec as P

MESH = pl.DeviceIdType.MESH
F32 = jnp.float32
BF16 = jnp.bfloat16
NZ, NY, NX = 16, 4, 4
MASKED = -1e30
PIECES = ((0, 7), (7, 6), (13, 3))


def nt(a, b):
    return lax.dot_general(a, b, (((1,), (1,)), ((), ())), preferred_element_type=F32)


def nn(a, b):
    return lax.dot_general(a, b, (((1,), (0,)), ((), ())), preferred_element_type=F32)


def split(a):
    high = a.astype(BF16)
    return high, (a - high.astype(F32)).astype(BF16)


def kernel(
    q_hbm, k_hbm, v_hbm, g_hbm, o_hbm, dq_hbm, dkv_ref,
    q_home, k_home, v_home, g_home, kv_wide, kv_home, q_rows, g_rows, kv_all,
    mate, keys_t, values_t, diagonal, row_delta, tops, attended_t, dq_t, scores, probs, dscores, g_twice, q_twice,
    o_rows, dq_rows, part, other, row_in, row_sum, block_in, first_in, final,
    in_sem, zkv_s, zkv_r, own_s, own_r, zq_s, zq_r, zg_s, zg_r, ag_s, ag_r, fw_s, fw_r,
    o_s, o_r, own_o, dq_s, dq_r, own_dq, sib_s, sib_r, row_s, row_r, blk_s, blk_r, dir_s, dir_r, fin_s, fin_r,
):
    z, y, x, c = (lax.axis_index(a) for a in ("z", "y", "x", "c"))
    chip = y * NX + x
    layer, group = z >> 3, z & 7
    scale = 128 ** -0.5

    def z_at(d):
        return (z + d) & 15

    def chip_at(e, sign):
        dy, dx = e >> 2, e & 3
        return (y + 4 + sign * dy) & 3, (x + 4 + sign * dx) & 3

    barrier = pltpu.get_barrier_semaphore()

    def greet(*device):
        pl.semaphore_signal(barrier, inc=1, device_id=device, device_id_type=MESH)

    for d in (8, 7, 9, 6, 10, 5, 11, 4, 12, 3, 13, 2, 14, 1, 15):
        greet(z_at(d), y, x, c)
        greet(z_at(d), y, x, 1 - c)
    for e in (10, 6, 9, 11, 14, 2, 8, 5, 7, 13, 15, 1, 3, 4, 12):
        greet(z, *chip_at(e, 1), c)
    greet(z, y, x, 1 - c)

    stage = [
        pltpu.make_async_copy(k_hbm, k_home, in_sem.at[0]),
        pltpu.make_async_copy(v_hbm, v_home, in_sem.at[1]),
        pltpu.make_async_copy(q_hbm, q_home, in_sem.at[2]),
        pltpu.make_async_copy(g_hbm, g_home, in_sem.at[3]),
        pltpu.make_async_copy(q_hbm.at[layer, :, group], q_rows.at[z], in_sem.at[4]),
        pltpu.make_async_copy(g_hbm.at[layer, :, group], g_rows.at[z], in_sem.at[5]),
    ]
    for copy in stage:
        copy.start()

    def drain(ref, sem):
        pltpu.make_async_remote_copy(
            src_ref=ref, dst_ref=ref, send_sem=sem, recv_sem=sem,
            device_id=(z, y, x, 1 - c), device_id_type=MESH,
        ).wait_recv()

    key_pos = lax.broadcasted_iota(jnp.int32, (512, 128), 0)
    lane = lax.broadcasted_iota(jnp.int32, (512, 128), 1)
    row_pos = 128 * (lane >> 5) + ((lane >> 3) & 3) + 8 * chip + 4 * c
    diagonal[...] = key_pos - row_pos
    identity = (
        lax.broadcasted_iota(jnp.int32, (128, 128), 0)
        == lax.broadcasted_iota(jnp.int32, (128, 128), 1)
    ).astype(F32).astype(BF16)

    with jax.named_scope("p0_kv"):
        stage[0].wait()
        stage[1].wait()
        for l in range(2):
            for i in range(4):
                kv_wide[l, :, i, :] = k_home[l, i].astype(F32)
                kv_wide[l, :, 4 + i, :] = v_home[l, i].astype(F32)
        kv_home[...] = kv_wide[...].astype(BF16)
        for copy in stage[2:]:
            copy.wait()
    with jax.named_scope("p1_barrier"):
        pl.semaphore_wait(barrier, 46)

    def to_z(src, dst, send, recv):
        def make(d):
            t = z_at(d)
            return pltpu.make_async_remote_copy(
                src_ref=src.at[t >> 3, :, t & 7], dst_ref=dst.at[z], send_sem=send,
                recv_sem=recv, device_id=(t, y, x, c), device_id_type=MESH,
            )
        return make

    half = pl.ds(pl.multiple_of(4 * c, 4), 4)

    def slot_of(u):
        return u + jnp.where(u < 10, 0, jnp.where(u < 13, 3, -3))

    def to_core(core, d, far):
        t = z_at(d)
        return pltpu.make_async_remote_copy(
            src_ref=kv_home.at[t >> 3, t & 7, pl.ds(4 - 4 * core, 4)],
            dst_ref=kv_all.at[1 - core, slot_of((19 - d) & 15), chip, half],
            send_sem=zkv_s, recv_sem=zkv_r.at[far],
            device_id=(t, y, x, core), device_id_type=MESH,
        )

    own_kv = pltpu.make_async_remote_copy(
        src_ref=kv_home.at[layer, group], dst_ref=mate, send_sem=own_s,
        recv_sem=own_r, device_id=(z, y, x, 1 - c), device_id_type=MESH,
    )
    zq = to_z(q_home, q_rows, zq_s, zq_r)
    zg = to_z(g_home, g_rows, zg_s, zg_r)

    def loop(low, high, body):
        def step(i, _):
            body(i)
            return 0
        lax.fori_loop(low, high, step, 0)

    def far_first(body):
        loop(1, 9, lambda i: body(9 - i))
        loop(9, 16, body)

    with jax.named_scope("p2_zstart"):
        own_kv.start()
        def send_kv(d, far):
            to_core(0, d, far).start()
            to_core(1, d, far).start()

        loop(1, 4, lambda d: (send_kv(d, 0), send_kv(16 - d, 0)))
        loop(4, 7, lambda d: (send_kv(d, 1), send_kv(16 - d, 1)))
        loop(7, 10, lambda d: send_kv(d, 2))
        loop(1, 16, lambda d: zq(d).start())
        far_first(lambda d: zg(d).start())


    def gather(n, e):
        j = jnp.where(e - 1 < chip, e - 1, e)
        block = kv_all.at[1 - c, pl.ds(*PIECES[n]), chip]
        return pltpu.make_async_remote_copy(
            src_ref=block, dst_ref=block, send_sem=ag_s,
            recv_sem=ag_r.at[n], device_id=(z, j >> 2, j & 3, c), device_id_type=MESH,
        )

    def forward(n):
        block = kv_all.at[1 - c, pl.ds(*PIECES[n])]
        return pltpu.make_async_remote_copy(
            src_ref=block, dst_ref=block, send_sem=fw_s,
            recv_sem=fw_r.at[n], device_id=(z, y, x, 1 - c), device_id_type=MESH,
        )

    with jax.named_scope("p3_zkvn"):
        own_kv.wait_recv()
        mine = pltpu.roll(kv_wide[layer, group], 4, 0)
        own_half = (lax.broadcasted_iota(jnp.int32, (8, 128), 0) >> 2) == c
        kv_all[1 - c, 3, chip] = jnp.where(own_half, mine, mate[...].astype(F32)).astype(BF16)
        drain(kv_all.at[0, 0, pl.ds(0, 6)], zkv_r.at[0])
        loop(1, 16, lambda e: gather(0, e).start())
    with jax.named_scope("p3_zkvm"):
        drain(kv_all.at[0, 0, pl.ds(0, 6)], zkv_r.at[1])
        loop(1, 16, lambda e: gather(1, e).start())
    with jax.named_scope("p3_zkvf"):
        drain(kv_all.at[0, 0, pl.ds(0, 3)], zkv_r.at[2])
        loop(1, 16, lambda e: gather(2, e).start())

    for n in range(3):
        with jax.named_scope(f"p4_ag{n}"):
            drain(kv_all.at[1 - c, pl.ds(*PIECES[n]), pl.ds(0, 15)], ag_r.at[n])
            forward(n).start()
    def of_core(core, body):
        @pl.when(c == core)
        def _():
            body()

    def from_sibling():
        for n in range(3):
            drain(kv_all.at[c, pl.ds(*PIECES[n])], fw_r.at[n])

    with jax.named_scope("p6_keys"):
        of_core(0, from_sibling)

    def plane_group(kind, kg):
        return jnp.concatenate(
            [kv_all[kind, slot_of((4 * kg + i + 19 - z) & 15)].reshape(128, 128) for i in range(4)], axis=0
        )

    with jax.named_scope("p8_qwait"):
        drain(q_rows.at[pl.ds(0, 15)], zq_r)

    def home(rows, out, send, recv, own_sem):
        def make(t):
            return pltpu.make_async_remote_copy(
                src_ref=rows.at[t], dst_ref=out.at[layer, :, group], send_sem=send,
                recv_sem=recv, device_id=(t, y, x, c), device_id_type=MESH,
            )
        own = pltpu.make_async_copy(rows.at[z], out.at[layer, :, group], own_sem)
        def start():
            far_first(lambda d: make(z_at(d)).start())
            own.start()
        def start_at(t):
            @pl.when(t != z)
            def _():
                make(t).start()
            @pl.when(t == z)
            def _():
                own.start()
        def finish():
            drain(rows.at[pl.ds(0, 15)], send)
            drain(rows.at[pl.ds(0, 15)], recv)
            own.wait()
        return start, start_at, finish

    o_start, _, o_finish = home(o_rows, o_hbm, o_s, o_r, own_o)
    _, dq_start, dq_finish = home(dq_rows, dq_hbm, dq_s, dq_r, own_dq)

    factor_2 = scale * 1.4426950408889634

    def pair(rg):
        return slice(256 * rg, 256 * rg + 256)

    def scores_of(rg):
        lanes = pair(rg)
        q = q_rows[4 * rg : 4 * rg + 4].astype(F32).reshape(128, 128).astype(BF16)
        q_twice[lanes] = jnp.concatenate([q, q], axis=0)
        top = jnp.full((8, 128), MASKED, F32)
        for kg in range(rg + 1):
            s = nt(plane_group(0, kg), q) * factor_2
            if kg == rg:
                s = jnp.where(diagonal[...] <= 0, s, MASKED)
            scores[rg, kg] = s
            top = jnp.maximum(top, jnp.max(s.reshape(64, 8, 128), axis=0))
        return jnp.max(top, axis=0, keepdims=True)

    def forward_of(rg, top):
        lanes = pair(rg)
        total = jnp.zeros((8, 128), F32)
        for kg in range(rg + 1):
            e = jnp.exp2(scores[rg, kg] - top)
            scores[rg, kg] = e
            total = total + jnp.sum(e.reshape(64, 8, 128), axis=0)
        inverse = 1.0 / jnp.sum(total, axis=0, keepdims=True)
        acc = jnp.zeros((128, 256), F32)
        for kg in range(rg + 1):
            p = scores[rg, kg] * inverse
            p2 = jnp.concatenate(split(p), axis=1)
            probs[kg, :, lanes] = p2
            scores[rg, kg] = p
            acc = acc + nn(values_t[kg], p2)
        o_t = acc[:, :128] + acc[:, 128:]
        attended_t[rg] = o_t.astype(BF16).astype(F32)
        o_rows[4 * rg : 4 * rg + 4] = o_t.T.reshape(4, 4, 8, 128).astype(BF16)

    def deltas(rg):
        g = g_rows[4 * rg : 4 * rg + 4].astype(F32).reshape(128, 128).astype(BF16)
        g_twice[pair(rg)] = jnp.concatenate([g, g], axis=0)
        delta = nt(identity, g) * attended_t[rg]
        row_delta[rg : rg + 1] = jnp.sum(delta, axis=0, keepdims=True)

    def backward_of(kg):
        for rg in range(kg, 4):
            g = g_twice[256 * rg : 256 * rg + 128]
            ds = scores[rg, kg] * (nt(plane_group(1, kg), g) - row_delta[rg : rg + 1])
            ds2 = jnp.concatenate(split(ds), axis=1)
            dscores[kg, :, pair(rg)] = ds2
            term = nn(keys_t[kg], ds2)
            term = term[:, :128] + term[:, 128:]
            dq_t[rg] = dq_t[rg] + term if kg else term
        dq_rows[4 * kg : 4 * kg + 4] = (dq_t[kg] * scale).T.reshape(4, 4, 8, 128).astype(BF16)
        part[0, kg] = key_sum(kg, kg, 4)
        part[1, kg] = value_sum(kg, kg, 4)

    def value_sum(kg, low, high):
        lanes = slice(256 * low, 256 * high)
        return nn(probs[kg, :, lanes], g_twice[lanes]).reshape(4, 4, 4, 8, 128)

    def key_sum(kg, low, high):
        lanes = slice(256 * low, 256 * high)
        dk = nn(dscores[kg, :, lanes], q_twice[lanes])
        return jnp.swapaxes(dk.reshape(4, 4, 4, 8, 128), 1, 2)

    kind = 1 - c
    along = jnp.where(c == 0, y, x)
    across = jnp.where(c == 0, x, y)

    def sibling(kg):
        return pltpu.make_async_remote_copy(
            src_ref=part.at[c, kg], dst_ref=other.at[kg], send_sem=sib_s,
            recv_sem=sib_r.at[kg], device_id=(z, y, x, 1 - c), device_id_type=MESH,
        )

    def row_send(kg, a):
        t = (along + a) & 3
        return pltpu.make_async_remote_copy(
            src_ref=part.at[kind, kg, :, t], dst_ref=row_in.at[kg, a - 1], send_sem=row_s,
            recv_sem=row_r.at[kg],
            device_id=(z, jnp.where(c == 0, t, y), jnp.where(c == 0, x, t), c), device_id_type=MESH,
        )

    def block_send(kg, a):
        t = (across + a) & 3
        return pltpu.make_async_remote_copy(
            src_ref=row_sum.at[kg, :, t], dst_ref=block_in.at[kg, a - 1], send_sem=blk_s,
            recv_sem=blk_r.at[kg],
            device_id=(z, jnp.where(c == 0, y, t), jnp.where(c == 0, t, x), c), device_id_type=MESH,
        )

    def direct_send(j):
        yy, xx = j >> 2, j & 3
        a, b = jnp.where(c == 0, yy, xx), jnp.where(c == 0, xx, yy)
        return pltpu.make_async_remote_copy(
            src_ref=part.at[kind, 0, :, a, b], dst_ref=first_in.at[(j - chip + 15) & 15],
            send_sem=dir_s, recv_sem=dir_r, device_id=(z, yy, xx, c), device_id_type=MESH,
        )

    def combine(kg):
        sibling(kg).wait_recv()
        part[kind, kg] = part[kind, kg] + other[kg]
        if kg:
            loop(1, 4, lambda a: row_send(kg, a).start())
        else:
            loop(1, 16, lambda e: direct_send(jnp.where(e - 1 < chip, e - 1, e)).start())

    with jax.named_scope("p9_scores"):
        for rg in range(4):
            tops[rg : rg + 1] = scores_of(rg)
        for kg in range(4):
            keys_t[kg] = nt(identity, plane_group(0, kg)).astype(BF16)
    with jax.named_scope("p9_values"):
        of_core(1, from_sibling)
    with jax.named_scope("p9_fwd"):
        for kg in range(4):
            values_t[kg] = nt(identity, plane_group(1, kg)).astype(BF16)
        for rg in range(4):
            forward_of(rg, tops[rg : rg + 1])

    with jax.named_scope("pa_osend"):
        o_start()
        drain(g_rows.at[pl.ds(0, 15)], zg_r)
    for kg in range(4):
        with jax.named_scope(f"p9_bwd{kg}"):
            if kg == 0:
                for rg in range(4):
                    deltas(rg)
            backward_of(kg)
        with jax.named_scope(f"pa_comb{kg}"):
            sibling(kg).start()
            loop(4 * kg, 4 * kg + 4, dq_start)
            if kg:
                combine(kg - 1)
    with jax.named_scope("pb_combine"):
        combine(3)

    def row_finish(kg):
        drain(row_in.at[kg], row_r.at[kg])
        total = part[kind, kg, :, along]
        for a in range(3):
            total = total + row_in[kg, a]
        row_sum[kg] = total
        loop(1, 4, lambda a: block_send(kg, a).start())

    factor = jnp.where(c == 0, 1.0, scale).astype(F32)

    def finish_first():
        drain(first_in, dir_r)
        total = part[kind, 0, :, along, across]
        for e in range(15):
            total = total + first_in[e]
        final[pl.ds(0, 4)] = (total * factor).astype(BF16)

    def finish(kg):
        drain(block_in.at[kg], blk_r.at[kg])
        total = row_sum[kg, :, across]
        for a in range(3):
            total = total + block_in[kg, a]
        final[pl.ds(4 * kg, 4)] = (total * factor).astype(BF16)

    def out(t, other_core):
        core = 1 - c if other_core else c
        return pltpu.make_async_remote_copy(
            src_ref=final.at[t], dst_ref=dkv_ref.at[kind, z], send_sem=fin_s.at[other_core],
            recv_sem=fin_r.at[other_core], device_id=(t, y, x, core), device_id_type=MESH,
        )

    def send_out(t):
        out(t, 1).start()
        @pl.when(t != z)
        def _():
            out(t, 0).start()

    with jax.named_scope("pc_first"):
        finish_first()
        loop(0, 4, send_out)
    for kg in range(1, 4):
        with jax.named_scope(f"pc_row{kg}"):
            row_finish(kg)
    for kg in range(1, 4):
        with jax.named_scope(f"pc_blk{kg}"):
            finish(kg)
            loop(4 * kg, 4 * kg + 4, send_out)
    dkv_ref[kind, z] = final[z]

    with jax.named_scope("pe_sends"):
        own_kv.wait_send()
        drain(kv_all.at[0, 0, pl.ds(0, 15)], zkv_s)
        drain(q_rows.at[pl.ds(0, 15)], zq_s)
        drain(g_rows.at[pl.ds(0, 15)], zg_s)
        drain(kv_all.at[0, :, pl.ds(0, 15)], ag_s)
        drain(kv_all.at[0], fw_s)
        o_finish()
        dq_finish()
        drain(other, sib_s)
        drain(first_in, dir_s)
        drain(row_in.at[pl.ds(0, 3)], row_s)
        drain(block_in.at[pl.ds(0, 3)], blk_s)
    with jax.named_scope("pf_dkv"):
        drain(dkv_ref.at[0, pl.ds(0, 15)], fin_s.at[0])
        drain(dkv_ref.at[0], fin_s.at[1])
        drain(dkv_ref.at[0, pl.ds(0, 15)], fin_r.at[0])
        drain(dkv_ref.at[1], fin_r.at[1])


def deliver(o_ref, dq_ref, dkv_ref, o_hbm, dq_hbm, dk_hbm, dv_hbm, wide, narrow, sem):
    c = lax.axis_index("c")
    copies = [
        pltpu.make_async_copy(o_ref, o_hbm, sem.at[0]),
        pltpu.make_async_copy(dq_ref, dq_hbm, sem.at[1]),
        pltpu.make_async_copy(narrow.at[0], dk_hbm, sem.at[2]),
        pltpu.make_async_copy(narrow.at[1], dv_hbm, sem.at[3]),
    ]
    copies[0].start()
    copies[1].start()
    wide[...] = dkv_ref[...].astype(F32)
    for core in range(2):
        @pl.when(c == core)
        def _():
            for kind in range(2):
                for l in range(2):
                    for i in range(4):
                        rows = wide[kind, 8 * l : 8 * l + 8, 4 * core + i, :]
                        narrow[kind, l, i] = rows.astype(BF16)
    copies[2].start()
    copies[3].start()
    for copy in copies:
        copy.wait()


def on_device(q, k, v, g):
    wide = (2, 4, 8, 8, 128)
    dma = pltpu.SemaphoreType.DMA
    hbm = pl.BlockSpec(memory_space=pltpu.MemorySpace.HBM)
    vmem = pl.BlockSpec(memory_space=pltpu.VMEM)
    inputs = (q.reshape(wide), k, v, g.reshape(wide))
    o, dq, dkv = pl.pallas_call(
        kernel,
        out_shape=(
            jax.ShapeDtypeStruct(wide, BF16),
            jax.ShapeDtypeStruct(wide, BF16),
            jax.ShapeDtypeStruct((2, 16, 8, 128), BF16),
        ),
        in_specs=[hbm, hbm, hbm, hbm],
        out_specs=(hbm, hbm, vmem),
        scratch_shapes=[
            pltpu.VMEM(wide, BF16),
            pltpu.VMEM((2, 4, 8, 128), BF16),
            pltpu.VMEM((2, 4, 8, 128), BF16),
            pltpu.VMEM(wide, BF16),
            pltpu.VMEM((2, 8, 8, 128), F32),
            pltpu.VMEM((2, 8, 8, 128), BF16),
            pltpu.VMEM((16, 4, 8, 128), BF16),
            pltpu.VMEM((16, 4, 8, 128), BF16),
            pltpu.VMEM((2, 16, 16, 8, 128), BF16),
            pltpu.VMEM((8, 128), BF16),
            pltpu.VMEM((4, 128, 512), BF16),
            pltpu.VMEM((4, 128, 512), BF16),
            pltpu.VMEM((512, 128), jnp.int32),
            pltpu.VMEM((8, 128), F32),
            pltpu.VMEM((8, 128), F32),
            pltpu.VMEM((4, 128, 128), F32),
            pltpu.VMEM((4, 128, 128), F32),
            pltpu.VMEM((4, 4, 512, 128), F32),
            pltpu.VMEM((4, 512, 1024), BF16),
            pltpu.VMEM((4, 512, 1024), BF16),
            pltpu.VMEM((1024, 128), BF16),
            pltpu.VMEM((1024, 128), BF16),
            pltpu.VMEM((16, 4, 8, 128), BF16),
            pltpu.VMEM((16, 4, 8, 128), BF16),
            pltpu.VMEM((2, 4, 4, 4, 4, 8, 128), F32),
            pltpu.VMEM((4, 4, 4, 4, 8, 128), F32),
            pltpu.VMEM((4, 3, 4, 4, 8, 128), F32),
            pltpu.VMEM((4, 4, 4, 8, 128), F32),
            pltpu.VMEM((4, 3, 4, 8, 128), F32),
            pltpu.VMEM((15, 4, 8, 128), F32),
            pltpu.VMEM((16, 8, 128), BF16),
            dma((6,)),
            dma, dma((3,)), dma, dma, dma, dma, dma, dma,
            dma, dma((3,)), dma, dma((3,)),
            dma, dma, dma, dma, dma, dma,
            dma, dma((4,)), dma, dma((4,)), dma, dma((4,)), dma, dma, dma((2,)), dma((2,)),
        ],
        compiler_params=pltpu.CompilerParams(
            collective_id=1, has_side_effects=True, vmem_limit_bytes=48 * 2**20
        ),
        name="attend",
    )(*(pltpu.with_memory_space_constraint(a, pltpu.MemorySpace.HBM) for a in inputs))
    o, dq, dk, dv = pl.pallas_call(
        deliver,
        out_shape=tuple(jax.ShapeDtypeStruct(a.shape, BF16) for a in (o, dq, k, v)),
        in_specs=[hbm, hbm, vmem],
        out_specs=(hbm,) * 4,
        scratch_shapes=[
            pltpu.VMEM((2, 16, 8, 128), F32), pltpu.VMEM((2, 2, 4, 8, 128), BF16), dma((4,))
        ],
        compiler_params=pltpu.CompilerParams(vmem_limit_bytes=8 * 2**20),
        name="deliver",
    )(o, dq, dkv)
    return o.reshape(q.shape), dq.reshape(q.shape), dk, dv


def solution(mesh):
    grid = Mesh(mesh.devices.reshape(NZ, NY, NX, 2), ("z", "y", "x", "c"))
    spec = P(None, ("z", "y", "x", "c"), None, None)
    return jax.shard_map(
        on_device, mesh=grid, in_specs=(spec,) * 4, out_specs=(spec,) * 4, check_vma=False
    )
```

```python
import functools

import jax
import jax.numpy as jnp
from jax import lax
from jax.experimental import pallas as pl
from jax.experimental.pallas import tpu as pltpu
from jax.sharding import Mesh
from jax.sharding import PartitionSpec as P

MESH = pl.DeviceIdType.MESH
F32 = jnp.float32
BF16 = jnp.bfloat16
NZ, NY, NX = 16, 4, 4
MASKED = -1e30
PIECES = ((0, 7), (7, 6), (13, 3))


def nt(a, b):
    return lax.dot_general(a, b, (((1,), (1,)), ((), ())), preferred_element_type=F32)


def nn(a, b):
    return lax.dot_general(a, b, (((1,), (0,)), ((), ())), preferred_element_type=F32)


def split(a):
    high = a.astype(BF16)
    return high, (a - high.astype(F32)).astype(BF16)


def kernel(
    q_hbm, k_hbm, v_hbm, g_hbm, o_hbm, dq_hbm, dkv_ref,
    q_home, k_home, v_home, g_home, kv_wide, kv_home, q_rows, g_rows, kv_all,
    mate, keys_t, values_t, diagonal, row_delta, tops, attended_t, dq_t, scores, probs, dscores, g_twice, q_twice,
    o_rows, dq_rows, part, other, row_in, row_sum, block_in, first_in, final,
    in_sem, zkv_s, zkv_r, own_s, own_r, zq_s, zq_r, zg_s, zg_r, ag_s, ag_r, fw_s, fw_r,
    o_s, o_r, own_o, dq_s, dq_r, own_dq, sib_s, sib_r, row_s, row_r, blk_s, blk_r, dir_s, dir_r, fin_s, fin_r,
):
    z, y, x, c = (lax.axis_index(a) for a in ("z", "y", "x", "c"))
    chip = y * NX + x
    layer, group = z >> 3, z & 7
    scale = 128 ** -0.5

    def z_at(d):
        return (z + d) & 15

    def chip_at(e, sign):
        dy, dx = e >> 2, e & 3
        return (y + 4 + sign * dy) & 3, (x + 4 + sign * dx) & 3

    barrier = pltpu.get_barrier_semaphore()

    def greet(*device):
        pl.semaphore_signal(barrier, inc=1, device_id=device, device_id_type=MESH)

    for d in (8, 7, 9, 6, 10, 5, 11, 4, 12, 3, 13, 2, 14, 1, 15):
        greet(z_at(d), y, x, c)
        greet(z_at(d), y, x, 1 - c)
    for e in (10, 6, 9, 11, 14, 2, 8, 5, 7, 13, 15, 1, 3, 4, 12):
        greet(z, *chip_at(e, 1), c)
    greet(z, y, x, 1 - c)

    stage = [
        pltpu.make_async_copy(k_hbm, k_home, in_sem.at[0]),
        pltpu.make_async_copy(v_hbm, v_home, in_sem.at[1]),
        pltpu.make_async_copy(q_hbm, q_home, in_sem.at[2]),
        pltpu.make_async_copy(g_hbm, g_home, in_sem.at[3]),
        pltpu.make_async_copy(q_hbm.at[layer, :, group], q_rows.at[z], in_sem.at[4]),
        pltpu.make_async_copy(g_hbm.at[layer, :, group], g_rows.at[z], in_sem.at[5]),
    ]
    for copy in stage:
        copy.start()

    def drain(ref, sem):
        pltpu.make_async_remote_copy(
            src_ref=ref, dst_ref=ref, send_sem=sem, recv_sem=sem,
            device_id=(z, y, x, 1 - c), device_id_type=MESH,
        ).wait_recv()

    key_pos = lax.broadcasted_iota(jnp.int32, (512, 128), 0)
    lane = lax.broadcasted_iota(jnp.int32, (512, 128), 1)
    row_pos = 128 * (lane >> 5) + ((lane >> 3) & 3) + 8 * chip + 4 * c
    diagonal[...] = key_pos - row_pos
    identity = (
        lax.broadcasted_iota(jnp.int32, (128, 128), 0)
        == lax.broadcasted_iota(jnp.int32, (128, 128), 1)
    ).astype(F32).astype(BF16)

    with jax.named_scope("p0_kv"):
        stage[0].wait()
        stage[1].wait()
        for l in range(2):
            for i in range(4):
                kv_wide[l, :, i, :] = k_home[l, i].astype(F32)
                kv_wide[l, :, 4 + i, :] = v_home[l, i].astype(F32)
        kv_home[...] = kv_wide[...].astype(BF16)
        for copy in stage[2:]:
            copy.wait()
    with jax.named_scope("p1_barrier"):
        pl.semaphore_wait(barrier, 46)

    def to_z(src, dst, send, recv):
        def make(d):
            t = z_at(d)
            return pltpu.make_async_remote_copy(
                src_ref=src.at[t >> 3, :, t & 7], dst_ref=dst.at[z], send_sem=send,
                recv_sem=recv, device_id=(t, y, x, c), device_id_type=MESH,
            )
        return make

    half = pl.ds(pl.multiple_of(4 * c, 4), 4)

    def slot_of(u):
        return u + jnp.where(u < 10, 0, jnp.where(u < 13, 3, -3))

    def to_core(core, d, far):
        t = z_at(d)
        return pltpu.make_async_remote_copy(
            src_ref=kv_home.at[t >> 3, t & 7, pl.ds(4 - 4 * core, 4)],
            dst_ref=kv_all.at[1 - core, slot_of((19 - d) & 15), chip, half],
            send_sem=zkv_s, recv_sem=zkv_r.at[far],
            device_id=(t, y, x, core), device_id_type=MESH,
        )

    own_kv = pltpu.make_async_remote_copy(
        src_ref=kv_home.at[layer, group], dst_ref=mate, send_sem=own_s,
        recv_sem=own_r, device_id=(z, y, x, 1 - c), device_id_type=MESH,
    )
    zq = to_z(q_home, q_rows, zq_s, zq_r)
    zg = to_z(g_home, g_rows, zg_s, zg_r)

    def loop(low, high, body):
        def step(i, _):
            body(i)
            return 0
        lax.fori_loop(low, high, step, 0)

    def far_first(body):
        loop(1, 9, lambda i: body(9 - i))
        loop(9, 16, body)

    with jax.named_scope("p2_zstart"):
        own_kv.start()
        def send_kv(d, far):
            to_core(0, d, far).start()
            to_core(1, d, far).start()

        loop(1, 4, lambda d: (send_kv(d, 0), send_kv(16 - d, 0)))
        loop(4, 7, lambda d: (send_kv(d, 1), send_kv(16 - d, 1)))
        loop(7, 10, lambda d: send_kv(d, 2))
        loop(1, 16, lambda d: zq(d).start())
        far_first(lambda d: zg(d).start())


    def gather(n, e):
        j = jnp.where(e - 1 < chip, e - 1, e)
        block = kv_all.at[1 - c, pl.ds(*PIECES[n]), chip]
        return pltpu.make_async_remote_copy(
            src_ref=block, dst_ref=block, send_sem=ag_s,
            recv_sem=ag_r.at[n], device_id=(z, j >> 2, j & 3, c), device_id_type=MESH,
        )

    def forward(n):
        block = kv_all.at[1 - c, pl.ds(*PIECES[n])]
        return pltpu.make_async_remote_copy(
            src_ref=block, dst_ref=block, send_sem=fw_s,
            recv_sem=fw_r.at[n], device_id=(z, y, x, 1 - c), device_id_type=MESH,
        )

    with jax.named_scope("p3_zkvn"):
        own_kv.wait_recv()
        mine = pltpu.roll(kv_wide[layer, group], 4, 0)
        own_half = (lax.broadcasted_iota(jnp.int32, (8, 128), 0) >> 2) == c
        kv_all[1 - c, 3, chip] = jnp.where(own_half, mine, mate[...].astype(F32)).astype(BF16)
        drain(kv_all.at[0, 0, pl.ds(0, 6)], zkv_r.at[0])
        loop(1, 16, lambda e: gather(0, e).start())
    with jax.named_scope("p3_zkvm"):
        drain(kv_all.at[0, 0, pl.ds(0, 6)], zkv_r.at[1])
        loop(1, 16, lambda e: gather(1, e).start())
    with jax.named_scope("p3_zkvf"):
        drain(kv_all.at[0, 0, pl.ds(0, 3)], zkv_r.at[2])
        loop(1, 16, lambda e: gather(2, e).start())

    for n in range(3):
        with jax.named_scope(f"p4_ag{n}"):
            drain(kv_all.at[1 - c, pl.ds(*PIECES[n]), pl.ds(0, 15)], ag_r.at[n])
            forward(n).start()
    def of_core(core, body):
        @pl.when(c == core)
        def _():
            body()

    def from_sibling():
        for n in range(3):
            drain(kv_all.at[c, pl.ds(*PIECES[n])], fw_r.at[n])

    with jax.named_scope("p6_keys"):
        of_core(0, from_sibling)

    def plane_group(kind, kg):
        return jnp.concatenate(
            [kv_all[kind, slot_of((4 * kg + i + 19 - z) & 15)].reshape(128, 128) for i in range(4)], axis=0
        )

    with jax.named_scope("p8_qwait"):
        drain(q_rows.at[pl.ds(0, 15)], zq_r)

    def home(rows, out, send, recv, own_sem):
        def make(t):
            return pltpu.make_async_remote_copy(
                src_ref=rows.at[t], dst_ref=out.at[layer, :, group], send_sem=send,
                recv_sem=recv, device_id=(t, y, x, c), device_id_type=MESH,
            )
        own = pltpu.make_async_copy(rows.at[z], out.at[layer, :, group], own_sem)
        def start():
            far_first(lambda d: make(z_at(d)).start())
            own.start()
        def start_at(t):
            @pl.when(t != z)
            def _():
                make(t).start()
            @pl.when(t == z)
            def _():
                own.start()
        def finish():
            drain(rows.at[pl.ds(0, 15)], send)
            drain(rows.at[pl.ds(0, 15)], recv)
            own.wait()
        return start, start_at, finish

    o_start, _, o_finish = home(o_rows, o_hbm, o_s, o_r, own_o)
    _, dq_start, dq_finish = home(dq_rows, dq_hbm, dq_s, dq_r, own_dq)

    factor_2 = scale * 1.4426950408889634

    def pair(rg):
        return slice(256 * rg, 256 * rg + 256)

    def scores_of(rg):
        lanes = pair(rg)
        q = q_rows[4 * rg : 4 * rg + 4].astype(F32).reshape(128, 128).astype(BF16)
        q_twice[lanes] = jnp.concatenate([q, q], axis=0)
        top = jnp.full((8, 128), MASKED, F32)
        for kg in range(rg + 1):
            s = nt(plane_group(0, kg), q) * factor_2
            if kg == rg:
                s = jnp.where(diagonal[...] <= 0, s, MASKED)
            scores[rg, kg] = s
            top = jnp.maximum(top, jnp.max(s.reshape(64, 8, 128), axis=0))
        return jnp.max(top, axis=0, keepdims=True)

    def forward_of(rg, top):
        lanes = pair(rg)
        total = jnp.zeros((8, 128), F32)
        for kg in range(rg + 1):
            e = jnp.exp2(scores[rg, kg] - top)
            scores[rg, kg] = e
            total = total + jnp.sum(e.reshape(64, 8, 128), axis=0)
        inverse = 1.0 / jnp.sum(total, axis=0, keepdims=True)
        acc = jnp.zeros((128, 256), F32)
        for kg in range(rg + 1):
            p = scores[rg, kg] * inverse
            p2 = jnp.concatenate(split(p), axis=1)
            probs[kg, :, lanes] = p2
            scores[rg, kg] = p
            acc = acc + nn(values_t[kg], p2)
        o_t = acc[:, :128] + acc[:, 128:]
        attended_t[rg] = o_t.astype(BF16).astype(F32)
        o_rows[4 * rg : 4 * rg + 4] = o_t.T.reshape(4, 4, 8, 128).astype(BF16)

    def deltas(rg):
        g = g_rows[4 * rg : 4 * rg + 4].astype(F32).reshape(128, 128).astype(BF16)
        g_twice[pair(rg)] = jnp.concatenate([g, g], axis=0)
        delta = nt(identity, g) * attended_t[rg]
        row_delta[rg : rg + 1] = jnp.sum(delta, axis=0, keepdims=True)

    def backward_of(kg):
        for rg in range(kg, 4):
            g = g_twice[256 * rg : 256 * rg + 128]
            ds = scores[rg, kg] * (nt(plane_group(1, kg), g) - row_delta[rg : rg + 1])
            ds2 = jnp.concatenate(split(ds), axis=1)
            dscores[kg, :, pair(rg)] = ds2
            term = nn(keys_t[kg], ds2)
            term = term[:, :128] + term[:, 128:]
            dq_t[rg] = dq_t[rg] + term if kg else term
        dq_rows[4 * kg : 4 * kg + 4] = (dq_t[kg] * scale).T.reshape(4, 4, 8, 128).astype(BF16)
        part[0, kg] = key_sum(kg, kg, 4)
        part[1, kg] = value_sum(kg, kg, 4)

    def value_sum(kg, low, high):
        lanes = slice(256 * low, 256 * high)
        return nn(probs[kg, :, lanes], g_twice[lanes]).reshape(4, 4, 4, 8, 128)

    def key_sum(kg, low, high):
        lanes = slice(256 * low, 256 * high)
        dk = nn(dscores[kg, :, lanes], q_twice[lanes])
        return jnp.swapaxes(dk.reshape(4, 4, 4, 8, 128), 1, 2)

    kind = 1 - c
    along = jnp.where(c == 0, y, x)
    across = jnp.where(c == 0, x, y)

    def sibling(kg):
        return pltpu.make_async_remote_copy(
            src_ref=part.at[c, kg], dst_ref=other.at[kg], send_sem=sib_s,
            recv_sem=sib_r.at[kg], device_id=(z, y, x, 1 - c), device_id_type=MESH,
        )

    def row_send(kg, a):
        t = (along + a) & 3
        return pltpu.make_async_remote_copy(
            src_ref=part.at[kind, kg, :, t], dst_ref=row_in.at[kg, a - 1], send_sem=row_s,
            recv_sem=row_r.at[kg],
            device_id=(z, jnp.where(c == 0, t, y), jnp.where(c == 0, x, t), c), device_id_type=MESH,
        )

    def block_send(kg, a):
        t = (across + a) & 3
        return pltpu.make_async_remote_copy(
            src_ref=row_sum.at[kg, :, t], dst_ref=block_in.at[kg, a - 1], send_sem=blk_s,
            recv_sem=blk_r.at[kg],
            device_id=(z, jnp.where(c == 0, y, t), jnp.where(c == 0, t, x), c), device_id_type=MESH,
        )

    def direct_send(j):
        yy, xx = j >> 2, j & 3
        a, b = jnp.where(c == 0, yy, xx), jnp.where(c == 0, xx, yy)
        return pltpu.make_async_remote_copy(
            src_ref=part.at[kind, 0, :, a, b], dst_ref=first_in.at[(j - chip + 15) & 15],
            send_sem=dir_s, recv_sem=dir_r, device_id=(z, yy, xx, c), device_id_type=MESH,
        )

    def combine(kg):
        sibling(kg).wait_recv()
        part[kind, kg] = part[kind, kg] + other[kg]
        if kg:
            loop(1, 4, lambda a: row_send(kg, a).start())
        else:
            loop(1, 16, lambda e: direct_send(jnp.where(e - 1 < chip, e - 1, e)).start())

    with jax.named_scope("p9_scores"):
        for rg in range(4):
            tops[rg : rg + 1] = scores_of(rg)
        for kg in range(4):
            keys_t[kg] = nt(identity, plane_group(0, kg)).astype(BF16)
    with jax.named_scope("p9_values"):
        of_core(1, from_sibling)
    with jax.named_scope("p9_fwd"):
        for kg in range(4):
            values_t[kg] = nt(identity, plane_group(1, kg)).astype(BF16)
        for rg in range(4):
            forward_of(rg, tops[rg : rg + 1])

    with jax.named_scope("pa_osend"):
        o_start()
        drain(g_rows.at[pl.ds(0, 15)], zg_r)
    for kg in range(4):
        with jax.named_scope(f"p9_bwd{kg}"):
            if kg == 0:
                for rg in range(4):
                    deltas(rg)
            backward_of(kg)
        with jax.named_scope(f"pa_comb{kg}"):
            sibling(kg).start()
            loop(4 * kg, 4 * kg + 4, dq_start)
            if kg:
                combine(kg - 1)
    with jax.named_scope("pb_combine"):
        combine(3)

    def row_finish(kg):
        drain(row_in.at[kg], row_r.at[kg])
        total = part[kind, kg, :, along]
        for a in range(3):
            total = total + row_in[kg, a]
        row_sum[kg] = total
        loop(1, 4, lambda a: block_send(kg, a).start())

    factor = jnp.where(c == 0, 1.0, scale).astype(F32)

    def finish_first():
        drain(first_in, dir_r)
        total = part[kind, 0, :, along, across]
        for e in range(15):
            total = total + first_in[e]
        final[pl.ds(0, 4)] = (total * factor).astype(BF16)

    def finish(kg):
        drain(block_in.at[kg], blk_r.at[kg])
        total = row_sum[kg, :, across]
        for a in range(3):
            total = total + block_in[kg, a]
        final[pl.ds(4 * kg, 4)] = (total * factor).astype(BF16)

    def out(t, other_core):
        core = 1 - c if other_core else c
        rows = pl.ds(pl.multiple_of(4 * core, 4), 4)
        return pltpu.make_async_remote_copy(
            src_ref=final.at[t, rows], dst_ref=dkv_ref.at[kind, z, rows], send_sem=fin_s.at[other_core],
            recv_sem=fin_r.at[other_core], device_id=(t, y, x, core), device_id_type=MESH,
        )

    def send_out(t):
        out(t, 1).start()
        @pl.when(t != z)
        def _():
            out(t, 0).start()

    with jax.named_scope("pc_first"):
        finish_first()
        loop(0, 4, send_out)
    for kg in range(1, 4):
        with jax.named_scope(f"pc_row{kg}"):
            row_finish(kg)
    for kg in range(1, 4):
        with jax.named_scope(f"pc_blk{kg}"):
            finish(kg)
            loop(4 * kg, 4 * kg + 4, send_out)
    dkv_ref[kind, z] = final[z]

    with jax.named_scope("pe_sends"):
        own_kv.wait_send()
        drain(kv_all.at[0, 0, pl.ds(0, 15)], zkv_s)
        drain(q_rows.at[pl.ds(0, 15)], zq_s)
        drain(g_rows.at[pl.ds(0, 15)], zg_s)
        drain(kv_all.at[0, :, pl.ds(0, 15)], ag_s)
        drain(kv_all.at[0], fw_s)
        o_finish()
        dq_finish()
        drain(other, sib_s)
        drain(first_in, dir_s)
        drain(row_in.at[pl.ds(0, 3)], row_s)
        drain(block_in.at[pl.ds(0, 3)], blk_s)
    with jax.named_scope("pf_dkv"):
        for sem in (fin_s, fin_r):
            drain(dkv_ref.at[0, pl.ds(0, 15), pl.ds(0, 4)], sem.at[0])
            drain(dkv_ref.at[1, :, pl.ds(0, 4)], sem.at[1])


def deliver(o_ref, dq_ref, dkv_ref, o_hbm, dq_hbm, dk_hbm, dv_hbm, wide, narrow, sem):
    c = lax.axis_index("c")
    copies = [
        pltpu.make_async_copy(o_ref, o_hbm, sem.at[0]),
        pltpu.make_async_copy(dq_ref, dq_hbm, sem.at[1]),
        pltpu.make_async_copy(narrow.at[0], dk_hbm, sem.at[2]),
        pltpu.make_async_copy(narrow.at[1], dv_hbm, sem.at[3]),
    ]
    copies[0].start()
    copies[1].start()
    wide[...] = dkv_ref[...].astype(F32)
    for core in range(2):
        @pl.when(c == core)
        def _():
            for kind in range(2):
                for l in range(2):
                    for i in range(4):
                        rows = wide[kind, 8 * l : 8 * l + 8, 4 * core + i, :]
                        narrow[kind, l, i] = rows.astype(BF16)
    copies[2].start()
    copies[3].start()
    for copy in copies:
        copy.wait()


def on_device(q, k, v, g):
    wide = (2, 4, 8, 8, 128)
    dma = pltpu.SemaphoreType.DMA
    hbm = pl.BlockSpec(memory_space=pltpu.MemorySpace.HBM)
    vmem = pl.BlockSpec(memory_space=pltpu.VMEM)
    inputs = (q.reshape(wide), k, v, g.reshape(wide))
    o, dq, dkv = pl.pallas_call(
        kernel,
        out_shape=(
            jax.ShapeDtypeStruct(wide, BF16),
            jax.ShapeDtypeStruct(wide, BF16),
            jax.ShapeDtypeStruct((2, 16, 8, 128), BF16),
        ),
        in_specs=[hbm, hbm, hbm, hbm],
        out_specs=(hbm, hbm, vmem),
        scratch_shapes=[
            pltpu.VMEM(wide, BF16),
            pltpu.VMEM((2, 4, 8, 128), BF16),
            pltpu.VMEM((2, 4, 8, 128), BF16),
            pltpu.VMEM(wide, BF16),
            pltpu.VMEM((2, 8, 8, 128), F32),
            pltpu.VMEM((2, 8, 8, 128), BF16),
            pltpu.VMEM((16, 4, 8, 128), BF16),
            pltpu.VMEM((16, 4, 8, 128), BF16),
            pltpu.VMEM((2, 16, 16, 8, 128), BF16),
            pltpu.VMEM((8, 128), BF16),
            pltpu.VMEM((4, 128, 512), BF16),
            pltpu.VMEM((4, 128, 512), BF16),
            pltpu.VMEM((512, 128), jnp.int32),
            pltpu.VMEM((8, 128), F32),
            pltpu.VMEM((8, 128), F32),
            pltpu.VMEM((4, 128, 128), F32),
            pltpu.VMEM((4, 128, 128), F32),
            pltpu.VMEM((4, 4, 512, 128), F32),
            pltpu.VMEM((4, 512, 1024), BF16),
            pltpu.VMEM((4, 512, 1024), BF16),
            pltpu.VMEM((1024, 128), BF16),
            pltpu.VMEM((1024, 128), BF16),
            pltpu.VMEM((16, 4, 8, 128), BF16),
            pltpu.VMEM((16, 4, 8, 128), BF16),
            pltpu.VMEM((2, 4, 4, 4, 4, 8, 128), F32),
            pltpu.VMEM((4, 4, 4, 4, 8, 128), F32),
            pltpu.VMEM((4, 3, 4, 4, 8, 128), F32),
            pltpu.VMEM((4, 4, 4, 8, 128), F32),
            pltpu.VMEM((4, 3, 4, 8, 128), F32),
            pltpu.VMEM((15, 4, 8, 128), F32),
            pltpu.VMEM((16, 8, 128), BF16),
            dma((6,)),
            dma, dma((3,)), dma, dma, dma, dma, dma, dma,
            dma, dma((3,)), dma, dma((3,)),
            dma, dma, dma, dma, dma, dma,
            dma, dma((4,)), dma, dma((4,)), dma, dma((4,)), dma, dma, dma((2,)), dma((2,)),
        ],
        compiler_params=pltpu.CompilerParams(
            collective_id=1, has_side_effects=True, vmem_limit_bytes=48 * 2**20
        ),
        name="attend",
    )(*(pltpu.with_memory_space_constraint(a, pltpu.MemorySpace.HBM) for a in inputs))
    o, dq, dk, dv = pl.pallas_call(
        deliver,
        out_shape=tuple(jax.ShapeDtypeStruct(a.shape, BF16) for a in (o, dq, k, v)),
        in_specs=[hbm, hbm, vmem],
        out_specs=(hbm,) * 4,
        scratch_shapes=[
            pltpu.VMEM((2, 16, 8, 128), F32), pltpu.VMEM((2, 2, 4, 8, 128), BF16), dma((4,))
        ],
        compiler_params=pltpu.CompilerParams(vmem_limit_bytes=8 * 2**20),
        name="deliver",
    )(o, dq, dkv)
    return o.reshape(q.shape), dq.reshape(q.shape), dk, dv


def solution(mesh):
    grid = Mesh(mesh.devices.reshape(NZ, NY, NX, 2), ("z", "y", "x", "c"))
    spec = P(None, ("z", "y", "x", "c"), None, None)
    return jax.shard_map(
        on_device, mesh=grid, in_specs=(spec,) * 4, out_specs=(spec,) * 4, check_vma=False
    )
```

```python
import functools

import jax
import jax.numpy as jnp
from jax import lax
from jax.experimental import pallas as pl
from jax.experimental.pallas import tpu as pltpu
from jax.sharding import Mesh
from jax.sharding import PartitionSpec as P

MESH = pl.DeviceIdType.MESH
F32 = jnp.float32
BF16 = jnp.bfloat16
NZ, NY, NX = 16, 4, 4
MASKED = -1e30
PIECES = ((0, 7), (7, 6), (13, 3))


def nt(a, b):
    return lax.dot_general(a, b, (((1,), (1,)), ((), ())), preferred_element_type=F32)


def nn(a, b):
    return lax.dot_general(a, b, (((1,), (0,)), ((), ())), preferred_element_type=F32)


def split(a):
    high = a.astype(BF16)
    return high, (a - high.astype(F32)).astype(BF16)


def kernel(
    q_hbm, k_hbm, v_hbm, g_hbm, o_hbm, dq_hbm, dkv_ref,
    q_home, k_home, v_home, g_home, kv_wide, kv_home, q_rows, g_rows, kv_all,
    mate, keys_t, values_t, diagonal, row_delta, tops, attended_t, dq_t, scores, probs, dscores, g_twice, q_twice,
    o_rows, dq_rows, part, other, row_in, row_sum, block_in, first_in, final,
    in_sem, zkv_s, zkv_r, own_s, own_r, zq_s, zq_r, zg_s, zg_r, ag_s, ag_r, fw_s, fw_r,
    o_s, o_r, own_o, dq_s, dq_r, own_dq, sib_s, sib_r, row_s, row_r, blk_s, blk_r, dir_s, dir_r, fin_s, fin_r,
):
    z, y, x, c = (lax.axis_index(a) for a in ("z", "y", "x", "c"))
    chip = y * NX + x
    layer, group = z >> 3, z & 7
    scale = 128 ** -0.5

    def z_at(d):
        return (z + d) & 15

    def chip_at(e, sign):
        dy, dx = e >> 2, e & 3
        return (y + 4 + sign * dy) & 3, (x + 4 + sign * dx) & 3

    barrier = pltpu.get_barrier_semaphore()

    def greet(*device):
        pl.semaphore_signal(barrier, inc=1, device_id=device, device_id_type=MESH)

    for d in (8, 7, 9, 6, 10, 5, 11, 4, 12, 3, 13, 2, 14, 1, 15):
        greet(z_at(d), y, x, c)
        greet(z_at(d), y, x, 1 - c)
    for e in (10, 6, 9, 11, 14, 2, 8, 5, 7, 13, 15, 1, 3, 4, 12):
        greet(z, *chip_at(e, 1), c)
    greet(z, y, x, 1 - c)

    stage = [
        pltpu.make_async_copy(k_hbm, k_home, in_sem.at[0]),
        pltpu.make_async_copy(v_hbm, v_home, in_sem.at[1]),
        pltpu.make_async_copy(q_hbm, q_home, in_sem.at[2]),
        pltpu.make_async_copy(g_hbm, g_home, in_sem.at[3]),
        pltpu.make_async_copy(q_hbm.at[layer, :, group], q_rows.at[z], in_sem.at[4]),
        pltpu.make_async_copy(g_hbm.at[layer, :, group], g_rows.at[z], in_sem.at[5]),
    ]
    for copy in stage:
        copy.start()

    def drain(ref, sem):
        pltpu.make_async_remote_copy(
            src_ref=ref, dst_ref=ref, send_sem=sem, recv_sem=sem,
            device_id=(z, y, x, 1 - c), device_id_type=MESH,
        ).wait_recv()

    key_pos = lax.broadcasted_iota(jnp.int32, (512, 128), 0)
    lane = lax.broadcasted_iota(jnp.int32, (512, 128), 1)
    row_pos = 128 * (lane >> 5) + ((lane >> 3) & 3) + 8 * chip + 4 * c
    diagonal[...] = key_pos - row_pos
    identity = (
        lax.broadcasted_iota(jnp.int32, (128, 128), 0)
        == lax.broadcasted_iota(jnp.int32, (128, 128), 1)
    ).astype(F32).astype(BF16)

    with jax.named_scope("p0_kv"):
        stage[0].wait()
        stage[1].wait()
        for l in range(2):
            for i in range(4):
                kv_wide[l, :, i, :] = k_home[l, i].astype(F32)
                kv_wide[l, :, 4 + i, :] = v_home[l, i].astype(F32)
        kv_home[...] = kv_wide[...].astype(BF16)
        for copy in stage[2:]:
            copy.wait()
    with jax.named_scope("p1_barrier"):
        pl.semaphore_wait(barrier, 46)

    def to_z(src, dst, send, recv):
        def make(d):
            t = z_at(d)
            return pltpu.make_async_remote_copy(
                src_ref=src.at[t >> 3, :, t & 7], dst_ref=dst.at[z], send_sem=send,
                recv_sem=recv, device_id=(t, y, x, c), device_id_type=MESH,
            )
        return make

    half = pl.ds(pl.multiple_of(4 * c, 4), 4)

    def slot_of(u):
        return u + jnp.where(u < 10, 0, jnp.where(u < 13, 3, -3))

    def to_core(core, d, far):
        t = z_at(d)
        return pltpu.make_async_remote_copy(
            src_ref=kv_home.at[t >> 3, t & 7, pl.ds(4 - 4 * core, 4)],
            dst_ref=kv_all.at[1 - core, slot_of((19 - d) & 15), chip, half],
            send_sem=zkv_s, recv_sem=zkv_r.at[far],
            device_id=(t, y, x, core), device_id_type=MESH,
        )

    own_kv = pltpu.make_async_remote_copy(
        src_ref=kv_home.at[layer, group], dst_ref=mate, send_sem=own_s,
        recv_sem=own_r, device_id=(z, y, x, 1 - c), device_id_type=MESH,
    )
    zq = to_z(q_home, q_rows, zq_s, zq_r)
    zg = to_z(g_home, g_rows, zg_s, zg_r)

    def loop(low, high, body):
        def step(i, _):
            body(i)
            return 0
        lax.fori_loop(low, high, step, 0)

    def far_first(body):
        loop(1, 9, lambda i: body(9 - i))
        loop(9, 16, body)

    with jax.named_scope("p2_zstart"):
        own_kv.start()
        def send_kv(d, far):
            to_core(0, d, far).start()
            to_core(1, d, far).start()

        loop(1, 4, lambda d: (send_kv(d, 0), send_kv(16 - d, 0)))
        loop(4, 7, lambda d: (send_kv(d, 1), send_kv(16 - d, 1)))
        loop(7, 10, lambda d: send_kv(d, 2))
        loop(1, 16, lambda d: zq(d).start())
        far_first(lambda d: zg(d).start())


    def gather(n, e):
        j = jnp.where(e - 1 < chip, e - 1, e)
        block = kv_all.at[1 - c, pl.ds(*PIECES[n]), chip]
        return pltpu.make_async_remote_copy(
            src_ref=block, dst_ref=block, send_sem=ag_s,
            recv_sem=ag_r.at[n], device_id=(z, j >> 2, j & 3, c), device_id_type=MESH,
        )

    def forward(n):
        block = kv_all.at[1 - c, pl.ds(*PIECES[n])]
        return pltpu.make_async_remote_copy(
            src_ref=block, dst_ref=block, send_sem=fw_s,
            recv_sem=fw_r.at[n], device_id=(z, y, x, 1 - c), device_id_type=MESH,
        )

    with jax.named_scope("p3_zkvn"):
        own_kv.wait_recv()
        mine = pltpu.roll(kv_wide[layer, group], 4, 0)
        own_half = (lax.broadcasted_iota(jnp.int32, (8, 128), 0) >> 2) == c
        kv_all[1 - c, 3, chip] = jnp.where(own_half, mine, mate[...].astype(F32)).astype(BF16)
        drain(kv_all.at[0, 0, pl.ds(0, 6)], zkv_r.at[0])
        loop(1, 16, lambda e: gather(0, e).start())
    with jax.named_scope("p3_zkvm"):
        drain(kv_all.at[0, 0, pl.ds(0, 6)], zkv_r.at[1])
        loop(1, 16, lambda e: gather(1, e).start())
    with jax.named_scope("p3_zkvf"):
        drain(kv_all.at[0, 0, pl.ds(0, 3)], zkv_r.at[2])
        loop(1, 16, lambda e: gather(2, e).start())

    for n in range(3):
        with jax.named_scope(f"p4_ag{n}"):
            drain(kv_all.at[1 - c, pl.ds(*PIECES[n]), pl.ds(0, 15)], ag_r.at[n])
            forward(n).start()
    def of_core(core, body):
        @pl.when(c == core)
        def _():
            body()

    def from_sibling():
        for n in range(3):
            drain(kv_all.at[c, pl.ds(*PIECES[n])], fw_r.at[n])

    with jax.named_scope("p6_keys"):
        of_core(0, from_sibling)

    def plane_group(kind, kg):
        return jnp.concatenate(
            [kv_all[kind, slot_of((4 * kg + i + 19 - z) & 15)].reshape(128, 128) for i in range(4)], axis=0
        )

    with jax.named_scope("p8_qwait"):
        drain(q_rows.at[pl.ds(0, 15)], zq_r)

    def home(rows, out, send, recv, own_sem):
        def make(t):
            return pltpu.make_async_remote_copy(
                src_ref=rows.at[t], dst_ref=out.at[layer, :, group], send_sem=send,
                recv_sem=recv, device_id=(t, y, x, c), device_id_type=MESH,
            )
        own = pltpu.make_async_copy(rows.at[z], out.at[layer, :, group], own_sem)
        def start():
            far_first(lambda d: make(z_at(d)).start())
            own.start()
        def start_at(t):
            @pl.when(t != z)
            def _():
                make(t).start()
            @pl.when(t == z)
            def _():
                own.start()
        def finish():
            drain(rows.at[pl.ds(0, 15)], send)
            drain(rows.at[pl.ds(0, 15)], recv)
            own.wait()
        return start, start_at, finish

    o_start, _, o_finish = home(o_rows, o_hbm, o_s, o_r, own_o)
    _, dq_start, dq_finish = home(dq_rows, dq_hbm, dq_s, dq_r, own_dq)

    factor_2 = scale * 1.4426950408889634

    def pair(rg):
        return slice(256 * rg, 256 * rg + 256)

    def scores_of(rg):
        lanes = pair(rg)
        q = q_rows[4 * rg : 4 * rg + 4].astype(F32).reshape(128, 128).astype(BF16)
        q_twice[lanes] = jnp.concatenate([q, q], axis=0)
        top = jnp.full((8, 128), MASKED, F32)
        for kg in range(rg + 1):
            s = nt(plane_group(0, kg), q) * factor_2
            if kg == rg:
                s = jnp.where(diagonal[...] <= 0, s, MASKED)
            scores[rg, kg] = s
            top = jnp.maximum(top, jnp.max(s.reshape(64, 8, 128), axis=0))
        return jnp.max(top, axis=0, keepdims=True)

    def forward_of(rg, top):
        lanes = pair(rg)
        total = jnp.zeros((8, 128), F32)
        for kg in range(rg + 1):
            e = jnp.exp2(scores[rg, kg] - top)
            scores[rg, kg] = e
            total = total + jnp.sum(e.reshape(64, 8, 128), axis=0)
        inverse = 1.0 / jnp.sum(total, axis=0, keepdims=True)
        acc = jnp.zeros((128, 256), F32)
        for kg in range(rg + 1):
            p = scores[rg, kg] * inverse
            p2 = jnp.concatenate(split(p), axis=1)
            probs[kg, :, lanes] = p2
            scores[rg, kg] = p
            acc = acc + nn(values_t[kg], p2)
        o_t = acc[:, :128] + acc[:, 128:]
        attended_t[rg] = o_t.astype(BF16).astype(F32)
        o_rows[4 * rg : 4 * rg + 4] = o_t.T.reshape(4, 4, 8, 128).astype(BF16)

    def deltas(rg):
        g = g_rows[4 * rg : 4 * rg + 4].astype(F32).reshape(128, 128).astype(BF16)
        g_twice[pair(rg)] = jnp.concatenate([g, g], axis=0)
        delta = nt(identity, g) * attended_t[rg]
        row_delta[rg : rg + 1] = jnp.sum(delta, axis=0, keepdims=True)

    def backward_of(kg):
        for rg in range(kg, 4):
            g = g_twice[256 * rg : 256 * rg + 128]
            ds = scores[rg, kg] * (nt(plane_group(1, kg), g) - row_delta[rg : rg + 1])
            ds2 = jnp.concatenate(split(ds), axis=1)
            dscores[kg, :, pair(rg)] = ds2
            term = nn(keys_t[kg], ds2)
            term = term[:, :128] + term[:, 128:]
            dq_t[rg] = dq_t[rg] + term if kg else term
        dq_rows[4 * kg : 4 * kg + 4] = (dq_t[kg] * scale).T.reshape(4, 4, 8, 128).astype(BF16)
        part[0, kg] = key_sum(kg, kg, 4)
        part[1, kg] = value_sum(kg, kg, 4)

    def value_sum(kg, low, high):
        lanes = slice(256 * low, 256 * high)
        return nn(probs[kg, :, lanes], g_twice[lanes]).reshape(4, 4, 4, 8, 128)

    def key_sum(kg, low, high):
        lanes = slice(256 * low, 256 * high)
        dk = nn(dscores[kg, :, lanes], q_twice[lanes])
        return jnp.swapaxes(dk.reshape(4, 4, 4, 8, 128), 1, 2)

    kind = 1 - c
    along = jnp.where(c == 0, y, x)
    across = jnp.where(c == 0, x, y)

    def sibling(kg):
        return pltpu.make_async_remote_copy(
            src_ref=part.at[c, kg], dst_ref=other.at[kg], send_sem=sib_s,
            recv_sem=sib_r.at[kg], device_id=(z, y, x, 1 - c), device_id_type=MESH,
        )

    def row_send(kg, a):
        t = (along + a) & 3
        return pltpu.make_async_remote_copy(
            src_ref=part.at[kind, kg, :, t], dst_ref=row_in.at[kg, a - 1], send_sem=row_s,
            recv_sem=row_r.at[kg],
            device_id=(z, jnp.where(c == 0, t, y), jnp.where(c == 0, x, t), c), device_id_type=MESH,
        )

    def block_send(kg, a):
        t = (across + a) & 3
        return pltpu.make_async_remote_copy(
            src_ref=row_sum.at[kg, :, t], dst_ref=block_in.at[kg, a - 1], send_sem=blk_s,
            recv_sem=blk_r.at[kg],
            device_id=(z, jnp.where(c == 0, y, t), jnp.where(c == 0, t, x), c), device_id_type=MESH,
        )

    def direct_send(j):
        yy, xx = j >> 2, j & 3
        a, b = jnp.where(c == 0, yy, xx), jnp.where(c == 0, xx, yy)
        return pltpu.make_async_remote_copy(
            src_ref=part.at[kind, 0, :, a, b], dst_ref=first_in.at[(j - chip + 15) & 15],
            send_sem=dir_s, recv_sem=dir_r, device_id=(z, yy, xx, c), device_id_type=MESH,
        )

    def combine(kg):
        sibling(kg).wait_recv()
        part[kind, kg] = part[kind, kg] + other[kg]
        if kg:
            loop(1, 4, lambda a: row_send(kg, a).start())
        else:
            loop(1, 16, lambda e: direct_send(jnp.where(e - 1 < chip, e - 1, e)).start())

    with jax.named_scope("p9_scores"):
        for rg in range(4):
            tops[rg : rg + 1] = scores_of(rg)
        for kg in range(4):
            keys_t[kg] = nt(identity, plane_group(0, kg)).astype(BF16)
    with jax.named_scope("p9_values"):
        of_core(1, from_sibling)
    with jax.named_scope("p9_fwd"):
        for kg in range(4):
            values_t[kg] = nt(identity, plane_group(1, kg)).astype(BF16)
        for rg in range(4):
            forward_of(rg, tops[rg : rg + 1])

    with jax.named_scope("pa_osend"):
        o_start()
        drain(g_rows.at[pl.ds(0, 15)], zg_r)
    for kg in range(4):
        with jax.named_scope(f"p9_bwd{kg}"):
            if kg == 0:
                for rg in range(4):
                    deltas(rg)
            backward_of(kg)
        with jax.named_scope(f"pa_comb{kg}"):
            sibling(kg).start()
            if kg == 0:
                loop(0, 4, dq_start)
            if kg:
                combine(kg - 1)
    with jax.named_scope("pb_combine"):
        combine(3)

    def row_finish(kg):
        drain(row_in.at[kg], row_r.at[kg])
        total = part[kind, kg, :, along]
        for a in range(3):
            total = total + row_in[kg, a]
        row_sum[kg] = total
        loop(1, 4, lambda a: block_send(kg, a).start())

    factor = jnp.where(c == 0, 1.0, scale).astype(F32)

    def finish_first():
        drain(first_in, dir_r)
        total = part[kind, 0, :, along, across]
        for e in range(15):
            total = total + first_in[e]
        final[pl.ds(0, 4)] = (total * factor).astype(BF16)

    def finish(kg):
        drain(block_in.at[kg], blk_r.at[kg])
        total = row_sum[kg, :, across]
        for a in range(3):
            total = total + block_in[kg, a]
        final[pl.ds(4 * kg, 4)] = (total * factor).astype(BF16)

    def out(t, other_core):
        core = 1 - c if other_core else c
        rows = pl.ds(pl.multiple_of(4 * core, 4), 4)
        return pltpu.make_async_remote_copy(
            src_ref=final.at[t, rows], dst_ref=dkv_ref.at[kind, z, rows], send_sem=fin_s.at[other_core],
            recv_sem=fin_r.at[other_core], device_id=(t, y, x, core), device_id_type=MESH,
        )

    def send_out(t):
        out(t, 1).start()
        @pl.when(t != z)
        def _():
            out(t, 0).start()

    with jax.named_scope("pc_first"):
        finish_first()
        loop(0, 4, send_out)
        loop(4, 16, dq_start)
    for kg in range(1, 4):
        with jax.named_scope(f"pc_row{kg}"):
            row_finish(kg)
    for kg in range(1, 4):
        with jax.named_scope(f"pc_blk{kg}"):
            finish(kg)
            loop(4 * kg, 4 * kg + 4, send_out)
    dkv_ref[kind, z] = final[z]

    with jax.named_scope("pe_sends"):
        own_kv.wait_send()
        drain(kv_all.at[0, 0, pl.ds(0, 15)], zkv_s)
        drain(q_rows.at[pl.ds(0, 15)], zq_s)
        drain(g_rows.at[pl.ds(0, 15)], zg_s)
        drain(kv_all.at[0, :, pl.ds(0, 15)], ag_s)
        drain(kv_all.at[0], fw_s)
        o_finish()
        dq_finish()
        drain(other, sib_s)
        drain(first_in, dir_s)
        drain(row_in.at[pl.ds(0, 3)], row_s)
        drain(block_in.at[pl.ds(0, 3)], blk_s)
    with jax.named_scope("pf_dkv"):
        for sem in (fin_s, fin_r):
            drain(dkv_ref.at[0, pl.ds(0, 15), pl.ds(0, 4)], sem.at[0])
            drain(dkv_ref.at[1, :, pl.ds(0, 4)], sem.at[1])


def deliver(o_ref, dq_ref, dkv_ref, o_hbm, dq_hbm, dk_hbm, dv_hbm, wide, narrow, sem):
    c = lax.axis_index("c")
    copies = [
        pltpu.make_async_copy(o_ref, o_hbm, sem.at[0]),
        pltpu.make_async_copy(dq_ref, dq_hbm, sem.at[1]),
        pltpu.make_async_copy(narrow.at[0], dk_hbm, sem.at[2]),
        pltpu.make_async_copy(narrow.at[1], dv_hbm, sem.at[3]),
    ]
    copies[0].start()
    copies[1].start()
    wide[...] = dkv_ref[...].astype(F32)
    for core in range(2):
        @pl.when(c == core)
        def _():
            for kind in range(2):
                for l in range(2):
                    for i in range(4):
                        rows = wide[kind, 8 * l : 8 * l + 8, 4 * core + i, :]
                        narrow[kind, l, i] = rows.astype(BF16)
    copies[2].start()
    copies[3].start()
    for copy in copies:
        copy.wait()


def on_device(q, k, v, g):
    wide = (2, 4, 8, 8, 128)
    dma = pltpu.SemaphoreType.DMA
    hbm = pl.BlockSpec(memory_space=pltpu.MemorySpace.HBM)
    vmem = pl.BlockSpec(memory_space=pltpu.VMEM)
    inputs = (q.reshape(wide), k, v, g.reshape(wide))
    o, dq, dkv = pl.pallas_call(
        kernel,
        out_shape=(
            jax.ShapeDtypeStruct(wide, BF16),
            jax.ShapeDtypeStruct(wide, BF16),
            jax.ShapeDtypeStruct((2, 16, 8, 128), BF16),
        ),
        in_specs=[hbm, hbm, hbm, hbm],
        out_specs=(hbm, hbm, vmem),
        scratch_shapes=[
            pltpu.VMEM(wide, BF16),
            pltpu.VMEM((2, 4, 8, 128), BF16),
            pltpu.VMEM((2, 4, 8, 128), BF16),
            pltpu.VMEM(wide, BF16),
            pltpu.VMEM((2, 8, 8, 128), F32),
            pltpu.VMEM((2, 8, 8, 128), BF16),
            pltpu.VMEM((16, 4, 8, 128), BF16),
            pltpu.VMEM((16, 4, 8, 128), BF16),
            pltpu.VMEM((2, 16, 16, 8, 128), BF16),
            pltpu.VMEM((8, 128), BF16),
            pltpu.VMEM((4, 128, 512), BF16),
            pltpu.VMEM((4, 128, 512), BF16),
            pltpu.VMEM((512, 128), jnp.int32),
            pltpu.VMEM((8, 128), F32),
            pltpu.VMEM((8, 128), F32),
            pltpu.VMEM((4, 128, 128), F32),
            pltpu.VMEM((4, 128, 128), F32),
            pltpu.VMEM((4, 4, 512, 128), F32),
            pltpu.VMEM((4, 512, 1024), BF16),
            pltpu.VMEM((4, 512, 1024), BF16),
            pltpu.VMEM((1024, 128), BF16),
            pltpu.VMEM((1024, 128), BF16),
            pltpu.VMEM((16, 4, 8, 128), BF16),
            pltpu.VMEM((16, 4, 8, 128), BF16),
            pltpu.VMEM((2, 4, 4, 4, 4, 8, 128), F32),
            pltpu.VMEM((4, 4, 4, 4, 8, 128), F32),
            pltpu.VMEM((4, 3, 4, 4, 8, 128), F32),
            pltpu.VMEM((4, 4, 4, 8, 128), F32),
            pltpu.VMEM((4, 3, 4, 8, 128), F32),
            pltpu.VMEM((15, 4, 8, 128), F32),
            pltpu.VMEM((16, 8, 128), BF16),
            dma((6,)),
            dma, dma((3,)), dma, dma, dma, dma, dma, dma,
            dma, dma((3,)), dma, dma((3,)),
            dma, dma, dma, dma, dma, dma,
            dma, dma((4,)), dma, dma((4,)), dma, dma((4,)), dma, dma, dma((2,)), dma((2,)),
        ],
        compiler_params=pltpu.CompilerParams(
            collective_id=1,
            has_side_effects=True,
            vmem_limit_bytes=48 * 2**20,
        ),
        name="attend",
    )(*(pltpu.with_memory_space_constraint(a, pltpu.MemorySpace.HBM) for a in inputs))
    o, dq, dk, dv = pl.pallas_call(
        deliver,
        out_shape=tuple(jax.ShapeDtypeStruct(a.shape, BF16) for a in (o, dq, k, v)),
        in_specs=[hbm, hbm, vmem],
        out_specs=(hbm,) * 4,
        scratch_shapes=[
            pltpu.VMEM((2, 16, 8, 128), F32), pltpu.VMEM((2, 2, 4, 8, 128), BF16), dma((4,))
        ],
        compiler_params=pltpu.CompilerParams(vmem_limit_bytes=8 * 2**20),
        name="deliver",
    )(o, dq, dkv)
    return o.reshape(q.shape), dq.reshape(q.shape), dk, dv


def solution(mesh):
    grid = Mesh(mesh.devices.reshape(NZ, NY, NX, 2), ("z", "y", "x", "c"))
    spec = P(None, ("z", "y", "x", "c"), None, None)
    return jax.shard_map(
        on_device, mesh=grid, in_specs=(spec,) * 4, out_specs=(spec,) * 4, check_vma=False
    )
```

```python
import functools

import jax
import jax.numpy as jnp
from jax import lax
from jax.experimental import pallas as pl
from jax.experimental.pallas import tpu as pltpu
from jax.sharding import Mesh
from jax.sharding import PartitionSpec as P

MESH = pl.DeviceIdType.MESH
F32 = jnp.float32
BF16 = jnp.bfloat16
NZ, NY, NX = 16, 4, 4
MASKED = -1e30
PIECES = ((0, 7), (7, 6), (13, 3))


def nt(a, b):
    return lax.dot_general(a, b, (((1,), (1,)), ((), ())), preferred_element_type=F32)


def nn(a, b):
    return lax.dot_general(a, b, (((1,), (0,)), ((), ())), preferred_element_type=F32)


def split(a):
    high = a.astype(BF16)
    return high, (a - high.astype(F32)).astype(BF16)


def kernel(
    q_hbm, k_hbm, v_hbm, g_hbm, o_hbm, dq_hbm, dkv_ref,
    q_home, k_home, v_home, g_home, kv_wide, kv_home, q_rows, g_rows, kv_all,
    mate, keys_t, values_t, diagonal, row_delta, tops, attended_t, dq_t, scores, probs, dscores, g_twice, q_twice,
    o_rows, dq_rows, part, other, row_in, row_sum, block_in, first_in, final,
    in_sem, zkv_s, zkv_r, own_s, own_r, zq_s, zq_r, zg_s, zg_r, ag_s, ag_r, fw_s, fw_r,
    o_s, o_r, own_o, dq_s, dq_r, own_dq, sib_s, sib_r, row_s, row_r, blk_s, blk_r, dir_s, dir_r, fin_s, fin_r,
):
    z, y, x, c = (lax.axis_index(a) for a in ("z", "y", "x", "c"))
    chip = y * NX + x
    layer, group = z >> 3, z & 7
    scale = 128 ** -0.5

    def z_at(d):
        return (z + d) & 15

    def chip_at(e, sign):
        dy, dx = e >> 2, e & 3
        return (y + 4 + sign * dy) & 3, (x + 4 + sign * dx) & 3

    barrier = pltpu.get_barrier_semaphore()

    def greet(*device):
        pl.semaphore_signal(barrier, inc=1, device_id=device, device_id_type=MESH)

    for d in (8, 7, 9, 6, 10, 5, 11, 4, 12, 3, 13, 2, 14, 1, 15):
        greet(z_at(d), y, x, c)
        greet(z_at(d), y, x, 1 - c)
    for e in (10, 6, 9, 11, 14, 2, 8, 5, 7, 13, 15, 1, 3, 4, 12):
        greet(z, *chip_at(e, 1), c)
    greet(z, y, x, 1 - c)

    stage = [
        pltpu.make_async_copy(k_hbm, k_home, in_sem.at[0]),
        pltpu.make_async_copy(v_hbm, v_home, in_sem.at[1]),
        pltpu.make_async_copy(q_hbm, q_home, in_sem.at[2]),
        pltpu.make_async_copy(g_hbm, g_home, in_sem.at[3]),
        pltpu.make_async_copy(q_hbm.at[layer, :, group], q_rows.at[z], in_sem.at[4]),
        pltpu.make_async_copy(g_hbm.at[layer, :, group], g_rows.at[z], in_sem.at[5]),
    ]
    for copy in stage:
        copy.start()

    def drain(ref, sem):
        pltpu.make_async_remote_copy(
            src_ref=ref, dst_ref=ref, send_sem=sem, recv_sem=sem,
            device_id=(z, y, x, 1 - c), device_id_type=MESH,
        ).wait_recv()

    key_pos = lax.broadcasted_iota(jnp.int32, (512, 128), 0)
    lane = lax.broadcasted_iota(jnp.int32, (512, 128), 1)
    row_pos = 128 * (lane >> 5) + ((lane >> 3) & 3) + 8 * chip + 4 * c
    diagonal[...] = key_pos - row_pos
    identity = (
        lax.broadcasted_iota(jnp.int32, (128, 128), 0)
        == lax.broadcasted_iota(jnp.int32, (128, 128), 1)
    ).astype(F32).astype(BF16)

    with jax.named_scope("p0_kv"):
        stage[0].wait()
        stage[1].wait()
        for l in range(2):
            for i in range(4):
                kv_wide[l, :, i, :] = k_home[l, i].astype(F32)
                kv_wide[l, :, 4 + i, :] = v_home[l, i].astype(F32)
        kv_home[...] = kv_wide[...].astype(BF16)
        for copy in stage[2:]:
            copy.wait()
    with jax.named_scope("p1_barrier"):
        pl.semaphore_wait(barrier, 46)

    def to_z(src, dst, send, recv):
        def make(d):
            t = z_at(d)
            return pltpu.make_async_remote_copy(
                src_ref=src.at[t >> 3, :, t & 7], dst_ref=dst.at[z], send_sem=send,
                recv_sem=recv, device_id=(t, y, x, c), device_id_type=MESH,
            )
        return make

    half = pl.ds(pl.multiple_of(4 * c, 4), 4)

    def slot_of(u):
        return u + jnp.where(u < 10, 0, jnp.where(u < 13, 3, -3))

    def to_core(core, d, far):
        t = z_at(d)
        return pltpu.make_async_remote_copy(
            src_ref=kv_home.at[t >> 3, t & 7, pl.ds(4 - 4 * core, 4)],
            dst_ref=kv_all.at[1 - core, slot_of((19 - d) & 15), chip, half],
            send_sem=zkv_s, recv_sem=zkv_r.at[far],
            device_id=(t, y, x, core), device_id_type=MESH,
        )

    own_kv = pltpu.make_async_remote_copy(
        src_ref=kv_home.at[layer, group], dst_ref=mate, send_sem=own_s,
        recv_sem=own_r, device_id=(z, y, x, 1 - c), device_id_type=MESH,
    )
    zq = to_z(q_home, q_rows, zq_s, zq_r)
    zg = to_z(g_home, g_rows, zg_s, zg_r)

    def loop(low, high, body):
        def step(i, _):
            body(i)
            return 0
        lax.fori_loop(low, high, step, 0)

    def far_first(body):
        loop(1, 9, lambda i: body(9 - i))
        loop(9, 16, body)

    with jax.named_scope("p2_zstart"):
        own_kv.start()
        def send_kv(d, far):
            to_core(0, d, far).start()
            to_core(1, d, far).start()

        loop(1, 4, lambda d: (send_kv(d, 0), send_kv(16 - d, 0)))
        loop(4, 7, lambda d: (send_kv(d, 1), send_kv(16 - d, 1)))
        loop(7, 10, lambda d: send_kv(d, 2))
        loop(1, 16, lambda d: zq(d).start())
        far_first(lambda d: zg(d).start())


    def gather(n, e):
        j = jnp.where(e - 1 < chip, e - 1, e)
        block = kv_all.at[1 - c, pl.ds(*PIECES[n]), chip]
        return pltpu.make_async_remote_copy(
            src_ref=block, dst_ref=block, send_sem=ag_s,
            recv_sem=ag_r.at[n], device_id=(z, j >> 2, j & 3, c), device_id_type=MESH,
        )

    def forward(n):
        block = kv_all.at[1 - c, pl.ds(*PIECES[n])]
        return pltpu.make_async_remote_copy(
            src_ref=block, dst_ref=block, send_sem=fw_s,
            recv_sem=fw_r.at[n], device_id=(z, y, x, 1 - c), device_id_type=MESH,
        )

    with jax.named_scope("p3_zkvn"):
        own_kv.wait_recv()
        mine = pltpu.roll(kv_wide[layer, group], 4, 0)
        own_half = (lax.broadcasted_iota(jnp.int32, (8, 128), 0) >> 2) == c
        kv_all[1 - c, 3, chip] = jnp.where(own_half, mine, mate[...].astype(F32)).astype(BF16)
        drain(kv_all.at[0, 0, pl.ds(0, 6)], zkv_r.at[0])
        loop(1, 16, lambda e: gather(0, e).start())
    with jax.named_scope("p3_zkvm"):
        drain(kv_all.at[0, 0, pl.ds(0, 6)], zkv_r.at[1])
        loop(1, 16, lambda e: gather(1, e).start())
    with jax.named_scope("p3_zkvf"):
        drain(kv_all.at[0, 0, pl.ds(0, 3)], zkv_r.at[2])
        loop(1, 16, lambda e: gather(2, e).start())

    for n in range(3):
        with jax.named_scope(f"p4_ag{n}"):
            drain(kv_all.at[1 - c, pl.ds(*PIECES[n]), pl.ds(0, 15)], ag_r.at[n])
            forward(n).start()
    def of_core(core, body):
        @pl.when(c == core)
        def _():
            body()

    def from_sibling():
        for n in range(3):
            drain(kv_all.at[c, pl.ds(*PIECES[n])], fw_r.at[n])

    with jax.named_scope("p6_keys"):
        of_core(0, from_sibling)

    def plane_group(kind, kg):
        return jnp.concatenate(
            [kv_all[kind, slot_of((4 * kg + i + 19 - z) & 15)].reshape(128, 128) for i in range(4)], axis=0
        )

    with jax.named_scope("p8_qwait"):
        drain(q_rows.at[pl.ds(0, 15)], zq_r)

    def home(rows, out, send, recv, own_sem):
        def make(t):
            return pltpu.make_async_remote_copy(
                src_ref=rows.at[t], dst_ref=out.at[layer, :, group], send_sem=send,
                recv_sem=recv, device_id=(t, y, x, c), device_id_type=MESH,
            )
        own = pltpu.make_async_copy(rows.at[z], out.at[layer, :, group], own_sem)
        def start():
            far_first(lambda d: make(z_at(d)).start())
            own.start()
        def start_at(t):
            @pl.when(t != z)
            def _():
                make(t).start()
            @pl.when(t == z)
            def _():
                own.start()
        def finish():
            drain(rows.at[pl.ds(0, 15)], send)
            drain(rows.at[pl.ds(0, 15)], recv)
            own.wait()
        return start, start_at, finish

    o_start, _, o_finish = home(o_rows, o_hbm, o_s, o_r, own_o)
    _, dq_start, dq_finish = home(dq_rows, dq_hbm, dq_s, dq_r, own_dq)

    factor_2 = scale * 1.4426950408889634

    def pair(rg):
        return slice(256 * rg, 256 * rg + 256)

    def scores_of(rg):
        lanes = pair(rg)
        q = q_rows[4 * rg : 4 * rg + 4].astype(F32).reshape(128, 128).astype(BF16)
        q_twice[lanes] = jnp.concatenate([q, q], axis=0)
        top = jnp.full((8, 128), MASKED, F32)
        for kg in range(rg + 1):
            s = nt(plane_group(0, kg), q) * factor_2
            if kg == rg:
                s = jnp.where(diagonal[...] <= 0, s, MASKED)
            scores[rg, kg] = s
            top = jnp.maximum(top, jnp.max(s.reshape(64, 8, 128), axis=0))
        return jnp.max(top, axis=0, keepdims=True)

    def forward_of(rg, top):
        lanes = pair(rg)
        total = jnp.zeros((8, 128), F32)
        for kg in range(rg + 1):
            e = jnp.exp2(scores[rg, kg] - top)
            scores[rg, kg] = e
            total = total + jnp.sum(e.reshape(64, 8, 128), axis=0)
        inverse = 1.0 / jnp.sum(total, axis=0, keepdims=True)
        acc = jnp.zeros((128, 256), F32)
        for kg in range(rg + 1):
            p = scores[rg, kg] * inverse
            p2 = jnp.concatenate(split(p), axis=1)
            probs[kg, :, lanes] = p2
            scores[rg, kg] = p
            acc = acc + nn(values_t[kg], p2)
        o_t = acc[:, :128] + acc[:, 128:]
        attended_t[rg] = o_t.astype(BF16).astype(F32)
        o_rows[4 * rg : 4 * rg + 4] = o_t.T.reshape(4, 4, 8, 128).astype(BF16)

    def deltas(rg):
        g = g_rows[4 * rg : 4 * rg + 4].astype(F32).reshape(128, 128).astype(BF16)
        g_twice[pair(rg)] = jnp.concatenate([g, g], axis=0)
        delta = nt(identity, g) * attended_t[rg]
        row_delta[rg : rg + 1] = jnp.sum(delta, axis=0, keepdims=True)

    def backward_of(kg):
        for rg in range(kg, 4):
            g = g_twice[256 * rg : 256 * rg + 128]
            ds = scores[rg, kg] * (nt(plane_group(1, kg), g) - row_delta[rg : rg + 1])
            ds2 = jnp.concatenate(split(ds), axis=1)
            dscores[kg, :, pair(rg)] = ds2
            term = nn(keys_t[kg], ds2)
            term = term[:, :128] + term[:, 128:]
            dq_t[rg] = dq_t[rg] + term if kg else term
        dq_rows[4 * kg : 4 * kg + 4] = (dq_t[kg] * scale).T.reshape(4, 4, 8, 128).astype(BF16)
        part[0, kg] = key_sum(kg, kg, 4)
        part[1, kg] = value_sum(kg, kg, 4)

    def value_sum(kg, low, high):
        lanes = slice(256 * low, 256 * high)
        return nn(probs[kg, :, lanes], g_twice[lanes]).reshape(4, 4, 4, 8, 128)

    def key_sum(kg, low, high):
        lanes = slice(256 * low, 256 * high)
        dk = nn(dscores[kg, :, lanes], q_twice[lanes])
        return jnp.swapaxes(dk.reshape(4, 4, 4, 8, 128), 1, 2)

    kind = 1 - c
    along = jnp.where(c == 0, y, x)
    across = jnp.where(c == 0, x, y)

    def sibling(kg):
        return pltpu.make_async_remote_copy(
            src_ref=part.at[c, kg], dst_ref=other.at[kg], send_sem=sib_s,
            recv_sem=sib_r.at[kg], device_id=(z, y, x, 1 - c), device_id_type=MESH,
        )

    def row_send(kg, a):
        t = (along + a) & 3
        return pltpu.make_async_remote_copy(
            src_ref=part.at[kind, kg, :, t], dst_ref=row_in.at[kg, a - 1], send_sem=row_s,
            recv_sem=row_r.at[kg],
            device_id=(z, jnp.where(c == 0, t, y), jnp.where(c == 0, x, t), c), device_id_type=MESH,
        )

    def block_send(kg, a):
        t = (across + a) & 3
        return pltpu.make_async_remote_copy(
            src_ref=row_sum.at[kg, :, t], dst_ref=block_in.at[kg, a - 1], send_sem=blk_s,
            recv_sem=blk_r.at[kg],
            device_id=(z, jnp.where(c == 0, y, t), jnp.where(c == 0, t, x), c), device_id_type=MESH,
        )

    def direct_send(j):
        yy, xx = j >> 2, j & 3
        a, b = jnp.where(c == 0, yy, xx), jnp.where(c == 0, xx, yy)
        return pltpu.make_async_remote_copy(
            src_ref=part.at[kind, 0, :, a, b], dst_ref=first_in.at[(j - chip + 15) & 15],
            send_sem=dir_s, recv_sem=dir_r, device_id=(z, yy, xx, c), device_id_type=MESH,
        )

    def combine(kg):
        sibling(kg).wait_recv()
        part[kind, kg] = part[kind, kg] + other[kg]
        if kg:
            loop(1, 4, lambda a: row_send(kg, a).start())
        else:
            loop(1, 16, lambda e: direct_send(jnp.where(e - 1 < chip, e - 1, e)).start())

    with jax.named_scope("p9_scores"):
        for rg in range(4):
            tops[rg : rg + 1] = scores_of(rg)
        for kg in range(4):
            keys_t[kg] = nt(identity, plane_group(0, kg)).astype(BF16)
    with jax.named_scope("p9_values"):
        of_core(1, from_sibling)
    with jax.named_scope("p9_fwd"):
        for kg in range(4):
            values_t[kg] = nt(identity, plane_group(1, kg)).astype(BF16)
        for rg in range(4):
            forward_of(rg, tops[rg : rg + 1])

    with jax.named_scope("pa_osend"):
        o_start()
        drain(g_rows.at[pl.ds(0, 15)], zg_r)
    for kg in range(4):
        with jax.named_scope(f"p9_bwd{kg}"):
            if kg == 0:
                for rg in range(4):
                    deltas(rg)
            backward_of(kg)
        with jax.named_scope(f"pa_comb{kg}"):
            sibling(kg).start()
            if kg == 0:
                loop(0, 4, dq_start)
            if kg:
                combine(kg - 1)
    with jax.named_scope("pb_combine"):
        combine(3)

    def row_finish(kg):
        drain(row_in.at[kg], row_r.at[kg])
        total = part[kind, kg, :, along]
        for a in range(3):
            total = total + row_in[kg, a]
        row_sum[kg] = total
        loop(1, 4, lambda a: block_send(kg, a).start())

    factor = jnp.where(c == 0, 1.0, scale).astype(F32)

    def finish_first():
        drain(first_in, dir_r)
        total = part[kind, 0, :, along, across]
        for e in range(15):
            total = total + first_in[e]
        final[pl.ds(0, 4)] = (total * factor).astype(BF16)

    def finish(kg):
        drain(block_in.at[kg], blk_r.at[kg])
        total = row_sum[kg, :, across]
        for a in range(3):
            total = total + block_in[kg, a]
        final[pl.ds(4 * kg, 4)] = (total * factor).astype(BF16)

    def out(t, other_core):
        core = 1 - c if other_core else c
        rows = pl.ds(pl.multiple_of(4 * core, 4), 4)
        return pltpu.make_async_remote_copy(
            src_ref=final.at[t, rows], dst_ref=dkv_ref.at[kind, z, rows], send_sem=fin_s.at[other_core],
            recv_sem=fin_r.at[other_core], device_id=(t, y, x, core), device_id_type=MESH,
        )

    def send_out(t):
        out(t, 1).start()
        @pl.when(t != z)
        def _():
            out(t, 0).start()

    with jax.named_scope("pc_first"):
        finish_first()
        loop(0, 4, send_out)
        loop(4, 8, dq_start)
    for kg in range(1, 4):
        with jax.named_scope(f"pc_row{kg}"):
            row_finish(kg)
    loop(8, 16, dq_start)
    for kg in range(1, 4):
        with jax.named_scope(f"pc_blk{kg}"):
            finish(kg)
            loop(4 * kg, 4 * kg + 4, send_out)
    dkv_ref[kind, z] = final[z]

    with jax.named_scope("pe_sends"):
        own_kv.wait_send()
        drain(kv_all.at[0, 0, pl.ds(0, 15)], zkv_s)
        drain(q_rows.at[pl.ds(0, 15)], zq_s)
        drain(g_rows.at[pl.ds(0, 15)], zg_s)
        drain(kv_all.at[0, :, pl.ds(0, 15)], ag_s)
        drain(kv_all.at[0], fw_s)
        o_finish()
        dq_finish()
        drain(other, sib_s)
        drain(first_in, dir_s)
        drain(row_in.at[pl.ds(0, 3)], row_s)
        drain(block_in.at[pl.ds(0, 3)], blk_s)
    with jax.named_scope("pf_dkv"):
        for sem in (fin_s, fin_r):
            drain(dkv_ref.at[0, pl.ds(0, 15), pl.ds(0, 4)], sem.at[0])
            drain(dkv_ref.at[1, :, pl.ds(0, 4)], sem.at[1])


def deliver(o_ref, dq_ref, dkv_ref, o_hbm, dq_hbm, dk_hbm, dv_hbm, wide, narrow, sem):
    c = lax.axis_index("c")
    copies = [
        pltpu.make_async_copy(o_ref, o_hbm, sem.at[0]),
        pltpu.make_async_copy(dq_ref, dq_hbm, sem.at[1]),
        pltpu.make_async_copy(narrow.at[0], dk_hbm, sem.at[2]),
        pltpu.make_async_copy(narrow.at[1], dv_hbm, sem.at[3]),
    ]
    copies[0].start()
    copies[1].start()
    wide[...] = dkv_ref[...].astype(F32)
    for core in range(2):
        @pl.when(c == core)
        def _():
            for kind in range(2):
                for l in range(2):
                    for i in range(4):
                        rows = wide[kind, 8 * l : 8 * l + 8, 4 * core + i, :]
                        narrow[kind, l, i] = rows.astype(BF16)
    copies[2].start()
    copies[3].start()
    for copy in copies:
        copy.wait()


def on_device(q, k, v, g):
    wide = (2, 4, 8, 8, 128)
    dma = pltpu.SemaphoreType.DMA
    hbm = pl.BlockSpec(memory_space=pltpu.MemorySpace.HBM)
    vmem = pl.BlockSpec(memory_space=pltpu.VMEM)
    inputs = (q.reshape(wide), k, v, g.reshape(wide))
    o, dq, dkv = pl.pallas_call(
        kernel,
        out_shape=(
            jax.ShapeDtypeStruct(wide, BF16),
            jax.ShapeDtypeStruct(wide, BF16),
            jax.ShapeDtypeStruct((2, 16, 8, 128), BF16),
        ),
        in_specs=[hbm, hbm, hbm, hbm],
        out_specs=(hbm, hbm, vmem),
        scratch_shapes=[
            pltpu.VMEM(wide, BF16),
            pltpu.VMEM((2, 4, 8, 128), BF16),
            pltpu.VMEM((2, 4, 8, 128), BF16),
            pltpu.VMEM(wide, BF16),
            pltpu.VMEM((2, 8, 8, 128), F32),
            pltpu.VMEM((2, 8, 8, 128), BF16),
            pltpu.VMEM((16, 4, 8, 128), BF16),
            pltpu.VMEM((16, 4, 8, 128), BF16),
            pltpu.VMEM((2, 16, 16, 8, 128), BF16),
            pltpu.VMEM((8, 128), BF16),
            pltpu.VMEM((4, 128, 512), BF16),
            pltpu.VMEM((4, 128, 512), BF16),
            pltpu.VMEM((512, 128), jnp.int32),
            pltpu.VMEM((8, 128), F32),
            pltpu.VMEM((8, 128), F32),
            pltpu.VMEM((4, 128, 128), F32),
            pltpu.VMEM((4, 128, 128), F32),
            pltpu.VMEM((4, 4, 512, 128), F32),
            pltpu.VMEM((4, 512, 1024), BF16),
            pltpu.VMEM((4, 512, 1024), BF16),
            pltpu.VMEM((1024, 128), BF16),
            pltpu.VMEM((1024, 128), BF16),
            pltpu.VMEM((16, 4, 8, 128), BF16),
            pltpu.VMEM((16, 4, 8, 128), BF16),
            pltpu.VMEM((2, 4, 4, 4, 4, 8, 128), F32),
            pltpu.VMEM((4, 4, 4, 4, 8, 128), F32),
            pltpu.VMEM((4, 3, 4, 4, 8, 128), F32),
            pltpu.VMEM((4, 4, 4, 8, 128), F32),
            pltpu.VMEM((4, 3, 4, 8, 128), F32),
            pltpu.VMEM((15, 4, 8, 128), F32),
            pltpu.VMEM((16, 8, 128), BF16),
            dma((6,)),
            dma, dma((3,)), dma, dma, dma, dma, dma, dma,
            dma, dma((3,)), dma, dma((3,)),
            dma, dma, dma, dma, dma, dma,
            dma, dma((4,)), dma, dma((4,)), dma, dma((4,)), dma, dma, dma((2,)), dma((2,)),
        ],
        compiler_params=pltpu.CompilerParams(
            collective_id=1,
            has_side_effects=True,
            vmem_limit_bytes=48 * 2**20,
        ),
        name="attend",
    )(*(pltpu.with_memory_space_constraint(a, pltpu.MemorySpace.HBM) for a in inputs))
    o, dq, dk, dv = pl.pallas_call(
        deliver,
        out_shape=tuple(jax.ShapeDtypeStruct(a.shape, BF16) for a in (o, dq, k, v)),
        in_specs=[hbm, hbm, vmem],
        out_specs=(hbm,) * 4,
        scratch_shapes=[
            pltpu.VMEM((2, 16, 8, 128), F32), pltpu.VMEM((2, 2, 4, 8, 128), BF16), dma((4,))
        ],
        compiler_params=pltpu.CompilerParams(vmem_limit_bytes=8 * 2**20),
        name="deliver",
    )(o, dq, dkv)
    return o.reshape(q.shape), dq.reshape(q.shape), dk, dv


def solution(mesh):
    grid = Mesh(mesh.devices.reshape(NZ, NY, NX, 2), ("z", "y", "x", "c"))
    spec = P(None, ("z", "y", "x", "c"), None, None)
    return jax.shard_map(
        on_device, mesh=grid, in_specs=(spec,) * 4, out_specs=(spec,) * 4, check_vma=False
    )
```

```python
import functools

import jax
import jax.numpy as jnp
from jax import lax
from jax.experimental import pallas as pl
from jax.experimental.pallas import tpu as pltpu
from jax.sharding import Mesh
from jax.sharding import PartitionSpec as P

MESH = pl.DeviceIdType.MESH
F32 = jnp.float32
BF16 = jnp.bfloat16
NZ, NY, NX = 16, 4, 4
MASKED = -1e30
PIECES = ((0, 7), (7, 6), (13, 3))


def nt(a, b):
    return lax.dot_general(a, b, (((1,), (1,)), ((), ())), preferred_element_type=F32)


def nn(a, b):
    return lax.dot_general(a, b, (((1,), (0,)), ((), ())), preferred_element_type=F32)


def split(a):
    high = a.astype(BF16)
    return high, (a - high.astype(F32)).astype(BF16)


def kernel(
    q_hbm, k_hbm, v_hbm, g_hbm, o_hbm, dq_hbm, dkv_ref,
    q_home, k_home, v_home, g_home, kv_wide, kv_home, q_rows, g_rows, kv_all,
    mate, keys_t, values_t, diagonal, row_delta, tops, attended_t, dq_t, scores, probs, dscores, g_twice, q_twice,
    o_rows, dq_rows, part, other, row_in, row_sum, block_in, first_in, final,
    in_sem, zkv_s, zkv_r, own_s, own_r, zq_s, zq_r, zg_s, zg_r, ag_s, ag_r, fw_s, fw_r,
    o_s, o_r, own_o, dq_s, dq_r, own_dq, sib_s, sib_r, row_s, row_r, blk_s, blk_r, dir_s, dir_r, fin_s, fin_r,
):
    z, y, x, c = (lax.axis_index(a) for a in ("z", "y", "x", "c"))
    chip = y * NX + x
    layer, group = z >> 3, z & 7
    scale = 128 ** -0.5

    def z_at(d):
        return (z + d) & 15

    def chip_at(e, sign):
        dy, dx = e >> 2, e & 3
        return (y + 4 + sign * dy) & 3, (x + 4 + sign * dx) & 3

    barrier = pltpu.get_barrier_semaphore()

    def greet(*device):
        pl.semaphore_signal(barrier, inc=1, device_id=device, device_id_type=MESH)

    for d in (8, 7, 9, 6, 10, 5, 11, 4, 12, 3, 13, 2, 14, 1, 15):
        greet(z_at(d), y, x, c)
        greet(z_at(d), y, x, 1 - c)
    for e in (10, 6, 9, 11, 14, 2, 8, 5, 7, 13, 15, 1, 3, 4, 12):
        greet(z, *chip_at(e, 1), c)
    greet(z, y, x, 1 - c)

    stage = [
        pltpu.make_async_copy(k_hbm, k_home, in_sem.at[0]),
        pltpu.make_async_copy(v_hbm, v_home, in_sem.at[1]),
        pltpu.make_async_copy(q_hbm, q_home, in_sem.at[2]),
        pltpu.make_async_copy(g_hbm, g_home, in_sem.at[3]),
        pltpu.make_async_copy(q_hbm.at[layer, :, group], q_rows.at[z], in_sem.at[4]),
        pltpu.make_async_copy(g_hbm.at[layer, :, group], g_rows.at[z], in_sem.at[5]),
    ]
    for copy in stage:
        copy.start()

    def drain(ref, sem):
        pltpu.make_async_remote_copy(
            src_ref=ref, dst_ref=ref, send_sem=sem, recv_sem=sem,
            device_id=(z, y, x, 1 - c), device_id_type=MESH,
        ).wait_recv()

    key_pos = lax.broadcasted_iota(jnp.int32, (512, 128), 0)
    lane = lax.broadcasted_iota(jnp.int32, (512, 128), 1)
    row_pos = 128 * (lane >> 5) + ((lane >> 3) & 3) + 8 * chip + 4 * c
    diagonal[...] = key_pos - row_pos
    identity = (
        lax.broadcasted_iota(jnp.int32, (128, 128), 0)
        == lax.broadcasted_iota(jnp.int32, (128, 128), 1)
    ).astype(F32).astype(BF16)

    with jax.named_scope("p0_kv"):
        stage[0].wait()
        stage[1].wait()
        for l in range(2):
            for i in range(4):
                kv_wide[l, :, i, :] = k_home[l, i].astype(F32)
                kv_wide[l, :, 4 + i, :] = v_home[l, i].astype(F32)
        kv_home[...] = kv_wide[...].astype(BF16)
        for copy in stage[2:]:
            copy.wait()
    with jax.named_scope("p1_barrier"):
        pl.semaphore_wait(barrier, 46)

    def to_z(src, dst, send, recv):
        def make(d):
            t = z_at(d)
            return pltpu.make_async_remote_copy(
                src_ref=src.at[t >> 3, :, t & 7], dst_ref=dst.at[z], send_sem=send,
                recv_sem=recv, device_id=(t, y, x, c), device_id_type=MESH,
            )
        return make

    half = pl.ds(pl.multiple_of(4 * c, 4), 4)

    def slot_of(u):
        return u + jnp.where(u < 10, 0, jnp.where(u < 13, 3, -3))

    def to_core(core, d, far):
        t = z_at(d)
        return pltpu.make_async_remote_copy(
            src_ref=kv_home.at[t >> 3, t & 7, pl.ds(4 - 4 * core, 4)],
            dst_ref=kv_all.at[1 - core, slot_of((19 - d) & 15), chip, half],
            send_sem=zkv_s, recv_sem=zkv_r.at[far],
            device_id=(t, y, x, core), device_id_type=MESH,
        )

    own_kv = pltpu.make_async_remote_copy(
        src_ref=kv_home.at[layer, group], dst_ref=mate, send_sem=own_s,
        recv_sem=own_r, device_id=(z, y, x, 1 - c), device_id_type=MESH,
    )
    zq = to_z(q_home, q_rows, zq_s, zq_r)
    zg = to_z(g_home, g_rows, zg_s, zg_r)

    def loop(low, high, body):
        def step(i, _):
            body(i)
            return 0
        lax.fori_loop(low, high, step, 0)

    def far_first(body):
        loop(1, 9, lambda i: body(9 - i))
        loop(9, 16, body)

    with jax.named_scope("p2_zstart"):
        own_kv.start()
        def send_kv(d, far):
            to_core(0, d, far).start()
            to_core(1, d, far).start()

        loop(1, 4, lambda d: (send_kv(d, 0), send_kv(16 - d, 0)))
        loop(4, 7, lambda d: (send_kv(d, 1), send_kv(16 - d, 1)))
        loop(7, 10, lambda d: send_kv(d, 2))
        loop(1, 16, lambda d: zq(d).start())
        far_first(lambda d: zg(d).start())


    def gather(n, e):
        j = jnp.where(e - 1 < chip, e - 1, e)
        block = kv_all.at[1 - c, pl.ds(*PIECES[n]), chip]
        return pltpu.make_async_remote_copy(
            src_ref=block, dst_ref=block, send_sem=ag_s,
            recv_sem=ag_r.at[n], device_id=(z, j >> 2, j & 3, c), device_id_type=MESH,
        )

    def forward(n):
        block = kv_all.at[1 - c, pl.ds(*PIECES[n])]
        return pltpu.make_async_remote_copy(
            src_ref=block, dst_ref=block, send_sem=fw_s,
            recv_sem=fw_r.at[n], device_id=(z, y, x, 1 - c), device_id_type=MESH,
        )

    with jax.named_scope("p3_zkvn"):
        own_kv.wait_recv()
        mine = pltpu.roll(kv_wide[layer, group], 4, 0)
        own_half = (lax.broadcasted_iota(jnp.int32, (8, 128), 0) >> 2) == c
        kv_all[1 - c, 3, chip] = jnp.where(own_half, mine, mate[...].astype(F32)).astype(BF16)
        drain(kv_all.at[0, 0, pl.ds(0, 6)], zkv_r.at[0])
        loop(1, 16, lambda e: gather(0, e).start())
    with jax.named_scope("p3_zkvm"):
        drain(kv_all.at[0, 0, pl.ds(0, 6)], zkv_r.at[1])
        loop(1, 16, lambda e: gather(1, e).start())
    with jax.named_scope("p3_zkvf"):
        drain(kv_all.at[0, 0, pl.ds(0, 3)], zkv_r.at[2])
        loop(1, 16, lambda e: gather(2, e).start())

    for n in range(3):
        with jax.named_scope(f"p4_ag{n}"):
            drain(kv_all.at[1 - c, pl.ds(*PIECES[n]), pl.ds(0, 15)], ag_r.at[n])
            forward(n).start()
    def of_core(core, body):
        @pl.when(c == core)
        def _():
            body()

    def from_sibling():
        for n in range(3):
            drain(kv_all.at[c, pl.ds(*PIECES[n])], fw_r.at[n])

    with jax.named_scope("p6_keys"):
        of_core(0, from_sibling)

    def plane_group(kind, kg):
        return jnp.concatenate(
            [kv_all[kind, slot_of((4 * kg + i + 19 - z) & 15)].reshape(128, 128) for i in range(4)], axis=0
        )

    with jax.named_scope("p8_qwait"):
        drain(q_rows.at[pl.ds(0, 15)], zq_r)

    def home(rows, out, send, recv, own_sem):
        def make(t):
            return pltpu.make_async_remote_copy(
                src_ref=rows.at[t], dst_ref=out.at[layer, :, group], send_sem=send,
                recv_sem=recv, device_id=(t, y, x, c), device_id_type=MESH,
            )
        own = pltpu.make_async_copy(rows.at[z], out.at[layer, :, group], own_sem)
        def start():
            far_first(lambda d: make(z_at(d)).start())
            own.start()
        def start_at(t):
            @pl.when(t != z)
            def _():
                make(t).start()
            @pl.when(t == z)
            def _():
                own.start()
        def finish():
            drain(rows.at[pl.ds(0, 15)], send)
            drain(rows.at[pl.ds(0, 15)], recv)
            own.wait()
        return start, start_at, finish

    o_start, _, o_finish = home(o_rows, o_hbm, o_s, o_r, own_o)
    _, dq_start, dq_finish = home(dq_rows, dq_hbm, dq_s, dq_r, own_dq)

    factor_2 = scale * 1.4426950408889634

    def pair(rg):
        return slice(256 * rg, 256 * rg + 256)

    def scores_of(rg):
        lanes = pair(rg)
        q = q_rows[4 * rg : 4 * rg + 4].astype(F32).reshape(128, 128).astype(BF16)
        q_twice[lanes] = jnp.concatenate([q, q], axis=0)
        top = jnp.full((8, 128), MASKED, F32)
        for kg in range(rg + 1):
            s = nt(plane_group(0, kg), q) * factor_2
            if kg == rg:
                s = jnp.where(diagonal[...] <= 0, s, MASKED)
            scores[rg, kg] = s
            top = jnp.maximum(top, jnp.max(s.reshape(64, 8, 128), axis=0))
        return jnp.max(top, axis=0, keepdims=True)

    def forward_of(rg, top):
        lanes = pair(rg)
        total = jnp.zeros((8, 128), F32)
        for kg in range(rg + 1):
            e = jnp.exp2(scores[rg, kg] - top)
            scores[rg, kg] = e
            total = total + jnp.sum(e.reshape(64, 8, 128), axis=0)
        inverse = 1.0 / jnp.sum(total, axis=0, keepdims=True)
        acc = jnp.zeros((128, 256), F32)
        for kg in range(rg + 1):
            p = scores[rg, kg] * inverse
            p2 = jnp.concatenate(split(p), axis=1)
            probs[kg, :, lanes] = p2
            scores[rg, kg] = p
            acc = acc + nn(values_t[kg], p2)
        o_t = acc[:, :128] + acc[:, 128:]
        attended_t[rg] = o_t.astype(BF16).astype(F32)
        o_rows[4 * rg : 4 * rg + 4] = o_t.T.reshape(4, 4, 8, 128).astype(BF16)

    def deltas(rg):
        g = g_rows[4 * rg : 4 * rg + 4].astype(F32).reshape(128, 128).astype(BF16)
        g_twice[pair(rg)] = jnp.concatenate([g, g], axis=0)
        delta = nt(identity, g) * attended_t[rg]
        row_delta[rg : rg + 1] = jnp.sum(delta, axis=0, keepdims=True)

    def backward_of(kg):
        for rg in range(kg, 4):
            g = g_twice[256 * rg : 256 * rg + 128]
            ds = scores[rg, kg] * (nt(plane_group(1, kg), g) - row_delta[rg : rg + 1])
            ds2 = jnp.concatenate(split(ds), axis=1)
            dscores[kg, :, pair(rg)] = ds2
            term = nn(keys_t[kg], ds2)
            term = term[:, :128] + term[:, 128:]
            dq_t[rg] = dq_t[rg] + term if kg else term
        dq_rows[4 * kg : 4 * kg + 4] = (dq_t[kg] * scale).T.reshape(4, 4, 8, 128).astype(BF16)
        part[0, kg] = key_sum(kg, kg, 4)
        part[1, kg] = value_sum(kg, kg, 4)

    def value_sum(kg, low, high):
        lanes = slice(256 * low, 256 * high)
        return nn(probs[kg, :, lanes], g_twice[lanes]).reshape(4, 4, 4, 8, 128)

    def key_sum(kg, low, high):
        lanes = slice(256 * low, 256 * high)
        dk = nn(dscores[kg, :, lanes], q_twice[lanes])
        return jnp.swapaxes(dk.reshape(4, 4, 4, 8, 128), 1, 2)

    kind = 1 - c
    along = jnp.where(c == 0, y, x)
    across = jnp.where(c == 0, x, y)

    def sibling(kg):
        return pltpu.make_async_remote_copy(
            src_ref=part.at[c, kg], dst_ref=other.at[kg], send_sem=sib_s,
            recv_sem=sib_r.at[kg], device_id=(z, y, x, 1 - c), device_id_type=MESH,
        )

    def row_send(kg, a):
        t = (along + a) & 3
        return pltpu.make_async_remote_copy(
            src_ref=part.at[kind, kg, :, t], dst_ref=row_in.at[kg, a - 1], send_sem=row_s,
            recv_sem=row_r.at[kg],
            device_id=(z, jnp.where(c == 0, t, y), jnp.where(c == 0, x, t), c), device_id_type=MESH,
        )

    def block_send(kg, a):
        t = (across + a) & 3
        return pltpu.make_async_remote_copy(
            src_ref=row_sum.at[kg, :, t], dst_ref=block_in.at[kg, a - 1], send_sem=blk_s,
            recv_sem=blk_r.at[kg],
            device_id=(z, jnp.where(c == 0, y, t), jnp.where(c == 0, t, x), c), device_id_type=MESH,
        )

    def direct_send(j):
        yy, xx = j >> 2, j & 3
        a, b = jnp.where(c == 0, yy, xx), jnp.where(c == 0, xx, yy)
        return pltpu.make_async_remote_copy(
            src_ref=part.at[kind, 0, :, a, b], dst_ref=first_in.at[(j - chip + 15) & 15],
            send_sem=dir_s, recv_sem=dir_r, device_id=(z, yy, xx, c), device_id_type=MESH,
        )

    def combine(kg):
        sibling(kg).wait_recv()
        part[kind, kg] = part[kind, kg] + other[kg]
        if kg:
            loop(1, 4, lambda a: row_send(kg, a).start())
        else:
            for e in (10, 6, 14, 9, 11, 2, 8, 5, 7, 13, 15, 1, 3, 4, 12):
                yy, xx = chip_at(e, 1)
                direct_send(4 * yy + xx).start()

    with jax.named_scope("p9_scores"):
        for rg in range(4):
            tops[rg : rg + 1] = scores_of(rg)
        for kg in range(4):
            keys_t[kg] = nt(identity, plane_group(0, kg)).astype(BF16)
    with jax.named_scope("p9_values"):
        of_core(1, from_sibling)
    with jax.named_scope("p9_fwd"):
        for kg in range(4):
            values_t[kg] = nt(identity, plane_group(1, kg)).astype(BF16)
        for rg in range(4):
            forward_of(rg, tops[rg : rg + 1])

    with jax.named_scope("pa_osend"):
        o_start()
        drain(g_rows.at[pl.ds(0, 15)], zg_r)
    for kg in range(4):
        with jax.named_scope(f"p9_bwd{kg}"):
            if kg == 0:
                for rg in range(4):
                    deltas(rg)
            backward_of(kg)
        with jax.named_scope(f"pa_comb{kg}"):
            sibling(kg).start()
            if kg == 0:
                loop(0, 4, dq_start)
            if kg:
                combine(kg - 1)
    with jax.named_scope("pb_combine"):
        combine(3)

    def row_finish(kg):
        drain(row_in.at[kg], row_r.at[kg])
        total = part[kind, kg, :, along]
        for a in range(3):
            total = total + row_in[kg, a]
        row_sum[kg] = total
        loop(1, 4, lambda a: block_send(kg, a).start())

    factor = jnp.where(c == 0, 1.0, scale).astype(F32)

    def finish_first():
        drain(first_in, dir_r)
        total = part[kind, 0, :, along, across]
        for e in range(15):
            total = total + first_in[e]
        final[pl.ds(0, 4)] = (total * factor).astype(BF16)

    def finish(kg):
        drain(block_in.at[kg], blk_r.at[kg])
        total = row_sum[kg, :, across]
        for a in range(3):
            total = total + block_in[kg, a]
        final[pl.ds(4 * kg, 4)] = (total * factor).astype(BF16)

    def out(t, other_core):
        core = 1 - c if other_core else c
        rows = pl.ds(pl.multiple_of(4 * core, 4), 4)
        return pltpu.make_async_remote_copy(
            src_ref=final.at[t, rows], dst_ref=dkv_ref.at[kind, z, rows], send_sem=fin_s.at[other_core],
            recv_sem=fin_r.at[other_core], device_id=(t, y, x, core), device_id_type=MESH,
        )

    def send_out(t):
        out(t, 1).start()
        @pl.when(t != z)
        def _():
            out(t, 0).start()

    with jax.named_scope("pc_first"):
        finish_first()
        loop(0, 4, send_out)
        loop(4, 16, dq_start)
    for kg in range(1, 4):
        with jax.named_scope(f"pc_row{kg}"):
            row_finish(kg)
    for kg in range(1, 4):
        with jax.named_scope(f"pc_blk{kg}"):
            finish(kg)
            loop(4 * kg, 4 * kg + 4, send_out)
    dkv_ref[kind, z] = final[z]

    with jax.named_scope("pe_sends"):
        own_kv.wait_send()
        drain(kv_all.at[0, 0, pl.ds(0, 15)], zkv_s)
        drain(q_rows.at[pl.ds(0, 15)], zq_s)
        drain(g_rows.at[pl.ds(0, 15)], zg_s)
        drain(kv_all.at[0, :, pl.ds(0, 15)], ag_s)
        drain(kv_all.at[0], fw_s)
        o_finish()
        dq_finish()
        drain(other, sib_s)
        drain(first_in, dir_s)
        drain(row_in.at[pl.ds(0, 3)], row_s)
        drain(block_in.at[pl.ds(0, 3)], blk_s)
    with jax.named_scope("pf_dkv"):
        for sem in (fin_s, fin_r):
            drain(dkv_ref.at[0, pl.ds(0, 15), pl.ds(0, 4)], sem.at[0])
            drain(dkv_ref.at[1, :, pl.ds(0, 4)], sem.at[1])


def deliver(o_ref, dq_ref, dkv_ref, o_hbm, dq_hbm, dk_hbm, dv_hbm, wide, narrow, sem):
    c = lax.axis_index("c")
    copies = [
        pltpu.make_async_copy(o_ref, o_hbm, sem.at[0]),
        pltpu.make_async_copy(dq_ref, dq_hbm, sem.at[1]),
        pltpu.make_async_copy(narrow.at[0], dk_hbm, sem.at[2]),
        pltpu.make_async_copy(narrow.at[1], dv_hbm, sem.at[3]),
    ]
    copies[0].start()
    copies[1].start()
    wide[...] = dkv_ref[...].astype(F32)
    for core in range(2):
        @pl.when(c == core)
        def _():
            for kind in range(2):
                for l in range(2):
                    for i in range(4):
                        rows = wide[kind, 8 * l : 8 * l + 8, 4 * core + i, :]
                        narrow[kind, l, i] = rows.astype(BF16)
    copies[2].start()
    copies[3].start()
    for copy in copies:
        copy.wait()


def on_device(q, k, v, g):
    wide = (2, 4, 8, 8, 128)
    dma = pltpu.SemaphoreType.DMA
    hbm = pl.BlockSpec(memory_space=pltpu.MemorySpace.HBM)
    vmem = pl.BlockSpec(memory_space=pltpu.VMEM)
    inputs = (q.reshape(wide), k, v, g.reshape(wide))
    o, dq, dkv = pl.pallas_call(
        kernel,
        out_shape=(
            jax.ShapeDtypeStruct(wide, BF16),
            jax.ShapeDtypeStruct(wide, BF16),
            jax.ShapeDtypeStruct((2, 16, 8, 128), BF16),
        ),
        in_specs=[hbm, hbm, hbm, hbm],
        out_specs=(hbm, hbm, vmem),
        scratch_shapes=[
            pltpu.VMEM(wide, BF16),
            pltpu.VMEM((2, 4, 8, 128), BF16),
            pltpu.VMEM((2, 4, 8, 128), BF16),
            pltpu.VMEM(wide, BF16),
            pltpu.VMEM((2, 8, 8, 128), F32),
            pltpu.VMEM((2, 8, 8, 128), BF16),
            pltpu.VMEM((16, 4, 8, 128), BF16),
            pltpu.VMEM((16, 4, 8, 128), BF16),
            pltpu.VMEM((2, 16, 16, 8, 128), BF16),
            pltpu.VMEM((8, 128), BF16),
            pltpu.VMEM((4, 128, 512), BF16),
            pltpu.VMEM((4, 128, 512), BF16),
            pltpu.VMEM((512, 128), jnp.int32),
            pltpu.VMEM((8, 128), F32),
            pltpu.VMEM((8, 128), F32),
            pltpu.VMEM((4, 128, 128), F32),
            pltpu.VMEM((4, 128, 128), F32),
            pltpu.VMEM((4, 4, 512, 128), F32),
            pltpu.VMEM((4, 512, 1024), BF16),
            pltpu.VMEM((4, 512, 1024), BF16),
            pltpu.VMEM((1024, 128), BF16),
            pltpu.VMEM((1024, 128), BF16),
            pltpu.VMEM((16, 4, 8, 128), BF16),
            pltpu.VMEM((16, 4, 8, 128), BF16),
            pltpu.VMEM((2, 4, 4, 4, 4, 8, 128), F32),
            pltpu.VMEM((4, 4, 4, 4, 8, 128), F32),
            pltpu.VMEM((4, 3, 4, 4, 8, 128), F32),
            pltpu.VMEM((4, 4, 4, 8, 128), F32),
            pltpu.VMEM((4, 3, 4, 8, 128), F32),
            pltpu.VMEM((15, 4, 8, 128), F32),
            pltpu.VMEM((16, 8, 128), BF16),
            dma((6,)),
            dma, dma((3,)), dma, dma, dma, dma, dma, dma,
            dma, dma((3,)), dma, dma((3,)),
            dma, dma, dma, dma, dma, dma,
            dma, dma((4,)), dma, dma((4,)), dma, dma((4,)), dma, dma, dma((2,)), dma((2,)),
        ],
        compiler_params=pltpu.CompilerParams(
            collective_id=1,
            has_side_effects=True,
            vmem_limit_bytes=48 * 2**20,
        ),
        name="attend",
    )(*(pltpu.with_memory_space_constraint(a, pltpu.MemorySpace.HBM) for a in inputs))
    o, dq, dk, dv = pl.pallas_call(
        deliver,
        out_shape=tuple(jax.ShapeDtypeStruct(a.shape, BF16) for a in (o, dq, k, v)),
        in_specs=[hbm, hbm, vmem],
        out_specs=(hbm,) * 4,
        scratch_shapes=[
            pltpu.VMEM((2, 16, 8, 128), F32), pltpu.VMEM((2, 2, 4, 8, 128), BF16), dma((4,))
        ],
        compiler_params=pltpu.CompilerParams(vmem_limit_bytes=8 * 2**20),
        name="deliver",
    )(o, dq, dkv)
    return o.reshape(q.shape), dq.reshape(q.shape), dk, dv


def solution(mesh):
    grid = Mesh(mesh.devices.reshape(NZ, NY, NX, 2), ("z", "y", "x", "c"))
    spec = P(None, ("z", "y", "x", "c"), None, None)
    return jax.shard_map(
        on_device, mesh=grid, in_specs=(spec,) * 4, out_specs=(spec,) * 4, check_vma=False
    )
```
